8 devices in a mesh: g: 1 (over z), y: 2 (over y), x: 4 (over x, core).
Axes of the slice: x: 2, y: 2, z: 1, core: 2. Of those that a mesh axis runs over, the one named last changes fastest.
Arguments:
- source: float32 [96, 96, 200], P(('g', 'x'), 'y')
- sigma_t: float32 [96, 96, 200], P(('g', 'x'), 'y')
- cos_x: float32 [10], replicated
- cos_y: float32 [10], replicated
- cos_z: float32 [10], replicated
- weights: float32 [10], replicated
Outputs:
- output: float32 [96, 96, 200], P(('g', 'x'), 'y')
All inputs are finite; a program needn't handle non-finite values.
Results may differ from the reference program's by a relative error of at most 0.001.
Values sent between devices are 32-bit elements.
A program may use at most 1 GiB of HBM per device.

```python
import jax
import jax.numpy as jnp
from jax import lax

GRID_X = 96
GRID_Y = 96
GRID_Z = 200
ANGLES = 10
CHIP_WIDTH = 48


def skew_last(values):
    n_rows, n_cols = values.shape[-2], values.shape[-1]
    lead_dims = values.shape[:-2]
    widths = [(0, 0)] * len(lead_dims) + [(0, 0), (0, n_rows)]
    flat_vals = jnp.pad(values, widths).reshape(lead_dims + (n_rows * (n_cols + n_rows),))
    kept_vals = flat_vals[..., : n_rows * (n_cols + n_rows - 1)]
    return kept_vals.reshape(lead_dims + (n_rows, n_cols + n_rows - 1))


def unskew_last(values, length):
    n_rows, n_cols = values.shape[-2], values.shape[-1]
    lead_dims = values.shape[:-2]
    flat_vals = values.reshape(lead_dims + (n_rows * n_cols,))
    flat_vals = jnp.pad(flat_vals, [(0, 0)] * len(lead_dims) + [(0, n_rows)])
    return flat_vals.reshape(lead_dims + (n_rows, n_cols + 1))[..., :length]


def skew_grid(grid_arr):
    first_pass = skew_last(grid_arr)
    second_pass = skew_last(jnp.transpose(first_pass, (0, 2, 1, 3)))
    return jnp.transpose(second_pass, (3, 0, 2, 1))


def unskew_grid(skewed, size_z):
    size_y = skewed.shape[3]
    first_pass = unskew_last(jnp.transpose(skewed, (1, 3, 2, 0)), size_z + size_y - 1)
    return unskew_last(jnp.transpose(first_pass, (0, 2, 1, 3)), size_z)


def face_to_skew(face_arr, n_steps):
    size_n, size_l = face_arr.shape[1], face_arr.shape[2]
    skewed = skew_last(jnp.transpose(face_arr, (0, 3, 1, 2)))
    skewed = jnp.pad(skewed, ((0, 0), (0, 0), (0, 0), (0, n_steps - size_l - size_n + 1)))
    return jnp.transpose(skewed, (3, 0, 2, 1))


def skew_to_face(skewed, offset, size_l):
    tail_part = jnp.transpose(skewed[offset:], (1, 3, 2, 0))
    return jnp.transpose(unskew_last(tail_part, size_l), (0, 2, 3, 1))


def sweep_box(src_sk, sig_sk, xin_sk, yin_sk, z_in, cos_x, cos_y, cos_z, weights, size_l):
    n_steps, size_x, size_y = src_sk.shape[0], src_sk.shape[2], src_sk.shape[3]
    coef_x = 2.0 * cos_x
    coef_y = 2.0 * cos_y
    coef_z = 2.0 * cos_z
    coef_sum = coef_x + coef_y + coef_z
    diagonal = jnp.arange(size_x)[:, None] + jnp.arange(size_y)[None, :]

    def plane_step(carry_in, inputs):
        face_x, face_y, face_z = carry_in
        src_t, sig_t, edge_x, edge_y, step_idx = inputs
        in_x = jnp.concatenate([edge_x[:, None], face_x[:, :-1]], axis=1)
        in_y = jnp.concatenate([edge_y[:, :, None], face_y[:, :, :-1]], axis=2)
        ang_flux = (src_t[..., None] + coef_x * in_x + coef_y * in_y + coef_z * face_z) / (sig_t[..., None] + coef_sum)
        z_level = step_idx - diagonal
        inside = ((z_level >= 0) & (z_level < size_l))[None, :, :, None]
        out_x = jnp.where(inside, 2.0 * ang_flux - in_x, 0.0)
        out_y = jnp.where(inside, 2.0 * ang_flux - in_y, 0.0)
        out_z = jnp.where(inside, 2.0 * ang_flux - face_z, face_z)
        flux_t = jnp.where(inside[..., 0], jnp.sum(ang_flux * weights, axis=-1), 0.0)
        return (out_x, out_y, out_z), (flux_t, out_x[:, size_x - 1], out_y[:, :, size_y - 1])

    zero_faces = jnp.zeros_like(z_in)
    carry_out, outputs = lax.scan(plane_step, (zero_faces, zero_faces, z_in), (src_sk, sig_sk, xin_sk, yin_sk, jnp.arange(n_steps)))
    return outputs[0], outputs[1], outputs[2], carry_out[2]


def sweep_grid(src_two, sig_two, in_x, in_y, cos_x, cos_y, cos_z, weights):
    size_x, size_y, size_z = src_two.shape[1], src_two.shape[2], src_two.shape[3]
    n_steps = size_x + size_y + size_z - 2
    z_in = jnp.zeros((2, size_x, size_y, cos_x.shape[0]), src_two.dtype)
    flux_sk, xout_sk, yout_sk, _ = sweep_box(skew_grid(src_two), skew_grid(sig_two), face_to_skew(in_x, n_steps), face_to_skew(in_y, n_steps), z_in, cos_x, cos_y, cos_z, weights, size_z)
    return unskew_grid(flux_sk, size_z), skew_to_face(xout_sk, size_x - 1, size_z), skew_to_face(yout_sk, size_y - 1, size_z)


def transport(source, sigma_t, cos_x, cos_y, cos_z, weights):
    size_x, size_y, size_z = source.shape
    n_dirs = cos_x.shape[0]
    src_two = jnp.stack([source, jnp.flip(source, 2)])
    sig_two = jnp.stack([sigma_t, jnp.flip(sigma_t, 2)])
    none_x = jnp.zeros((2, size_y, size_z, n_dirs), source.dtype)
    none_y = jnp.zeros((2, size_x, size_z, n_dirs), source.dtype)
    flux_mm, xout_mm, yout_mm = sweep_grid(jnp.flip(src_two, (1, 2)), jnp.flip(sig_two, (1, 2)), none_x, none_y, cos_x, cos_y, cos_z, weights)
    flux_pm, _, yout_pm = sweep_grid(jnp.flip(src_two, 2), jnp.flip(sig_two, 2), xout_mm, none_y, cos_x, cos_y, cos_z, weights)
    flux_mp, xout_mp, _ = sweep_grid(jnp.flip(src_two, 1), jnp.flip(sig_two, 1), none_x, yout_mm, cos_x, cos_y, cos_z, weights)
    flux_pp, _, _ = sweep_grid(src_two, sig_two, xout_mp, yout_pm, cos_x, cos_y, cos_z, weights)
    total_flux = jnp.flip(flux_mm, (1, 2)) + jnp.flip(flux_pm, 2) + jnp.flip(flux_mp, 1) + flux_pp
    return total_flux[0] + jnp.flip(total_flux[1], 2)


def setup_inputs(seed: int = 0, part: int = 0) -> dict:
    root_key = jax.random.key(seed)
    grid_key = jax.random.fold_in(root_key, part)
    key_src, key_sig = jax.random.split(grid_key)
    key_dir, key_wts = jax.random.split(jax.random.key(seed + 1))
    inv_width = 1.0 / CHIP_WIDTH
    corner = ((jnp.arange(GRID_X) < max(GRID_X // 4, 1))[:, None, None]
              & (jnp.arange(GRID_Y) < max(GRID_Y // 4, 1))[None, :, None]
              & (jnp.arange(GRID_Z) < max(GRID_Z // 4, 1))[None, None, :])
    src_rand = jax.random.uniform(key_src, (GRID_X, GRID_Y, GRID_Z), jnp.float32)
    source = (0.2 + 0.8 * src_rand + 2.0 * corner) * inv_width
    sig_rand = jax.random.uniform(key_sig, (GRID_X, GRID_Y, GRID_Z), jnp.float32)
    sigma_t = (0.2 + 0.8 * sig_rand) * inv_width
    cosines = jax.random.uniform(key_dir, (3, ANGLES), jnp.float32, 0.2, 1.0)
    cosines = cosines / jnp.sqrt(jnp.sum(cosines * cosines, axis=0))
    weight_raw = jax.random.uniform(key_wts, (ANGLES,), jnp.float32, 0.25, 1.75)
    weights = weight_raw / (8.0 * ANGLES)
    return {"source": source, "sigma_t": sigma_t, "cos_x": cosines[0], "cos_y": cosines[1], "cos_z": cosines[2], "weights": weights}


def reference(source, sigma_t, cos_x, cos_y, cos_z, weights):
    return transport(source, sigma_t, cos_x, cos_y, cos_z, weights)
```

```python
import functools

import jax
import jax.numpy as jnp
from jax import lax
from jax.experimental import pallas as pl
from jax.experimental.pallas import tpu as pltpu
from jax.sharding import PartitionSpec as P

F32 = jnp.float32
MESH = pl.DeviceIdType.MESH
NX, NY, NZ = 24, 48, 200
ND = 10
NB = NZ // 8
ROWS = NB * 72
D_NEAR = 8
D_FAR = 15
D_Y = 16
D_XR = 1
D_YR = 2
RING = 32
NSEND = 4


def x_lags():
    hops = [D_NEAR, D_FAR, D_NEAR, D_XR, D_NEAR, D_FAR, D_NEAR]
    lags = [0]
    for hop in hops:
        lags.append(lags[-1] + 8 + hop)
    return lags


def y_lags():
    lags = [0]
    for hop in [D_Y, D_YR, D_Y]:
        lags.append(lags[-1] + 16 + hop)
    return lags


LAG_X, LAG_Y = x_lags(), y_lags()
STEPS = ND * NB + LAG_X[-1] + LAG_Y[-1] + 7 + 15 + 1


def pick(values, idx):
    out = jnp.int32(values[0])
    for pos in range(1, len(values)):
        out = jnp.where(idx == pos, jnp.int32(values[pos]), out)
    return out


def kernel(cx_ref, cy_ref, cz_ref, wt_ref, src_ref, sig_ref, out_ref,
           nat, tab, flux, acc, hbuf, ctab, xbuf, ybuf, yraw, zbuf, eyb,
           xsend, xrecv, ysend, yrecv, v1ring, v2ring,
           xs_sem, xr_sem, ys_sem, yr_sem):
    dx = lax.axis_index("x")
    dy = lax.axis_index("y")
    has_left, has_right = dx > 0, dx < 3
    odd_x = lax.rem(dx, 2) == 1
    lag_left = jnp.where(odd_x, D_NEAR, D_FAR)
    lag_right = jnp.where(odd_x, D_FAR, D_NEAR)
    lane = lax.broadcasted_iota(jnp.int32, (8, 128), 1)
    subl = lax.broadcasted_iota(jnp.int32, (8, 128), 0)
    oct_id = lane // 16
    patch_y = lane - 16 * oct_id
    zero = jnp.zeros((8, 128), F32)
    low_half = lane < 64
    first_y = patch_y == 0

    lag_xm, lag_xp = pick(LAG_X[:4][::-1], dx), pick(LAG_X[4:], dx)
    lag_ym, lag_yp = pick(LAG_Y[:2][::-1], dy), pick(LAG_Y[2:], dy)
    lag_oct = (jnp.where(lane >= 64, lag_xp, lag_xm)
               + jnp.where((oct_id // 2) % 2 == 1, lag_yp, lag_ym))
    lag_lane = patch_y + lag_oct
    hbuf[...] = lag_lane + subl
    turn = lax.rem(lag_lane, NB)
    turn_bits = [(turn >> bit) & 1 == 1 for bit in range(5)]

    for pos in range(5):
        col = jnp.ones((8, 128), F32) if pos == 0 else zero
        for m in range(ND):
            two_x, two_y, two_z = 2.0 * cx_ref[m], 2.0 * cy_ref[m], 2.0 * cz_ref[m]
            val = (two_x + two_y + two_z, 2.0 * two_x, 2.0 * two_y, 2.0 * two_z, wt_ref[m])[pos]
            col = jnp.where(lane == m + 1, val, col)
        ctab[pos] = col

    for k in range(28):
        xbuf[pl.ds(8 * k, 8), :] = zero
    for k in range(24):
        ybuf[k] = zero
        eyb[k] = zero
    for k in range(12):
        yraw[k] = zero
    for k in range(9):
        zbuf[k] = zero
    for k in range(4):
        v1ring[k] = zero
        v2ring[k] = zero

    @pl.loop(0, RING)
    def _(k):
        for side in range(2):
            xrecv[side, k, pl.ds(0, 8), :] = zero
            xrecv[side, k, pl.ds(8, 8), :] = zero
        yrecv[k] = zero

    barrier = pltpu.get_barrier_semaphore()

    @pl.when(has_left)
    def _():
        pl.semaphore_signal(barrier, inc=1, device_id={"x": dx - 1}, device_id_type=MESH)

    @pl.when(has_right)
    def _():
        pl.semaphore_signal(barrier, inc=1, device_id={"x": dx + 1}, device_id_type=MESH)

    pl.semaphore_signal(barrier, inc=1, device_id={"y": 1 - dy}, device_id_type=MESH)

    mirror = (71 - lane) & 127
    tail = lane < 72

    @pl.loop(0, NX)
    def _(x):
        for arr, ref in enumerate((src_ref, sig_ref)):
            for yt in range(NY // 8):
                rows = pl.ds(8 * yt, 8)
                half_a = ref[x, rows, pl.ds(0, 128)]
                nat[arr, 0, x, rows, :] = half_a
                nat[arr, 1, x, rows, pl.ds(0, 72)] = ref[x, rows, pl.ds(128, 72)]
                half_b = nat[arr, 1, x, rows, :]
                flip_a = jnp.take_along_axis(half_a, mirror, axis=1)
                flip_b = jnp.take_along_axis(half_b, mirror, axis=1)
                nat[arr, 2, x, rows, :] = jnp.where(tail, flip_b, flip_a)
                nat[arr, 3, x, rows, :] = flip_a
        for part in range(8):
            for yt in range(NY // 8):
                acc[part, x, pl.ds(8 * yt, 8), :] = zero

    flip_rows = 7 - subl

    def row_groups(x_patch, i, j):
        for octant in range(8):
            bx, by = octant // 4, (octant // 2) % 2
            x_rel = 3 * x_patch + i
            x_abs = x_rel if bx else NX - 1 - x_rel
            for half in range(2):
                y_abs = (24 * half + j) if by else (26 - 24 * half - j)
                yield octant, half, x_abs, y_abs, by == 0

    def turn_blocks(blocks, step):
        for bit in range(5):
            shift = step * (1 << bit)
            blocks = [jnp.where(turn_bits[bit], blocks[(v - shift) % NB], blocks[v]) for v in range(NB)]
        return blocks

    @pl.loop(0, 8)
    def _(xp):
        for i in range(3):
            for j in range(3):
                cell = 3 * i + j
                for arr in range(2):
                    pieces = [[], []]
                    for octant, half, x_abs, y_abs, rev in row_groups(xp, i, j):
                        for zh in range(2):
                            kind = zh + (0 if octant % 2 else 2)
                            val = nat[arr, kind, x_abs, pl.ds(y_abs, 8, stride=3), :]
                            if rev:
                                val = jnp.take_along_axis(val, flip_rows, axis=0)
                            pieces[zh].append(val)
                    lo = jnp.concatenate(pieces[0], axis=0).T
                    hi = jnp.concatenate(pieces[1], axis=0).T
                    blocks = [lo[8 * v:8 * v + 8] for v in range(16)] + [hi[8 * v:8 * v + 8] for v in range(9)]
                    blocks = turn_blocks(blocks, 1)
                    for v in range(NB):
                        start = lax.rem(v + xp, NB) * 72 + xp
                        tab[arr, cell, pl.ds(start, 8, stride=9), :] = blocks[v]
                        if arr == 0:
                            flux[cell, pl.ds(start, 8, stride=9), :] = zero

    pl.semaphore_wait(barrier, has_left.astype(jnp.int32) + has_right.astype(jnp.int32) + 1)

    from_neg = ((oct_id + 1) // 2) % 2
    keep_send = from_neg == dy
    keep_recv = from_neg == 1 - dy
    mirror_y = dy == 0
    mirror_x = dx == 0

    def x_copy(side, n):
        lag = lag_left if side == 0 else lag_right
        slot = lax.rem(n + lag, RING)
        return pltpu.make_async_remote_copy(
            src_ref=xsend.at[side, lax.rem(n, NSEND)], dst_ref=xrecv.at[side, slot],
            send_sem=xs_sem.at[side, lax.rem(n, NSEND)], recv_sem=xr_sem.at[side, slot],
            device_id={"x": dx - 1 if side == 0 else dx + 1}, device_id_type=MESH)

    def y_copy(n):
        slot = lax.rem(n - 1 + D_Y, RING)
        return pltpu.make_async_remote_copy(
            src_ref=ysend.at[lax.rem(n, NSEND)], dst_ref=yrecv.at[slot],
            send_sem=ys_sem.at[lax.rem(n, NSEND)], recv_sem=yr_sem.at[slot],
            device_id={"y": 1 - dy}, device_id_type=MESH)

    def x_sends(side, n):
        has, lag = (has_left, lag_left) if side == 0 else (has_right, lag_right)
        return has & (n >= 1) & (n + lag <= STEPS - 1)

    def y_sends(n):
        return (n >= 2) & (n - 1 + D_Y <= STEPS - 1)

    def x_waits(side, n):
        has, lag = (has_right, lag_right) if side == 0 else (has_left, lag_left)
        return has & (n >= lag) & (n + 1 <= STEPS - 1)

    def y_waits(n):
        return (n >= D_Y) & (n + 1 <= STEPS - 1)

    def step(n, carry):
        next_slot = lax.rem(n + 1, RING)
        send_slot = lax.rem(n, NSEND)

        for side in range(2):
            @pl.when(x_waits(side, n))
            def _(side=side):
                pltpu.make_async_remote_copy(
                    src_ref=xsend.at[side, 0], dst_ref=xrecv.at[side, next_slot],
                    send_sem=xs_sem.at[side, 0], recv_sem=xr_sem.at[side, next_slot],
                    device_id={"x": dx}, device_id_type=MESH).wait_recv()

            @pl.when(x_sends(side, n - NSEND))
            def _(side=side):
                x_copy(side, n - NSEND).wait_send()

        @pl.when(y_waits(n))
        def _():
            pltpu.make_async_remote_copy(
                src_ref=ysend.at[0], dst_ref=yrecv.at[next_slot],
                send_sem=ys_sem.at[0], recv_sem=yr_sem.at[next_slot],
                device_id={"y": dy}, device_id_type=MESH).wait_recv()

        @pl.when(y_sends(n - NSEND))
        def _():
            y_copy(n - NSEND).wait_send()

        msg_slot = lax.rem(n + 2, 4)
        v1_old, v2_old = v1ring[msg_slot], v2ring[msg_slot]
        ysend[send_slot] = jnp.where(keep_send, v1_old, v2_old)

        outs = [xbuf[pl.ds(72 * q + 8, 8, stride=9), :] for q in range(3)]
        swapped = pltpu.roll(outs[1], 64, 1)
        left_a = jnp.where(low_half, outs[0], swapped)
        right_a = jnp.where(low_half, swapped, outs[0])
        xsend[0, send_slot, pl.ds(0, 8), :] = left_a
        xsend[0, send_slot, pl.ds(8, 8), :] = outs[2]
        xsend[1, send_slot, pl.ds(0, 8), :] = right_a
        xsend[1, send_slot, pl.ds(8, 8), :] = outs[2]

        from_r_a, from_r_b = xrecv[0, next_slot, pl.ds(0, 8), :], xrecv[0, next_slot, pl.ds(8, 8), :]
        from_l_a = jnp.where(mirror_x, pltpu.roll(left_a, 64, 1), xrecv[1, next_slot, pl.ds(0, 8), :])
        from_l_b = jnp.where(mirror_x, pltpu.roll(outs[2], 64, 1), xrecv[1, next_slot, pl.ds(8, 8), :])
        edges = [jnp.where(low_half, from_r_a, from_l_a),
                 pltpu.roll(jnp.where(low_half, from_l_a, from_r_a), 64, 1),
                 jnp.where(low_half, from_r_b, from_l_b)]

        pack2 = lax.rem(n + 3, 4)
        for k in range(12):
            raw = yraw[k]
            ybuf[12 + k] = jnp.where(first_y, eyb[12 + k], pltpu.roll(raw, 1, 1))
            pltpu.store(v2ring.at[pack2], pltpu.roll(raw, (33 + k) % 128, 1), mask=patch_y == k)

        got = yrecv[next_slot]
        in1 = jnp.where(keep_recv, got, jnp.where(mirror_y, pltpu.roll(v1_old, 32, 1), 0.0))
        in2 = jnp.where(keep_recv, pltpu.roll(got, 96, 1), jnp.where(mirror_y, v2_old, 0.0))
        new_ey = [pltpu.roll(in1, 112 - k, 1) for k in range(12)]
        for k in range(12):
            eyb[12 + k] = pltpu.roll(in2, 112 - k, 1)

        late = n - hbuf[...]
        m_idx = (late * 1311) >> 15
        fresh = late == m_idx * NB
        c_idx = jnp.clip(m_idx + 1, 0, ND + 1)
        asum, ax, ay, az, wt = [jnp.take_along_axis(ctab[pos], c_idx, axis=1) for pos in range(5)]

        base = lax.rem(n, NB) * 72
        z_face = [jnp.where(fresh, 0.0, zbuf[c]) for c in range(9)]
        pack1 = lax.rem(n, 4)
        for s in range(8):
            rows = pl.ds(base + 9 * s, 8)
            x_face = [xbuf[pl.ds(9 * (3 * s + j), 8), :] for j in range(3)]
            for i in range(3):
                k = 3 * s + i
                y_face = ybuf[k]
                for j in range(3):
                    c = 3 * i + j
                    total = ((tab[0, c, rows, :] + z_face[c]) + x_face[j]) + y_face
                    psi = total * (1.0 / (tab[1, c, rows, :] + asum))
                    x_face[j] = ax * psi - x_face[j]
                    y_face = ay * psi - y_face
                    z_face[c] = az * psi - z_face[c]
                    flux[c, rows, :] = flux[c, rows, :] + wt * psi
                if s < 4:
                    shifted = pltpu.roll(y_face, 1, 1)
                    ybuf[k] = jnp.where(first_y, new_ey[k], shifted)
                    packed = shifted if k == 0 else pltpu.roll(y_face, 1 + k, 1)
                    pltpu.store(v1ring.at[pack1], packed, mask=patch_y == k)
                else:
                    yraw[k - 12] = y_face
            for j in range(3):
                xbuf[pl.ds(9 * (3 * s + j) + 1, 8), :] = x_face[j]
            if s == 3:
                for side in range(2):
                    @pl.when(x_sends(side, n))
                    def _(side=side):
                        x_copy(side, n).start()

                @pl.when(y_sends(n))
                def _():
                    y_copy(n).start()
        for c in range(9):
            zbuf[c] = z_face[c]
        for q in range(3):
            xbuf[pl.ds(72 * q, 8, stride=9), :] = edges[q]
        return carry

    lax.fori_loop(0, STEPS, step, 0)

    for back in range(NSEND, 0, -1):
        n = STEPS - back
        for side in range(2):
            @pl.when(x_sends(side, jnp.int32(n)))
            def _(side=side, n=n):
                x_copy(side, jnp.int32(n)).wait_send()

        @pl.when(y_sends(jnp.int32(n)))
        def _(n=n):
            y_copy(jnp.int32(n)).wait_send()

    @pl.loop(0, 8)
    def _(xp):
        for i in range(3):
            for j in range(3):
                cell = 3 * i + j
                blocks = [flux[cell, pl.ds(lax.rem(v + xp, NB) * 72 + xp, 8, stride=9), :] for v in range(NB)]
                blocks = turn_blocks(blocks, -1)
                lo = jnp.concatenate(blocks[:16], axis=0).T
                hi = jnp.concatenate(blocks[16:] + [zero] * 7, axis=0).T
                parts, olds = [], []
                for octant, half, x_abs, y_abs, rev in row_groups(xp, i, j):
                    for zh in range(2):
                        part = 4 * (octant % 2) + 2 * ((octant // 2) % 2) + zh
                        row = 16 * octant + 8 * half
                        val = (lo, hi)[zh][row:row + 8]
                        if rev:
                            val = jnp.take_along_axis(val, flip_rows, axis=0)
                        where = (part, x_abs, pl.ds(y_abs, 8, stride=3))
                        olds.append(acc[where + (slice(None),)] + val)
                        parts.append(where)
                for where, val in zip(parts, olds):
                    acc[where + (slice(None),)] = val

    @pl.loop(0, NX)
    def _(x):
        for yt in range(NY // 8):
            rows = pl.ds(8 * yt, 8)
            up_a = acc[4, x, rows, :] + acc[6, x, rows, :]
            up_b = acc[5, x, rows, :] + acc[7, x, rows, :]
            dn_a = jnp.take_along_axis(acc[0, x, rows, :] + acc[2, x, rows, :], mirror, axis=1)
            dn_b = jnp.take_along_axis(acc[1, x, rows, :] + acc[3, x, rows, :], mirror, axis=1)
            out_ref[x, rows, pl.ds(0, 128)] = up_a + jnp.where(tail, dn_b, dn_a)
            out_ref[x, rows, pl.ds(128, 72)] = (up_b + dn_a)[:, :72]


def solution(mesh):
    grid_spec = P(("g", "x"), "y", None)

    def column_sweep(source, sigma_t, cos_x, cos_y, cos_z, weights):
        smem = pl.BlockSpec(memory_space=pltpu.SMEM)
        vmem = pl.BlockSpec(memory_space=pltpu.VMEM)
        return pl.pallas_call(
            kernel,
            out_shape=jax.ShapeDtypeStruct((NX, NY, NZ), F32),
            in_specs=[smem] * 4 + [vmem] * 2,
            out_specs=vmem,
            scratch_shapes=[
                pltpu.VMEM((2, 4, NX, NY, 128), F32),
                pltpu.VMEM((2, 9, ROWS, 128), F32),
                pltpu.VMEM((9, ROWS, 128), F32),
                pltpu.VMEM((8, NX, NY, 128), F32),
                pltpu.VMEM((8, 128), jnp.int32),
                pltpu.VMEM((5, 8, 128), F32),
                pltpu.VMEM((224, 128), F32),
                pltpu.VMEM((24, 8, 128), F32),
                pltpu.VMEM((12, 8, 128), F32),
                pltpu.VMEM((9, 8, 128), F32),
                pltpu.VMEM((24, 8, 128), F32),
                pltpu.VMEM((2, NSEND, 16, 128), F32),
                pltpu.VMEM((2, RING, 16, 128), F32),
                pltpu.VMEM((NSEND, 8, 128), F32),
                pltpu.VMEM((RING, 8, 128), F32),
                pltpu.VMEM((4, 8, 128), F32),
                pltpu.VMEM((4, 8, 128), F32),
                pltpu.SemaphoreType.DMA((2, NSEND)),
                pltpu.SemaphoreType.DMA((2, RING)),
                pltpu.SemaphoreType.DMA((NSEND,)),
                pltpu.SemaphoreType.DMA((RING,)),
            ],
            compiler_params=pltpu.CompilerParams(
                collective_id=0, has_side_effects=True, vmem_limit_bytes=60 * 1024 * 1024),
        )(cos_x, cos_y, cos_z, weights, source, sigma_t)

    return jax.shard_map(column_sweep, mesh=mesh, in_specs=(grid_spec, grid_spec, P(), P(), P(), P()),
                         out_specs=grid_spec, check_vma=False)
```

```python
import functools

import jax
import jax.numpy as jnp
from jax import lax
from jax.experimental import pallas as pl
from jax.experimental.pallas import tpu as pltpu
from jax.sharding import PartitionSpec as P

F32 = jnp.float32
MESH = pl.DeviceIdType.MESH
NX, NY, NZ = 24, 48, 200
ND = 10
NB = NZ // 8
ROWS = NB * 72
T_NEAR = 7
T_FAR = 14
T_Y = 14
D_XR = 1
D_YR = 2
RING = 32
NSEND = 8
SPOTS = [2, 13, 3, 4, 11, 12, 5, 10, 6, 7, 8, 9]
PARTNER = [SPOTS.index(15 - spot) for spot in SPOTS]


def x_lags():
    near, far = T_NEAR + 1, T_FAR + 1
    hops = [near, far, near, D_XR, near, far, near]
    lags = [0]
    for hop in hops:
        lags.append(lags[-1] + 8 + hop)
    return lags


def y_lags():
    lags = [0]
    for hop in [T_Y + 2, D_YR, T_Y + 2]:
        lags.append(lags[-1] + 16 + hop)
    return lags


LAG_X, LAG_Y = x_lags(), y_lags()
STEPS = ND * NB + LAG_X[-1] + LAG_Y[-1] + 7 + 15 + 1


def pick(values, idx):
    out = jnp.int32(values[0])
    for pos in range(1, len(values)):
        out = jnp.where(idx == pos, jnp.int32(values[pos]), out)
    return out


def kernel(cx_ref, cy_ref, cz_ref, wt_ref, src_ref, sig_ref, out_ref,
           nat, tab, flux, acc, hbuf, ctab, ntab, cbuf, xbuf, ybuf, yraw, zbuf, inodd, refl,
           xsend, xrecv, ysend, yrecv, pack,
           xs_sem, xr_sem, ys_sem, yr_sem):
    dx = lax.axis_index("x")
    dy = lax.axis_index("y")
    has_left, has_right = dx > 0, dx < 3
    odd_x = (dx & 1) == 1
    trip_left = jnp.where(odd_x, T_NEAR, T_FAR)
    trip_right = jnp.where(odd_x, T_FAR, T_NEAR)
    lane = lax.broadcasted_iota(jnp.int32, (8, 128), 1)
    subl = lax.broadcasted_iota(jnp.int32, (8, 128), 0)
    oct_id = lane // 16
    oct_y = (oct_id // 2) % 2
    patch_y = lane - 16 * oct_id
    zero = jnp.zeros((8, 128), F32)
    low_half = lane < 64
    first_y = patch_y == 0

    lag_xm, lag_xp = pick(LAG_X[:4][::-1], dx), pick(LAG_X[4:], dx)
    lag_ym, lag_yp = pick(LAG_Y[:2][::-1], dy), pick(LAG_Y[2:], dy)
    lag_oct = jnp.where(lane >= 64, lag_xp, lag_xm) + jnp.where(oct_y == 1, lag_yp, lag_ym)
    lag_lane = patch_y + lag_oct
    hbuf[...] = lax.rem(lag_lane + subl, NB)
    turn = lax.rem(lag_lane, NB)
    turn_bits = [(turn >> bit) & 1 == 1 for bit in range(5)]

    for pos in range(5):
        col = jnp.ones((8, 128), F32) if pos == 0 else zero
        for m in range(ND):
            two_x, two_y, two_z = 2.0 * cx_ref[m], 2.0 * cy_ref[m], 2.0 * cz_ref[m]
            val = (two_x + two_y + two_z, 2.0 * two_x, 2.0 * two_y, 2.0 * two_z, wt_ref[m])[pos]
            col = jnp.where(lane == m + 1, val, col)
        ctab[pos] = col
        cbuf[pos] = jnp.ones((8, 128), F32) if pos == 0 else zero

    @pl.loop(0, ntab.shape[1] // 8)
    def _(k):
        late = 8 * k + subl - lag_oct
        c_idx = jnp.clip(((late * 1311) >> 15) + 1, 0, ND + 1)
        for pos in range(5):
            ntab[pos, pl.ds(8 * k, 8), :] = jnp.take_along_axis(ctab[pos], c_idx, axis=1)

    for k in range(28):
        xbuf[pl.ds(8 * k, 8), :] = zero
    for k in range(24):
        ybuf[k] = zero
    for k in range(12):
        yraw[k] = zero
    for k in range(9):
        zbuf[k] = zero
    inodd[...] = zero
    refl[...] = zero
    for k in range(4):
        pack[k, 0] = zero
        pack[k, 1] = zero

    @pl.loop(0, RING)
    def _(k):
        for side in range(2):
            for q in range(3):
                xrecv[side, k, pl.ds(8 * q, 8), :] = zero
        yrecv[k] = zero

    barrier = pltpu.get_barrier_semaphore()

    @pl.when(has_left)
    def _():
        pl.semaphore_signal(barrier, inc=1, device_id={"x": dx - 1}, device_id_type=MESH)

    @pl.when(has_right)
    def _():
        pl.semaphore_signal(barrier, inc=1, device_id={"x": dx + 1}, device_id_type=MESH)

    pl.semaphore_signal(barrier, inc=1, device_id={"y": 1 - dy}, device_id_type=MESH)

    mirror = (71 - lane) & 127
    tail = lane < 72

    @pl.loop(0, NX)
    def _(x):
        for arr, ref in enumerate((src_ref, sig_ref)):
            for yt in range(NY // 8):
                rows = pl.ds(8 * yt, 8)
                half_a = ref[x, rows, pl.ds(0, 128)]
                nat[arr, 0, x, rows, :] = half_a
                nat[arr, 1, x, rows, pl.ds(0, 72)] = ref[x, rows, pl.ds(128, 72)]
                half_b = nat[arr, 1, x, rows, :]
                flip_a = jnp.take_along_axis(half_a, mirror, axis=1)
                flip_b = jnp.take_along_axis(half_b, mirror, axis=1)
                nat[arr, 2, x, rows, :] = jnp.where(tail, flip_b, flip_a)
                nat[arr, 3, x, rows, :] = flip_a
        for part in range(8):
            for yt in range(NY // 8):
                acc[part, x, pl.ds(8 * yt, 8), :] = zero

    flip_rows = 7 - subl

    def row_groups(x_patch, i, j):
        for octant in range(8):
            bx, by = octant // 4, (octant // 2) % 2
            x_rel = 3 * x_patch + i
            x_abs = x_rel if bx else NX - 1 - x_rel
            for half in range(2):
                y_abs = (24 * half + j) if by else (26 - 24 * half - j)
                yield octant, half, x_abs, y_abs, by == 0

    def turn_blocks(blocks, step):
        for bit in range(5):
            shift = step * (1 << bit)
            blocks = [jnp.where(turn_bits[bit], blocks[(v - shift) % NB], blocks[v]) for v in range(NB)]
        return blocks

    @pl.loop(0, 8)
    def _(xp):
        for i in range(3):
            for j in range(3):
                cell = 3 * i + j
                for arr in range(2):
                    pieces = [[], []]
                    for octant, half, x_abs, y_abs, rev in row_groups(xp, i, j):
                        for zh in range(2):
                            kind = zh + (0 if octant % 2 else 2)
                            val = nat[arr, kind, x_abs, pl.ds(y_abs, 8, stride=3), :]
                            if rev:
                                val = jnp.take_along_axis(val, flip_rows, axis=0)
                            pieces[zh].append(val)
                    lo = jnp.concatenate(pieces[0], axis=0).T
                    hi = jnp.concatenate(pieces[1], axis=0).T
                    blocks = [lo[8 * v:8 * v + 8] for v in range(16)] + [hi[8 * v:8 * v + 8] for v in range(9)]
                    blocks = turn_blocks(blocks, 1)
                    for v in range(NB):
                        start = lax.rem(v + xp, NB) * 72 + xp
                        tab[arr, cell, pl.ds(start, 8, stride=9), :] = blocks[v]
                        if arr == 0:
                            flux[cell, pl.ds(start, 8, stride=9), :] = zero

    pl.semaphore_wait(barrier, has_left.astype(jnp.int32) + has_right.astype(jnp.int32) + 1)

    keep_send = oct_y == 1 - dy
    even_mask, odd_mask = oct_y == dy, oct_y == 1 - dy
    mirror_x, mirror_y = dx == 0, dy == 0
    has = (has_left, has_right, True)
    trips = (trip_left, trip_right, T_Y)

    def copy(kind, n):
        slot, here = (n + trips[kind]) & (RING - 1), n & (NSEND - 1)
        if kind == 2:
            return pltpu.make_async_remote_copy(
                src_ref=ysend.at[here], dst_ref=yrecv.at[slot], send_sem=ys_sem.at[here], recv_sem=yr_sem.at[slot],
                device_id={"y": 1 - dy}, device_id_type=MESH)
        return pltpu.make_async_remote_copy(
            src_ref=xsend.at[here], dst_ref=xrecv.at[kind, slot],
            send_sem=xs_sem.at[kind, here], recv_sem=xr_sem.at[kind, slot],
            device_id={"x": dx - 1 if kind == 0 else dx + 1}, device_id_type=MESH)

    def arrival(kind, n):
        slot = n & (RING - 1)
        if kind == 2:
            return pltpu.make_async_remote_copy(
                src_ref=ysend.at[0], dst_ref=yrecv.at[slot], send_sem=ys_sem.at[0], recv_sem=yr_sem.at[slot],
                device_id={"y": dy}, device_id_type=MESH)
        return pltpu.make_async_remote_copy(
            src_ref=xsend.at[0], dst_ref=xrecv.at[kind, slot], send_sem=xs_sem.at[kind, 0],
            recv_sem=xr_sem.at[kind, slot], device_id={"x": dx}, device_id_type=MESH)

    def when(cond, act):
        if cond is True:
            act()
        else:
            pl.when(cond)(act)

    def both(one, two):
        return two if one is True else (one if two is True else one & two)

    def sends(kind, n, full):
        if not full:
            return has[kind]
        return both(has[kind], (n >= 2) & (n + trips[kind] <= STEPS - 2))

    def waits(kind, n, full):
        if not full:
            return (has_right, has_left, True)[kind]
        trip = (trip_right, trip_left, T_Y)[kind]
        return both((has_right, has_left, True)[kind], (n >= trip + 2) & (n <= STEPS - 2))

    def step(n, base, full):
        here = n & (NSEND - 1)
        slot = n & (RING - 1)
        now, last, before = n & 3, (n + 3) & 3, (n + 2) & 3

        outs = [xbuf[pl.ds(72 * q + 8, 8, stride=9), :] for q in range(3)]
        pack_even, pack_odd = pack[before, 0], pack[before, 1]
        for kind in range(3):
            when(sends(kind, n - NSEND, full), lambda kind=kind: copy(kind, n - NSEND).wait_send())
        for q in range(3):
            xsend[here, pl.ds(8 * q, 8), :] = outs[q]
        ysend[here] = jnp.where(keep_send, pack_even, pack_odd)
        for kind in range(3):
            when(sends(kind, n, full), lambda kind=kind: copy(kind, n).start())
        for kind in range(3):
            when(waits(kind, n, full), lambda kind=kind: arrival(kind, n).wait_recv())

        edges = []
        for q in range(3):
            rows = pl.ds(8 * q, 8)
            from_left = jnp.where(mirror_x, pltpu.roll(outs[q], 64, 1), xrecv[1, slot, rows, :])
            edges.append(jnp.where(low_half, xrecv[0, slot, rows, :], from_left))
        got = yrecv[slot]
        in_even = jnp.where(even_mask, got, refl[...])
        in_odd = inodd[...]
        refl[...] = jnp.where(mirror_y, pltpu.roll(pack[last, 0], 32, 1), 0.0)
        inodd[...] = jnp.where(odd_mask, pltpu.roll(got, 64, 1),
                               jnp.where(mirror_y, pltpu.roll(pack_odd, 96, 1), 0.0))

        mains, mixes = {}, {}

        def serve(level, faces, odd):
            for i in range(3):
                f = 3 * (level % 4) + i
                spot = SPOTS[f]
                mains[f] = pltpu.roll(faces[i], 1, 1)
                mixed = jnp.where(patch_y == 15 - spot, in_odd if odd else in_even, faces[i])
                mixes[PARTNER[f]] = pltpu.roll(mixed, (1 + spot + (16 if odd else 112)) % 128, 1)
                pltpu.store(pack.at[last if odd else now, 1 if odd else 0], mixes[PARTNER[f]], mask=patch_y == spot)
            for f in [f for f in mains if f in mixes]:
                ybuf[f + (12 if odd else 0)] = jnp.where(first_y, mixes.pop(f), mains.pop(f))

        for level in range(4):
            serve(level, [yraw[3 * level + i] for i in range(3)], True)

        fresh = hbuf[...] == lax.div(base, 72)
        coef = []
        for pos in range(5):
            coef.append(jnp.where(fresh, ntab[pos, pl.ds(n, 1), :], cbuf[pos]))
            cbuf[pos] = coef[pos]
        asum, ax, ay, az, wt = coef
        z_face = [jnp.where(fresh, 0.0, zbuf[c]) for c in range(9)]

        for s in range(8):
            rows = pl.ds(base + 9 * s, 8)
            x_face = [xbuf[pl.ds(9 * (3 * s + j), 8), :] for j in range(3)]
            y_out = []
            for i in range(3):
                y_face = ybuf[3 * s + i]
                for j in range(3):
                    c = 3 * i + j
                    total = ((tab[0, c, rows, :] + z_face[c]) + x_face[j]) + y_face
                    psi = total * (1.0 / (tab[1, c, rows, :] + asum))
                    x_face[j] = ax * psi - x_face[j]
                    y_face = ay * psi - y_face
                    z_face[c] = az * psi - z_face[c]
                    flux[c, rows, :] = flux[c, rows, :] + wt * psi
                y_out.append(y_face)
            if s < 4:
                serve(s, y_out, False)
            else:
                for i in range(3):
                    yraw[3 * (s - 4) + i] = y_out[i]
            for j in range(3):
                xbuf[pl.ds(9 * (3 * s + j) + 1, 8), :] = x_face[j]
        for c in range(9):
            zbuf[c] = z_face[c]
        for q in range(3):
            xbuf[pl.ds(72 * q, 8, stride=9), :] = edges[q]
        return jnp.where(base == 72 * (NB - 1), 0, base + 72)

    ramp = max(T_FAR, T_Y) + 2 + NSEND
    base = lax.fori_loop(0, ramp, functools.partial(step, full=True), jnp.int32(0))
    base = lax.fori_loop(ramp, STEPS - ramp, functools.partial(step, full=False), base)
    lax.fori_loop(STEPS - ramp, STEPS, functools.partial(step, full=True), base)
    for back in range(NSEND, 0, -1):
        for kind in range(3):
            n = jnp.int32(STEPS - back)
            when(sends(kind, n, True), lambda kind=kind, n=n: copy(kind, n).wait_send())

    @pl.loop(0, 8)
    def _(xp):
        for i in range(3):
            for j in range(3):
                cell = 3 * i + j
                blocks = [flux[cell, pl.ds(lax.rem(v + xp, NB) * 72 + xp, 8, stride=9), :] for v in range(NB)]
                blocks = turn_blocks(blocks, -1)
                lo = jnp.concatenate(blocks[:16], axis=0).T
                hi = jnp.concatenate(blocks[16:] + [zero] * 7, axis=0).T
                parts, olds = [], []
                for octant, half, x_abs, y_abs, rev in row_groups(xp, i, j):
                    for zh in range(2):
                        part = 4 * (octant % 2) + 2 * ((octant // 2) % 2) + zh
                        row = 16 * octant + 8 * half
                        val = (lo, hi)[zh][row:row + 8]
                        if rev:
                            val = jnp.take_along_axis(val, flip_rows, axis=0)
                        where = (part, x_abs, pl.ds(y_abs, 8, stride=3))
                        olds.append(acc[where + (slice(None),)] + val)
                        parts.append(where)
                for where, val in zip(parts, olds):
                    acc[where + (slice(None),)] = val

    @pl.loop(0, NX)
    def _(x):
        for yt in range(NY // 8):
            rows = pl.ds(8 * yt, 8)
            up_a = acc[4, x, rows, :] + acc[6, x, rows, :]
            up_b = acc[5, x, rows, :] + acc[7, x, rows, :]
            dn_a = jnp.take_along_axis(acc[0, x, rows, :] + acc[2, x, rows, :], mirror, axis=1)
            dn_b = jnp.take_along_axis(acc[1, x, rows, :] + acc[3, x, rows, :], mirror, axis=1)
            out_ref[x, rows, pl.ds(0, 128)] = up_a + jnp.where(tail, dn_b, dn_a)
            out_ref[x, rows, pl.ds(128, 72)] = (up_b + dn_a)[:, :72]


def solution(mesh):
    grid_spec = P(("g", "x"), "y", None)

    def column_sweep(source, sigma_t, cos_x, cos_y, cos_z, weights):
        smem = pl.BlockSpec(memory_space=pltpu.SMEM)
        vmem = pl.BlockSpec(memory_space=pltpu.VMEM)
        return pl.pallas_call(
            kernel,
            out_shape=jax.ShapeDtypeStruct((NX, NY, NZ), F32),
            in_specs=[smem] * 4 + [vmem] * 2,
            out_specs=vmem,
            scratch_shapes=[
                pltpu.VMEM((2, 4, NX, NY, 128), F32),
                pltpu.VMEM((2, 9, ROWS, 128), F32),
                pltpu.VMEM((9, ROWS, 128), F32),
                pltpu.VMEM((8, NX, NY, 128), F32),
                pltpu.VMEM((8, 128), jnp.int32),
                pltpu.VMEM((5, 8, 128), F32),
                pltpu.VMEM((5, 8 * pl.cdiv(STEPS, 8), 128), F32),
                pltpu.VMEM((5, 8, 128), F32),
                pltpu.VMEM((224, 128), F32),
                pltpu.VMEM((24, 8, 128), F32),
                pltpu.VMEM((12, 8, 128), F32),
                pltpu.VMEM((9, 8, 128), F32),
                pltpu.VMEM((8, 128), F32),
                pltpu.VMEM((8, 128), F32),
                pltpu.VMEM((NSEND, 24, 128), F32),
                pltpu.VMEM((2, RING, 24, 128), F32),
                pltpu.VMEM((NSEND, 8, 128), F32),
                pltpu.VMEM((RING, 8, 128), F32),
                pltpu.VMEM((4, 2, 8, 128), F32),
                pltpu.SemaphoreType.DMA((2, NSEND)),
                pltpu.SemaphoreType.DMA((2, RING)),
                pltpu.SemaphoreType.DMA((NSEND,)),
                pltpu.SemaphoreType.DMA((RING,)),
            ],
            compiler_params=pltpu.CompilerParams(
                collective_id=0, has_side_effects=True, vmem_limit_bytes=60 * 1024 * 1024),
        )(cos_x, cos_y, cos_z, weights, source, sigma_t)

    return jax.shard_map(column_sweep, mesh=mesh, in_specs=(grid_spec, grid_spec, P(), P(), P(), P()),
                         out_specs=grid_spec, check_vma=False)
```

```python
import functools

import jax
import jax.numpy as jnp
from jax import lax
from jax.experimental import pallas as pl
from jax.experimental.pallas import tpu as pltpu
from jax.sharding import PartitionSpec as P

F32 = jnp.float32
MESH = pl.DeviceIdType.MESH
NX, NY, NZ = 24, 48, 200
ND = 10
NB = NZ // 8
LEVEL = 12
FRONT = 4 * LEVEL
PITCH = 8 * LEVEL
ROWS = NB * PITCH + 104
T_NEAR = 3
T_FAR = 7
T_Y = 7
D_XR = 2
D_YR = 5
RING = 16
NSEND = 16
HOIST = 64
SPOTS = [2, 13, 3, 4, 11, 12, 5, 10, 6, 7, 8, 9]
PARTNER = [SPOTS.index(15 - spot) for spot in SPOTS]


def x_lags():
    near, far = 2 * T_NEAR + 2, 2 * T_FAR + 2
    hops = [near, far, near, D_XR, near, far, near]
    lags = [0]
    for hop in hops:
        lags.append(lags[-1] + 4 + hop)
    return lags


def y_lags():
    lags = [0]
    for hop in [2 * T_Y + 3, D_YR, 2 * T_Y + 3]:
        lags.append(lags[-1] + 16 + hop)
    return lags


LAG_X, LAG_Y = x_lags(), y_lags()
STEPS = ND * NB + LAG_X[-1] + LAG_Y[-1] + 4 + 15 + 1
BLOCKS = (STEPS + 1) // 2


def pick(values, idx):
    out = jnp.int32(values[0])
    for pos in range(1, len(values)):
        out = jnp.where(idx == pos, jnp.int32(values[pos]), out)
    return out


def kernel(cx_ref, cy_ref, cz_ref, wt_ref, src_ref, sig_ref, out_ref,
           nat, tab, acc, hbuf, ctab, ntab, cbuf, xbuf, ybuf, yraw, zbuf, inodd, refl,
           xsend, xrecv, ysend, yrecv, pack,
           xs_sem, xr_sem, ys_sem, yr_sem):
    dx = lax.axis_index("x")
    dy = lax.axis_index("y")
    has_left, has_right = dx > 0, dx < 3
    odd_x = (dx & 1) == 1
    trip_left = jnp.where(odd_x, T_NEAR, T_FAR)
    trip_right = jnp.where(odd_x, T_FAR, T_NEAR)
    lane = lax.broadcasted_iota(jnp.int32, (8, 128), 1)
    subl = lax.broadcasted_iota(jnp.int32, (8, 128), 0)
    oct_id = lane // 16
    oct_y = (oct_id // 2) % 2
    patch_y = lane - 16 * oct_id
    zero = jnp.zeros((8, 128), F32)
    low_half = lane < 64
    first_y = patch_y == 0

    lag_xm, lag_xp = pick(LAG_X[:4][::-1], dx), pick(LAG_X[4:], dx)
    lag_ym, lag_yp = pick(LAG_Y[:2][::-1], dy), pick(LAG_Y[2:], dy)
    lag_oct = jnp.where(lane >= 64, lag_xp, lag_xm) + jnp.where(oct_y == 1, lag_yp, lag_ym)
    lag_lane = patch_y + lag_oct
    hbuf[...] = lax.rem(2 * lag_lane + subl, 2 * NB)
    turn = lax.rem(lag_lane, NB)
    turn_bits = [(turn >> bit) & 1 == 1 for bit in range(5)]

    for pos in range(5):
        col = jnp.ones((8, 128), F32) if pos == 0 else zero
        for m in range(ND):
            two_x, two_y, two_z = 2.0 * cx_ref[m], 2.0 * cy_ref[m], 2.0 * cz_ref[m]
            val = (two_x + two_y + two_z, 2.0 * two_x, 2.0 * two_y, 2.0 * two_z, wt_ref[m])[pos]
            col = jnp.where(lane == m + 1, val, col)
        ctab[pos] = col
        cbuf[pos] = jnp.ones((8, 128), F32) if pos == 0 else zero

    cols = [ctab[pos] for pos in range(5)]

    @pl.loop(0, ntab.shape[1] // 64)
    def _(k):
        for part in range(8):
            first = 64 * k + 8 * part
            c_idx = jnp.clip((((first + subl - lag_oct) * 1311) >> 15) + 1, 0, ND + 1)
            for pos in range(5):
                ntab[pos, pl.ds(first, 8), :] = jnp.take_along_axis(cols[pos], c_idx, axis=1)

    for k in range(55):
        xbuf[pl.ds(8 * k, 8), :] = zero
    for k in range(48):
        ybuf[k] = zero
    for k in range(12):
        yraw[k] = zero
    for k in range(9):
        zbuf[k] = zero
    inodd[...] = zero
    for k in range(4):
        refl[k] = zero
        for j in range(4):
            pack[k, j] = zero

    @pl.loop(0, RING)
    def _(k):
        for side in range(2):
            for q in range(6):
                xrecv[side, k, pl.ds(8 * q, 8), :] = zero
        for r in range(2):
            yrecv[k, r] = zero

    barrier = pltpu.get_barrier_semaphore()

    @pl.when(has_left)
    def _():
        pl.semaphore_signal(barrier, inc=1, device_id={"x": dx - 1}, device_id_type=MESH)

    @pl.when(has_right)
    def _():
        pl.semaphore_signal(barrier, inc=1, device_id={"x": dx + 1}, device_id_type=MESH)

    pl.semaphore_signal(barrier, inc=1, device_id={"y": 1 - dy}, device_id_type=MESH)

    mirror = (71 - lane) & 127
    tail = lane < 72

    @pl.loop(0, NX)
    def _(x):
        for arr, ref in enumerate((src_ref, sig_ref)):
            for yt in range(NY // 8):
                rows = pl.ds(8 * yt, 8)
                half_a = ref[x, rows, pl.ds(0, 128)]
                nat[arr, 0, x, rows, :] = half_a
                nat[arr, 1, x, rows, pl.ds(0, 72)] = ref[x, rows, pl.ds(128, 72)]
                half_b = nat[arr, 1, x, rows, :]
                flip_a = jnp.take_along_axis(half_a, mirror, axis=1)
                flip_b = jnp.take_along_axis(half_b, mirror, axis=1)
                nat[arr, 2, x, rows, :] = jnp.where(tail, flip_b, flip_a)
                nat[arr, 3, x, rows, :] = flip_a
        for part in range(8):
            for yt in range(NY // 8):
                acc[part, x, pl.ds(8 * yt, 8), :] = zero

    flip_rows = 7 - subl

    def row_groups(x_patch, i, j):
        for octant in range(8):
            bx, by = octant // 4, (octant // 2) % 2
            x_rel = 3 * x_patch + i
            x_abs = x_rel if bx else NX - 1 - x_rel
            for half in range(2):
                y_abs = (24 * half + j) if by else (26 - 24 * half - j)
                yield octant, half, x_abs, y_abs, by == 0

    def turn_blocks(blocks, step):
        for bit in range(5):
            shift = step * (1 << bit)
            blocks = [jnp.where(turn_bits[bit], blocks[(v - shift) % NB], blocks[v]) for v in range(NB)]
        return blocks

    odd_patch = (subl & 1) == 1

    def block_rows(v, half, odd):
        return pl.ds(FRONT + lax.rem(v + half, NB) * PITCH + (2 * half + odd) + 4 * LEVEL * odd, 8, stride=LEVEL)

    @pl.loop(0, 12)
    def _(trip):
        i, half = trip // 4, trip & 3
        for odd in range(2):
            for j in range(3):
                cell = 3 * i + j
                for arr in range(2):
                    pieces = [[], []]
                    for octant, part, x_abs, y_abs, rev in row_groups(2 * half + odd, i, j):
                        for zh in range(2):
                            kind = zh + (0 if octant % 2 else 2)
                            val = nat[arr, kind, x_abs, pl.ds(y_abs, 8, stride=3), :]
                            if rev:
                                val = jnp.take_along_axis(val, flip_rows, axis=0)
                            pieces[zh].append(val)
                    lo = jnp.concatenate(pieces[0], axis=0).T
                    hi = jnp.concatenate(pieces[1], axis=0).T
                    blocks = [lo[8 * v:8 * v + 8] for v in range(16)] + [hi[8 * v:8 * v + 8] for v in range(9)]
                    blocks = turn_blocks(blocks, 1)
                    for v in range(NB):
                        tab[arr, cell, block_rows(v, half, odd), :] = blocks[v]
                        if arr == 0:
                            tab[2, cell, block_rows(v, half, odd), :] = zero

    @pl.loop(0, 9)
    def _(cell):
        for arr in range(2):
            for k in range(4):
                first, wrapped = pl.ds(FRONT + LEVEL * k, 8), pl.ds(FRONT + NB * PITCH + LEVEL * k, 8)
                tab[arr, cell, first, :] = jnp.where(odd_patch, tab[arr, cell, wrapped, :], tab[arr, cell, first, :])
        for k in range(4):
            tab[2, cell, pl.ds(FRONT + LEVEL * k, 8), :] = zero

    pl.semaphore_wait(barrier, has_left.astype(jnp.int32) + has_right.astype(jnp.int32) + 1)

    keep_send = oct_y == 1 - dy
    even_mask, odd_mask = oct_y == dy, oct_y == 1 - dy
    mirror_x, mirror_y = dx == 0, dy == 0
    has = (has_left, has_right, True)
    trips = (trip_left, trip_right, T_Y)

    def copy(kind, n, count=1):
        slot, here, batch = (n + trips[kind]) & (RING - 1), n & (NSEND - 1), (n // 8) & 1
        if count > 1:
            here, slot = pl.ds(8 * batch, count), pl.ds(0, count)
        if kind == 2:
            return pltpu.make_async_remote_copy(
                src_ref=ysend.at[here], dst_ref=yrecv.at[slot], send_sem=ys_sem.at[batch],
                recv_sem=yr_sem.at[0 if count > 1 else slot], device_id={"y": 1 - dy}, device_id_type=MESH)
        return pltpu.make_async_remote_copy(
            src_ref=xsend.at[here], dst_ref=xrecv.at[kind, slot], send_sem=xs_sem.at[kind, batch],
            recv_sem=xr_sem.at[kind, 0 if count > 1 else slot],
            device_id={"x": dx - 1 if kind == 0 else dx + 1}, device_id_type=MESH)

    def arrival(kind, n):
        slot = n & (RING - 1)
        if kind == 2:
            return pltpu.make_async_remote_copy(
                src_ref=ysend.at[0], dst_ref=yrecv.at[slot], send_sem=ys_sem.at[0], recv_sem=yr_sem.at[slot],
                device_id={"y": dy}, device_id_type=MESH)
        return pltpu.make_async_remote_copy(
            src_ref=xsend.at[0], dst_ref=xrecv.at[kind, slot], send_sem=xs_sem.at[kind, 0],
            recv_sem=xr_sem.at[kind, slot], device_id={"x": dx}, device_id_type=MESH)

    def when(cond, act):
        if cond is True:
            act()
        else:
            pl.when(cond)(act)

    def both(one, two):
        return two if one is True else (one if two is True else one & two)

    def next_turn(turn_now):
        return jnp.where(turn_now == NB - 1, 0, turn_now + 1)

    senders = (has_right, has_left, True)
    delays = (trip_right, trip_left, T_Y)

    def block(n, turn_now):
        here = n & (NSEND - 1)
        slot = n & (RING - 1)
        now, last, before = n & 3, (n + 3) & 3, (n + 2) & 3

        outs = [xbuf[pl.ds(72 * q + 8, 8, stride=9), :] for q in range(6)]
        packs = [pack[before, 2], pack[before, 3], pack[last, 0], pack[last, 1]]
        for q in range(6):
            xsend[here, pl.ds(8 * q, 8), :] = outs[q]
        for r in range(2):
            ysend[here, r] = jnp.where(keep_send, packs[2 * r], packs[2 * r + 1])
        for kind in range(3):
            when(has[kind], lambda kind=kind: copy(kind, n).start())
        for kind in range(3):
            when(both(senders[kind], n >= delays[kind]), lambda kind=kind: arrival(kind, n).wait_recv())
        batch_end = ((n & 7) == 7) & (n >= 15)
        for kind in range(3):
            when(both(has[kind], batch_end), lambda kind=kind: copy(kind, n - 15, 8).wait_send())

        edges = []
        for q in range(6):
            rows = pl.ds(8 * q, 8)
            from_left = jnp.where(mirror_x, pltpu.roll(outs[q], 64, 1), xrecv[1, slot, rows, :])
            edges.append(jnp.where(low_half, xrecv[0, slot, rows, :], from_left))
        got = [yrecv[slot, r] for r in range(2)]
        incoming = [jnp.where(even_mask, got[0], refl[0]), jnp.where(odd_mask, pltpu.roll(got[0], 64, 1), refl[1]),
                    jnp.where(even_mask, got[1], refl[2]), inodd[...]]
        inodd[...] = jnp.where(odd_mask, pltpu.roll(got[1], 64, 1), refl[3])
        for k in range(4):
            refl[k] = jnp.where(mirror_y, pltpu.roll(packs[k], 96 if k % 2 else 32, 1), 0.0)

        mains, mixes = {}, {}

        def serve(s, faces):
            group = s // 4
            for i in range(3):
                f = 3 * (s % 4) + i
                spot = SPOTS[f]
                mains[f] = pltpu.roll(faces[i], 1, 1)
                mixed = jnp.where(patch_y == 15 - spot, incoming[group], faces[i])
                mixes[PARTNER[f]] = pltpu.roll(mixed, (1 + spot + (16 if group % 2 else 112)) % 128, 1)
                pltpu.store(pack.at[last if group == 3 else now, group], mixes[PARTNER[f]], mask=patch_y == spot)
            for f in [f for f in mains if f in mixes]:
                ybuf[(12 * group + f + 24) % 48] = jnp.where(first_y, mixes.pop(f), mains.pop(f))

        for s in range(12, 16):
            serve(s, [yraw[3 * (s - 12) + i] for i in range(3)])

        turns = [turn_now, next_turn(turn_now)]
        z_face = [zbuf[c] for c in range(9)]
        coef = [cbuf[pos] for pos in range(5)]
        for s in range(16):
            if s % 4 == 0:
                fresh = hbuf[...] == 2 * turns[s // 8] + (s // 4) % 2
                row = pl.ds(2 * n + s // 8, 1)
                coef = [jnp.where(fresh, ntab[pos, row, :], coef[pos]) for pos in range(5)]
                asum, ax, ay, az, wt = coef
                z_face = [jnp.where(fresh, 0.0, z_face[c]) for c in range(9)]
            if s == 4:
                for q in range(6):
                    xbuf[pl.ds(72 * q, 8, stride=9), :] = edges[q]
            rows = pl.ds(turns[s // 8] * PITCH + (FRONT + LEVEL * (s % 8)), 8)
            x_face = [xbuf[pl.ds(9 * (3 * s + j), 8), :] for j in range(3)]
            y_out = []
            for i in range(3):
                y_face = ybuf[3 * s + i]
                for j in range(3):
                    c = 3 * i + j
                    total = ((tab[0, c, rows, :] + z_face[c]) + x_face[j]) + y_face
                    psi = total * (1.0 / (tab[1, c, rows, :] + asum))
                    x_face[j] = ax * psi - x_face[j]
                    y_face = ay * psi - y_face
                    z_face[c] = az * psi - z_face[c]
                    tab[2, c, rows, :] = tab[2, c, rows, :] + wt * psi
                y_out.append(y_face)
            if s < 12:
                serve(s, y_out)
            else:
                for i in range(3):
                    yraw[3 * (s - 12) + i] = y_out[i]
            for j in range(3):
                xbuf[pl.ds(9 * ((3 * s + j + 12) % 48) + 1, 8), :] = x_face[j]
        for c in range(9):
            zbuf[c] = z_face[c]
        for pos in range(5):
            cbuf[pos] = coef[pos]
        return next_turn(turns[1])

    lax.fori_loop(0, BLOCKS, block, jnp.int32(0))

    @pl.loop(0, 9)
    def _(cell):
        for k in range(4):
            tab[2, cell, pl.ds(FRONT + NB * PITCH + LEVEL * k, 8), :] = tab[2, cell, pl.ds(FRONT + LEVEL * k, 8), :]

    @pl.loop(0, 12)
    def _(trip):
        i, half = trip // 4, trip & 3
        for odd in range(2):
            for j in range(3):
                cell = 3 * i + j
                blocks = turn_blocks([tab[2, cell, block_rows(v, half, odd), :] for v in range(NB)], -1)
                lo = jnp.concatenate(blocks[:16], axis=0).T
                hi = jnp.concatenate(blocks[16:] + [zero] * 7, axis=0).T
                parts, olds = [], []
                for octant, side, x_abs, y_abs, rev in row_groups(2 * half + odd, i, j):
                    for zh in range(2):
                        part = 4 * (octant % 2) + 2 * ((octant // 2) % 2) + zh
                        row = 16 * octant + 8 * side
                        val = (lo, hi)[zh][row:row + 8]
                        if rev:
                            val = jnp.take_along_axis(val, flip_rows, axis=0)
                        where = (part, x_abs, pl.ds(y_abs, 8, stride=3))
                        olds.append(acc[where + (slice(None),)] + val)
                        parts.append(where)
                for where, val in zip(parts, olds):
                    acc[where + (slice(None),)] = val

    @pl.loop(0, NX)
    def _(x):
        for yt in range(NY // 8):
            rows = pl.ds(8 * yt, 8)
            up_a = acc[4, x, rows, :] + acc[6, x, rows, :]
            up_b = acc[5, x, rows, :] + acc[7, x, rows, :]
            dn_a = jnp.take_along_axis(acc[0, x, rows, :] + acc[2, x, rows, :], mirror, axis=1)
            dn_b = jnp.take_along_axis(acc[1, x, rows, :] + acc[3, x, rows, :], mirror, axis=1)
            out_ref[x, rows, pl.ds(0, 128)] = up_a + jnp.where(tail, dn_b, dn_a)
            out_ref[x, rows, pl.ds(128, 72)] = (up_b + dn_a)[:, :72]

    for kind in range(3):
        for first in range(8 * ((BLOCKS - 8) // 8), BLOCKS, 8):
            when(has[kind], lambda kind=kind, first=first:
                 copy(kind, jnp.int32(first), min(8, BLOCKS - first)).wait_send())
        for late in range(max(T_NEAR, T_FAR) if kind < 2 else T_Y):
            when(both(senders[kind], late < delays[kind]), lambda kind=kind, late=late:
                 arrival(kind, jnp.int32(BLOCKS + late)).wait_recv())


def solution(mesh):
    grid_spec = P(("g", "x"), "y", None)

    def column_sweep(source, sigma_t, cos_x, cos_y, cos_z, weights):
        smem = pl.BlockSpec(memory_space=pltpu.SMEM)
        vmem = pl.BlockSpec(memory_space=pltpu.VMEM)
        return pl.pallas_call(
            kernel,
            out_shape=pltpu.VMEM((NX, NY, NZ), F32),
            in_specs=[smem] * 4 + [vmem] * 2,
            out_specs=vmem,
            scratch_shapes=[
                pltpu.VMEM((2, 4, NX, NY, 128), F32),
                pltpu.VMEM((3, 9, ROWS, 128), F32),
                pltpu.VMEM((8, NX, NY, 128), F32),
                pltpu.VMEM((8, 128), jnp.int32),
                pltpu.VMEM((5, 8, 128), F32),
                pltpu.VMEM((5, 64 * pl.cdiv(2 * BLOCKS, 64), 128), F32),
                pltpu.VMEM((5, 8, 128), F32),
                pltpu.VMEM((440, 128), F32),
                pltpu.VMEM((48, 8, 128), F32),
                pltpu.VMEM((12, 8, 128), F32),
                pltpu.VMEM((9, 8, 128), F32),
                pltpu.VMEM((8, 128), F32),
                pltpu.VMEM((4, 8, 128), F32),
                pltpu.VMEM((NSEND, 48, 128), F32),
                pltpu.VMEM((2, RING, 48, 128), F32),
                pltpu.VMEM((NSEND, 2, 8, 128), F32),
                pltpu.VMEM((RING, 2, 8, 128), F32),
                pltpu.VMEM((4, 4, 8, 128), F32),
                pltpu.SemaphoreType.DMA((2, 2)),
                pltpu.SemaphoreType.DMA((2, RING)),
                pltpu.SemaphoreType.DMA((2,)),
                pltpu.SemaphoreType.DMA((RING,)),
            ],
            compiler_params=pltpu.CompilerParams(
                collective_id=0, has_side_effects=True, vmem_limit_bytes=60 * 1024 * 1024),
        )(cos_x, cos_y, cos_z, weights, source, sigma_t)

    return jax.shard_map(column_sweep, mesh=mesh, in_specs=(grid_spec, grid_spec, P(), P(), P(), P()),
                         out_specs=grid_spec, check_vma=False)
```

```python
import functools

import jax
import jax.numpy as jnp
from jax import lax
from jax.experimental import pallas as pl
from jax.experimental.pallas import tpu as pltpu
from jax.sharding import PartitionSpec as P

F32 = jnp.float32
MESH = pl.DeviceIdType.MESH
NX, NY, NZ = 24, 48, 200
ND = 10
NB = NZ // 8
LEVEL = 12
FRONT = 4 * LEVEL
PITCH = 8 * LEVEL
ROWS = NB * PITCH + 104
T_NEAR = 3
T_FAR = 7
T_Y = 8
D_XR = 2
D_YR = 5
RING = 16
RING_Y = 32
NSEND = 16
HOIST = 64
PARTS = 2
SPOTS = [2, 13, 3, 4, 11, 12, 5, 10, 6, 7, 8, 9]
PARTNER = [SPOTS.index(15 - spot) for spot in SPOTS]


def x_lags():
    near, far = 2 * T_NEAR + 2, 2 * T_FAR + 2
    hops = [near, far, near, D_XR, near, far, near]
    lags = [0]
    for hop in hops:
        lags.append(lags[-1] + 4 + hop)
    return lags


def y_lags():
    lags = [0]
    for hop in [2 * T_Y + 3, D_YR, 2 * T_Y + 3]:
        lags.append(lags[-1] + 16 + hop)
    return lags


LAG_X, LAG_Y = x_lags(), y_lags()
STEPS = ND * NB + LAG_X[-1] + LAG_Y[-1] + 4 + 15 + 1
BLOCKS = (STEPS + 1) // 2


def tile(k):
    return pl.ds(8 * k, 8)


def pick(values, idx):
    out = jnp.int32(values[0])
    for pos in range(1, len(values)):
        out = jnp.where(idx == pos, jnp.int32(values[pos]), out)
    return out


def kernel(cx_ref, cy_ref, cz_ref, wt_ref, src_hbm, sig_hbm, out_ref,
           inbuf, nat, tab, acc, hbuf, ctab, ntab, cbuf, xbuf, ybuf, yraw, zbuf, inodd, refl,
           xsend, xrecv, ysend, yrecv, pack,
           in_sem, xs_sem, xr_sem, ys_sem, yr_sem):
    def load(arr, part):
        planes = pl.ds(part * (NX // PARTS), NX // PARTS)
        return pltpu.make_async_copy((src_hbm, sig_hbm)[arr].at[planes], inbuf.at[arr, planes], in_sem.at[arr, part])

    for part in range(PARTS):
        for arr in range(2):
            load(arr, part).start()

    dx = lax.axis_index("x")
    dy = lax.axis_index("y")
    has_left, has_right = dx > 0, dx < 3
    odd_x = (dx & 1) == 1
    trip_left = jnp.where(odd_x, T_NEAR, T_FAR)
    trip_right = jnp.where(odd_x, T_FAR, T_NEAR)
    lane = lax.broadcasted_iota(jnp.int32, (8, 128), 1)
    subl = lax.broadcasted_iota(jnp.int32, (8, 128), 0)
    oct_id = lane // 16
    oct_y = (oct_id // 2) % 2
    patch_y = lane - 16 * oct_id
    zero = jnp.zeros((8, 128), F32)
    low_half = lane < 64
    first_y = patch_y == 0

    lag_xm, lag_xp = pick(LAG_X[:4][::-1], dx), pick(LAG_X[4:], dx)
    lag_ym, lag_yp = pick(LAG_Y[:2][::-1], dy), pick(LAG_Y[2:], dy)
    lag_oct = jnp.where(lane >= 64, lag_xp, lag_xm) + jnp.where(oct_y == 1, lag_yp, lag_ym)
    lag_lane = patch_y + lag_oct
    hbuf[...] = lax.rem(2 * lag_lane + subl, 2 * NB)
    turn = lax.rem(lag_lane, NB)
    turn_bits = [(turn >> bit) & 1 == 1 for bit in range(5)]

    for pos in range(5):
        col = jnp.ones((8, 128), F32) if pos == 0 else zero
        for m in range(ND):
            two_x, two_y, two_z = 2.0 * cx_ref[m], 2.0 * cy_ref[m], 2.0 * cz_ref[m]
            val = (two_x + two_y + two_z, 2.0 * two_x, 2.0 * two_y, 2.0 * two_z, wt_ref[m])[pos]
            col = jnp.where(lane == m + 1, val, col)
        ctab[pos] = col
        cbuf[pos] = jnp.ones((8, 128), F32) if pos == 0 else zero

    cols = [ctab[pos] for pos in range(5)]

    @pl.loop(0, ntab.shape[1] // 64)
    def _(k):
        for part in range(8):
            first = 64 * k + 8 * part
            c_idx = jnp.clip((((first + subl - lag_oct) * 1311) >> 15) + 1, 0, ND + 1)
            for pos in range(5):
                ntab[pos, pl.ds(first, 8), :] = jnp.take_along_axis(cols[pos], c_idx, axis=1)

    for k in range(55):
        xbuf[tile(k), :] = zero
    for k in range(48):
        ybuf[k] = zero
    for k in range(12):
        yraw[k] = zero
    for k in range(9):
        zbuf[k] = zero
    inodd[...] = zero
    for k in range(4):
        refl[k] = zero
        for j in range(4):
            pack[k, j] = zero

    @pl.loop(0, RING)
    def _(k):
        for side in range(2):
            for q in range(6):
                xrecv[side, k, tile(q), :] = zero
            for r in range(2):
                yrecv[k + side * RING, r] = zero

    barrier = pltpu.get_barrier_semaphore()

    @pl.when(has_left)
    def _():
        pl.semaphore_signal(barrier, inc=1, device_id={"x": dx - 1}, device_id_type=MESH)

    @pl.when(has_right)
    def _():
        pl.semaphore_signal(barrier, inc=1, device_id={"x": dx + 1}, device_id_type=MESH)

    pl.semaphore_signal(barrier, inc=1, device_id={"y": 1 - dy}, device_id_type=MESH)

    mirror = (71 - lane) & 127
    tail = lane < 72

    for part in range(PARTS):
        for arr in range(2):
            load(arr, part).wait()

        @pl.loop(part * (NX // PARTS), (part + 1) * (NX // PARTS), step=2)
        def _(first):
            for x in (first, first + 1):
                for arr in range(2):
                    for yt in range(NY // 8):
                        rows = tile(yt)
                        half_a = inbuf[arr, x, rows, pl.ds(0, 128)]
                        nat[arr, 0, x, rows, :] = half_a
                        nat[arr, 1, x, rows, pl.ds(0, 72)] = inbuf[arr, x, rows, pl.ds(128, 72)]
                        half_b = nat[arr, 1, x, rows, :]
                        flip_a = jnp.take_along_axis(half_a, mirror, axis=1)
                        flip_b = jnp.take_along_axis(half_b, mirror, axis=1)
                        nat[arr, 2, x, rows, :] = jnp.where(tail, flip_b, flip_a)
                        nat[arr, 3, x, rows, :] = flip_a

    flip_rows = 7 - subl

    def row_groups(x_patch, i, j):
        for octant in range(8):
            bx, by = octant // 4, (octant // 2) % 2
            x_rel = 3 * x_patch + i
            x_abs = x_rel if bx else NX - 1 - x_rel
            for half in range(2):
                y_abs = (24 * half + j) if by else (26 - 24 * half - j)
                yield octant, half, x_abs, y_abs, by == 0

    def turn_blocks(blocks, step):
        for bit in range(5):
            shift = step * (1 << bit)
            blocks = [jnp.where(turn_bits[bit], blocks[(v - shift) % NB], blocks[v]) for v in range(NB)]
        return blocks

    odd_patch = (subl & 1) == 1

    def block_rows(v, half, odd):
        return pl.ds(FRONT + lax.rem(v + half, NB) * PITCH + (2 * half + odd) + 4 * LEVEL * odd, 8, stride=LEVEL)

    @pl.loop(0, 12)
    def _(trip):
        i, half = trip // 4, trip & 3
        for odd in range(2):
            for j in range(3):
                cell = 3 * i + j
                for arr in range(2):
                    pieces = [[], []]
                    for octant, part, x_abs, y_abs, rev in row_groups(2 * half + odd, i, j):
                        for zh in range(2):
                            kind = zh + (0 if octant % 2 else 2)
                            val = nat[arr, kind, x_abs, pl.ds(y_abs, 8, stride=3), :]
                            if rev:
                                val = jnp.take_along_axis(val, flip_rows, axis=0)
                            pieces[zh].append(val)
                    lo = jnp.concatenate(pieces[0], axis=0).T
                    hi = jnp.concatenate(pieces[1], axis=0).T
                    blocks = [lo[8 * v:8 * v + 8] for v in range(16)] + [hi[8 * v:8 * v + 8] for v in range(9)]
                    blocks = turn_blocks(blocks, 1)
                    for v in range(NB):
                        tab[arr, cell, block_rows(v, half, odd), :] = blocks[v]
                        if arr == 0:
                            tab[2, cell, block_rows(v, half, odd), :] = zero

    @pl.loop(0, 9)
    def _(cell):
        for arr in range(2):
            for k in range(4):
                first, wrapped = pl.ds(FRONT + LEVEL * k, 8), pl.ds(FRONT + NB * PITCH + LEVEL * k, 8)
                tab[arr, cell, first, :] = jnp.where(odd_patch, tab[arr, cell, wrapped, :], tab[arr, cell, first, :])
        for k in range(4):
            tab[2, cell, pl.ds(FRONT + LEVEL * k, 8), :] = zero

    pl.semaphore_wait(barrier, has_left.astype(jnp.int32) + has_right.astype(jnp.int32) + 1)

    keep_send = oct_y == 1 - dy
    even_mask, odd_mask = oct_y == dy, oct_y == 1 - dy
    mirror_x, mirror_y = dx == 0, dy == 0
    has = (has_left, has_right, True)
    trips = (trip_left, trip_right, T_Y)
    rings = (RING, RING, RING_Y)

    def copy(kind, n, count=1):
        slot, here, batch = (n + trips[kind]) & (rings[kind] - 1), n & (NSEND - 1), (n >> 3) & 1
        if count > 1:
            here, slot = pl.ds(8 * batch, count), pl.ds(0, count)
        if kind == 2:
            return pltpu.make_async_remote_copy(
                src_ref=ysend.at[here], dst_ref=yrecv.at[slot], send_sem=ys_sem.at[batch],
                recv_sem=yr_sem.at[0 if count > 1 else slot], device_id={"y": 1 - dy}, device_id_type=MESH)
        return pltpu.make_async_remote_copy(
            src_ref=xsend.at[here], dst_ref=xrecv.at[kind, slot], send_sem=xs_sem.at[kind, batch],
            recv_sem=xr_sem.at[kind, 0 if count > 1 else slot],
            device_id={"x": dx - 1 if kind == 0 else dx + 1}, device_id_type=MESH)

    def arrival(kind, n):
        slot = n & (rings[kind] - 1)
        if kind == 2:
            return pltpu.make_async_remote_copy(
                src_ref=ysend.at[0], dst_ref=yrecv.at[slot], send_sem=ys_sem.at[0], recv_sem=yr_sem.at[slot],
                device_id={"y": dy}, device_id_type=MESH)
        return pltpu.make_async_remote_copy(
            src_ref=xsend.at[0], dst_ref=xrecv.at[kind, slot], send_sem=xs_sem.at[kind, 0],
            recv_sem=xr_sem.at[kind, slot], device_id={"x": dx}, device_id_type=MESH)

    def when(cond, act):
        if cond is True:
            act()
        else:
            pl.when(cond)(act)

    def both(one, two):
        return two if one is True else (one if two is True else one & two)

    def next_turn(turn_now):
        return jnp.where(turn_now == NB - 1, 0, turn_now + 1)

    senders = (has_right, has_left, True)
    delays = (trip_right, trip_left, T_Y)

    def block(n, turn_now):
        here = n & (NSEND - 1)
        slot = n & (RING - 1)
        now, last, before = n & 3, (n + 3) & 3, (n + 2) & 3

        outs = [xbuf[pl.ds(72 * q + 8, 8, stride=9), :] for q in range(6)]
        packs = [pack[before, 2], pack[before, 3], pack[last, 0], pack[last, 1]]
        for q in range(6):
            xsend[here, tile(q), :] = outs[q]
        for r in range(2):
            ysend[here, r] = jnp.where(keep_send, packs[2 * r], packs[2 * r + 1])
        for kind in range(3):
            when(has[kind], lambda kind=kind: copy(kind, n).start())
        for kind in range(3):
            when(both(senders[kind], n >= delays[kind]), lambda kind=kind: arrival(kind, n).wait_recv())

        edges = []
        for q in range(6):
            rows = tile(q)
            from_left = jnp.where(mirror_x, pltpu.roll(outs[q], 64, 1), xrecv[1, slot, rows, :])
            edges.append(jnp.where(low_half, xrecv[0, slot, rows, :], from_left))
        got = [yrecv[n & (RING_Y - 1), r] for r in range(2)]
        incoming = [jnp.where(even_mask, got[0], refl[0]), jnp.where(odd_mask, pltpu.roll(got[0], 64, 1), refl[1]),
                    jnp.where(even_mask, got[1], refl[2]), inodd[...]]
        inodd[...] = jnp.where(odd_mask, pltpu.roll(got[1], 64, 1), refl[3])
        for k in range(4):
            refl[k] = jnp.where(mirror_y, pltpu.roll(packs[k], 96 if k % 2 else 32, 1), 0.0)

        mains, mixes = {}, {}

        def serve(s, faces):
            group = s // 4
            for i in range(3):
                f = 3 * (s % 4) + i
                spot = SPOTS[f]
                mains[f] = pltpu.roll(faces[i], 1, 1)
                mixed = jnp.where(patch_y == 15 - spot, incoming[group], faces[i])
                mixes[PARTNER[f]] = pltpu.roll(mixed, (1 + spot + (16 if group % 2 else 112)) % 128, 1)
                pltpu.store(pack.at[last if group == 3 else now, group], mixes[PARTNER[f]], mask=patch_y == spot)
            for f in [f for f in mains if f in mixes]:
                ybuf[(12 * group + f + 24) % 48] = jnp.where(first_y, mixes.pop(f), mains.pop(f))

        for s in range(12, 16):
            serve(s, [yraw[3 * (s - 12) + i] for i in range(3)])

        turns = [turn_now, next_turn(turn_now)]
        z_face = [zbuf[c] for c in range(9)]
        coef = [cbuf[pos] for pos in range(5)]
        for s in range(16):
            if s % 4 == 0:
                fresh = hbuf[...] == 2 * turns[s // 8] + (s // 4) % 2
                row = pl.ds(2 * n + s // 8, 1)
                coef = [jnp.where(fresh, ntab[pos, row, :], coef[pos]) for pos in range(5)]
                asum, ax, ay, az, wt = coef
                z_face = [jnp.where(fresh, 0.0, z_face[c]) for c in range(9)]
            if s == 4:
                for q in range(6):
                    xbuf[pl.ds(72 * q, 8, stride=9), :] = edges[q]
            rows = pl.ds(turns[s // 8] * PITCH + (FRONT + LEVEL * (s % 8)), 8)
            x_face = [xbuf[pl.ds(9 * (3 * s + j), 8), :] for j in range(3)]
            y_out = []
            for i in range(3):
                y_face = ybuf[3 * s + i]
                for j in range(3):
                    c = 3 * i + j
                    total = ((tab[0, c, rows, :] + z_face[c]) + x_face[j]) + y_face
                    psi = total * (1.0 / (tab[1, c, rows, :] + asum))
                    x_face[j] = ax * psi - x_face[j]
                    y_face = ay * psi - y_face
                    z_face[c] = az * psi - z_face[c]
                    tab[2, c, rows, :] = tab[2, c, rows, :] + wt * psi
                y_out.append(y_face)
            if s < 12:
                serve(s, y_out)
            else:
                for i in range(3):
                    yraw[3 * (s - 12) + i] = y_out[i]
            for j in range(3):
                xbuf[pl.ds(9 * ((3 * s + j + 12) % 48) + 1, 8), :] = x_face[j]
        for c in range(9):
            zbuf[c] = z_face[c]
        for pos in range(5):
            cbuf[pos] = coef[pos]
        return next_turn(turns[1])

    def batch(first, turn_now):
        for kind in range(3):
            when(both(has[kind], first >= 2), lambda kind=kind: copy(kind, 8 * (first - 2), 8).wait_send())
        return lax.fori_loop(8 * first, jnp.minimum(8 * first + 8, BLOCKS), block, turn_now)

    lax.fori_loop(0, (BLOCKS + 7) // 8, batch, jnp.int32(0))

    @pl.loop(0, 9)
    def _(cell):
        for k in range(4):
            tab[2, cell, pl.ds(FRONT + NB * PITCH + LEVEL * k, 8), :] = tab[2, cell, pl.ds(FRONT + LEVEL * k, 8), :]

    @pl.loop(0, 12)
    def _(trip):
        i, half = trip // 4, trip & 3
        for odd in range(2):
            for j in range(3):
                cell = 3 * i + j
                blocks = turn_blocks([tab[2, cell, block_rows(v, half, odd), :] for v in range(NB)], -1)
                lo = jnp.concatenate(blocks[:16], axis=0).T
                hi = jnp.concatenate(blocks[16:] + [zero] * 7, axis=0).T
                for octant, side, x_abs, y_abs, rev in row_groups(2 * half + odd, i, j):
                    for zh in range(2):
                        val = (lo, hi)[zh][16 * octant + 8 * side:16 * octant + 8 * side + 8]
                        if rev:
                            val = jnp.take_along_axis(val, flip_rows, axis=0)
                        acc[octant, zh, x_abs, pl.ds(y_abs, 8, stride=3), :] = val

    @pl.loop(0, NX)
    def _(x):
        for yt in range(NY // 8):
            rows = tile(yt)
            (dn_a, up_a), (dn_b, up_b) = [
                [sum(acc[octant, zh, x, rows, :] for octant in range(bz + 2, 8, 2)) + acc[bz, zh, x, rows, :]
                 for bz in range(2)] for zh in range(2)]
            dn_a = jnp.take_along_axis(dn_a, mirror, axis=1)
            dn_b = jnp.take_along_axis(dn_b, mirror, axis=1)
            out_ref[x, rows, pl.ds(0, 128)] = up_a + jnp.where(tail, dn_b, dn_a)
            out_ref[x, rows, pl.ds(128, 72)] = (up_b + dn_a)[:, :72]

    for kind in range(3):
        for first in range(max(0, 8 * ((BLOCKS + 7) // 8 - 2)), BLOCKS, 8):
            when(has[kind], lambda kind=kind, first=first:
                 copy(kind, jnp.int32(first), min(8, BLOCKS - first)).wait_send())
        for late in range(max(T_NEAR, T_FAR) if kind < 2 else T_Y):
            when(both(senders[kind], late < delays[kind]), lambda kind=kind, late=late:
                 arrival(kind, jnp.int32(BLOCKS + late)).wait_recv())


def solution(mesh):
    grid_spec = P(("g", "x"), "y", None)

    def column_sweep(source, sigma_t, cos_x, cos_y, cos_z, weights):
        smem = pl.BlockSpec(memory_space=pltpu.SMEM)
        vmem = pl.BlockSpec(memory_space=pltpu.VMEM)
        return pl.pallas_call(
            kernel,
            out_shape=pltpu.VMEM((NX, NY, NZ), F32),
            in_specs=[smem] * 4 + [pl.BlockSpec(memory_space=pl.ANY)] * 2,
            out_specs=vmem,
            scratch_shapes=[
                pltpu.VMEM((2, NX, NY, NZ), F32),
                pltpu.VMEM((2, 4, NX, NY, 128), F32),
                pltpu.VMEM((3, 9, ROWS, 128), F32),
                pltpu.VMEM((8, 2, NX, NY, 128), F32),
                pltpu.VMEM((8, 128), jnp.int32),
                pltpu.VMEM((5, 8, 128), F32),
                pltpu.VMEM((5, 64 * pl.cdiv(2 * BLOCKS, 64), 128), F32),
                pltpu.VMEM((5, 8, 128), F32),
                pltpu.VMEM((440, 128), F32),
                pltpu.VMEM((48, 8, 128), F32),
                pltpu.VMEM((12, 8, 128), F32),
                pltpu.VMEM((9, 8, 128), F32),
                pltpu.VMEM((8, 128), F32),
                pltpu.VMEM((4, 8, 128), F32),
                pltpu.VMEM((NSEND, 48, 128), F32),
                pltpu.VMEM((2, RING, 48, 128), F32),
                pltpu.VMEM((NSEND, 2, 8, 128), F32),
                pltpu.VMEM((RING_Y, 2, 8, 128), F32),
                pltpu.VMEM((4, 4, 8, 128), F32),
                pltpu.SemaphoreType.DMA((2, PARTS)),
                pltpu.SemaphoreType.DMA((2, 2)),
                pltpu.SemaphoreType.DMA((2, RING)),
                pltpu.SemaphoreType.DMA((2,)),
                pltpu.SemaphoreType.DMA((RING_Y,)),
            ],
            compiler_params=pltpu.CompilerParams(
                collective_id=0, has_side_effects=True, vmem_limit_bytes=60 * 1024 * 1024),
        )(cos_x, cos_y, cos_z, weights, source, sigma_t)

    return jax.shard_map(column_sweep, mesh=mesh, in_specs=(grid_spec, grid_spec, P(), P(), P(), P()),
                         out_specs=grid_spec, check_vma=False)
```

```python
import functools

import jax
import jax.numpy as jnp
from jax import lax
from jax.experimental import pallas as pl
from jax.experimental.pallas import tpu as pltpu
from jax.sharding import PartitionSpec as P

F32 = jnp.float32
MESH = pl.DeviceIdType.MESH
NX, NY, NZ = 24, 48, 200
ND = 10
NB = NZ // 8
LEVEL = 12
FRONT = 4 * LEVEL
PITCH = 8 * LEVEL
ROWS = NB * PITCH + 112
T_NEAR = 3
T_FAR = 8
T_Y = 8
D_XR = 2
D_YR = 5
RING = 32
NSEND = 16
HOIST = 40
THREE, CELLS = range(3), range(9)
PARTS = 2
SPOTS = [2, 13, 3, 4, 11, 12, 5, 10, 6, 7, 8, 9]
PARTNER = [SPOTS.index(15 - spot) for spot in SPOTS]


def x_lags():
    near, far = 2 * T_NEAR + 2, 2 * T_FAR + 2
    hops = [near, far, near, D_XR, near, far, near]
    lags = [0]
    for hop in hops:
        lags.append(lags[-1] + 4 + hop)
    return lags


def y_lags():
    lags = [0]
    for hop in [2 * T_Y + 3, D_YR, 2 * T_Y + 3]:
        lags.append(lags[-1] + 16 + hop)
    return lags


LAG_X, LAG_Y = x_lags(), y_lags()
STEPS = ND * NB + LAG_X[-1] + LAG_Y[-1] + 4 + 15 + 1
BLOCKS = (STEPS + 1) // 2


def tile(k):
    return pl.ds(8 * k, 8)


def pick(values, idx):
    out = jnp.int32(values[0])
    for pos in range(1, len(values)):
        out = jnp.where(idx == pos, jnp.int32(values[pos]), out)
    return out


def kernel(cx_ref, cy_ref, cz_ref, wt_ref, src_hbm, sig_hbm, out_ref,
           inbuf, nat, tab, flux, acc, hbuf, ctab, ntab, cbuf, xbuf, ybuf, yraw, zbuf, inodd, refl,
           xsend, xrecv, ysend, yrecv, pack,
           in_sem, xs_sem, xr_sem, ys_sem, yr_sem):
    def load(arr, part):
        planes = pl.ds(part * (NX // PARTS), NX // PARTS)
        return pltpu.make_async_copy((src_hbm, sig_hbm)[arr].at[planes], inbuf.at[arr, planes], in_sem.at[arr, part])

    for part in range(PARTS):
        for arr in range(2):
            load(arr, part).start()

    dx = lax.axis_index("x")
    dy = lax.axis_index("y")
    has_left, has_right = dx > 0, dx < 3
    odd_x = (dx & 1) == 1
    trip_left = jnp.where(odd_x, T_NEAR, T_FAR)
    trip_right = jnp.where(odd_x, T_FAR, T_NEAR)
    lane = lax.broadcasted_iota(jnp.int32, (8, 128), 1)
    subl = lax.broadcasted_iota(jnp.int32, (8, 128), 0)
    oct_id = lane // 16
    oct_y = (oct_id // 2) % 2
    patch_y = lane - 16 * oct_id
    zero = jnp.zeros((8, 128), F32)
    low_half = lane < 64
    first_y, last_y = patch_y == 0, patch_y == 15

    lag_xm, lag_xp = pick(LAG_X[:4][::-1], dx), pick(LAG_X[4:], dx)
    lag_ym, lag_yp = pick(LAG_Y[:2][::-1], dy), pick(LAG_Y[2:], dy)
    lag_oct = jnp.where(lane >= 64, lag_xp, lag_xm) + jnp.where(oct_y == 1, lag_yp, lag_ym)
    lag_lane = patch_y + lag_oct
    hbuf[...] = lax.rem(2 * lag_lane + subl, 2 * NB)
    turn = lax.rem(lag_lane, NB)
    turn_bits = [(turn >> bit) & 1 == 1 for bit in range(5)]

    for pos in range(5):
        col = jnp.ones((8, 128), F32) if pos == 0 else zero
        for m in range(ND):
            two_x, two_y, two_z = 2.0 * cx_ref[m], 2.0 * cy_ref[m], 2.0 * cz_ref[m]
            val = (two_x + two_y + two_z, 2.0 * two_x, 2.0 * two_y, 2.0 * two_z, wt_ref[m])[pos]
            col = jnp.where(lane == m + 1, val, col)
        ctab[pos] = col
        cbuf[pos] = jnp.ones((8, 128), F32) if pos == 0 else zero

    cols = [ctab[pos] for pos in range(5)]

    @pl.loop(0, ntab.shape[1] // 64)
    def _(k):
        for part in range(8):
            first = 64 * k + 8 * part
            c_idx = jnp.clip((((first + subl - lag_oct) * 1311) >> 15) + 1, 0, ND + 1)
            for pos in range(5):
                ntab[pos, pl.ds(first, 8), :] = jnp.take_along_axis(cols[pos], c_idx, axis=1)

    for k in range(55):
        xbuf[tile(k), :] = zero
    for k in range(48):
        ybuf[k] = zero
    for k in range(12):
        yraw[k] = zero
    for k in CELLS:
        zbuf[k] = zero
    inodd[...] = zero
    for k in range(4):
        refl[k] = zero
        for j in range(4):
            pack[k, j] = zero

    @pl.loop(0, RING)
    def _(k):
        for side in range(2):
            for q in range(6):
                xrecv[side, k, tile(q), :] = zero
            for r in range(2):
                yrecv[k, r] = zero

    barrier = pltpu.get_barrier_semaphore()

    @pl.when(has_left)
    def _():
        pl.semaphore_signal(barrier, inc=1, device_id={"x": dx - 1}, device_id_type=MESH)

    @pl.when(has_right)
    def _():
        pl.semaphore_signal(barrier, inc=1, device_id={"x": dx + 1}, device_id_type=MESH)

    pl.semaphore_signal(barrier, inc=1, device_id={"y": 1 - dy}, device_id_type=MESH)

    mirror = (71 - lane) & 127
    tail = lane < 72

    for part in range(PARTS):
        for arr in range(2):
            load(arr, part).wait()

        @pl.loop(part * (NX // PARTS), (part + 1) * (NX // PARTS), step=2)
        def _(first):
            for x in (first, first + 1):
                for arr in range(2):
                    for yt in range(NY // 8):
                        rows = tile(yt)
                        half_a = inbuf[arr, x, rows, pl.ds(0, 128)]
                        nat[arr, 0, x, rows, :] = half_a
                        nat[arr, 1, x, rows, pl.ds(0, 72)] = inbuf[arr, x, rows, pl.ds(128, 72)]
                        half_b = nat[arr, 1, x, rows, :]
                        flip_a = jnp.take_along_axis(half_a, mirror, axis=1)
                        flip_b = jnp.take_along_axis(half_b, mirror, axis=1)
                        nat[arr, 2, x, rows, :] = jnp.where(tail, flip_b, flip_a)
                        nat[arr, 3, x, rows, :] = flip_a

    flip_rows = 7 - subl

    def row_groups(x_patch, i, j):
        for octant in range(8):
            bx, by = octant // 4, (octant // 2) % 2
            x_rel = 3 * x_patch + i
            x_abs = x_rel if bx else NX - 1 - x_rel
            for half in range(2):
                y_abs = (24 * half + j) if by else (26 - 24 * half - j)
                yield octant, half, x_abs, y_abs, by == 0

    def turn_blocks(blocks, step):
        for bit in range(5):
            shift = step * (1 << bit)
            blocks = [jnp.where(turn_bits[bit], blocks[(v - shift) % NB], blocks[v]) for v in range(NB)]
        return blocks

    odd_patch = (subl & 1) == 1

    def block_rows(v, half, odd):
        return pl.ds(FRONT + lax.rem(v + half, NB) * PITCH + (2 * half + odd) + 4 * LEVEL * odd, 8, stride=LEVEL)

    @pl.loop(0, 12)
    def _(trip):
        i, half = trip // 4, trip & 3
        for odd in range(2):
            for j in THREE:
                cell = 3 * i + j
                for arr in range(2):
                    pieces = [[], []]
                    for octant, part, x_abs, y_abs, rev in row_groups(2 * half + odd, i, j):
                        for zh in range(2):
                            kind = zh + (0 if octant % 2 else 2)
                            val = nat[arr, kind, x_abs, pl.ds(y_abs, 8, stride=3), :]
                            if rev:
                                val = jnp.take_along_axis(val, flip_rows, axis=0)
                            pieces[zh].append(val)
                    lo = jnp.concatenate(pieces[0], axis=0).T
                    hi = jnp.concatenate(pieces[1], axis=0).T
                    blocks = [lo[8 * v:8 * v + 8] for v in range(16)] + [hi[8 * v:8 * v + 8] for v in CELLS]
                    blocks = turn_blocks(blocks, 1)
                    for v in range(NB):
                        tab[arr, cell, block_rows(v, half, odd), :] = blocks[v]
                        if arr == 0:
                            flux[cell, block_rows(v, half, odd), :] = zero

    @pl.loop(0, 9)
    def _(cell):
        for arr in range(2):
            for k in range(4):
                first, wrapped = pl.ds(FRONT + LEVEL * k, 8), pl.ds(FRONT + NB * PITCH + LEVEL * k, 8)
                tab[arr, cell, first, :] = jnp.where(odd_patch, tab[arr, cell, wrapped, :], tab[arr, cell, first, :])
        for k in range(4):
            flux[cell, pl.ds(FRONT + LEVEL * k, 8), :] = zero

    pl.semaphore_wait(barrier, has_left.astype(jnp.int32) + has_right.astype(jnp.int32) + 1)

    keep_send = oct_y == 1 - dy
    even_mask, odd_mask = oct_y == dy, oct_y == 1 - dy
    mirror_x, mirror_y = dx == 0, dy == 0
    has = (has_left, has_right, True)
    trips = (trip_left, trip_right, T_Y)

    def copy(kind, n, count=1):
        slot, here, batch = (n + 1 + trips[kind]) & (RING - 1), n & (NSEND - 1), (n >> 3) & 1
        if count > 1:
            here, slot = pl.ds(8 * batch, count), pl.ds(0, count)
        if kind == 2:
            return pltpu.make_async_remote_copy(
                src_ref=ysend.at[here], dst_ref=yrecv.at[slot], send_sem=ys_sem.at[batch],
                recv_sem=yr_sem.at[0 if count > 1 else slot], device_id={"y": 1 - dy}, device_id_type=MESH)
        return pltpu.make_async_remote_copy(
            src_ref=xsend.at[here], dst_ref=xrecv.at[kind, slot], send_sem=xs_sem.at[kind, batch],
            recv_sem=xr_sem.at[kind, 0 if count > 1 else slot],
            device_id={"x": dx - 1 if kind == 0 else dx + 1}, device_id_type=MESH)

    def arrival(kind, n):
        slot = n & (RING - 1)
        if kind == 2:
            return pltpu.make_async_remote_copy(
                src_ref=ysend.at[0], dst_ref=yrecv.at[slot], send_sem=ys_sem.at[0], recv_sem=yr_sem.at[slot],
                device_id={"y": dy}, device_id_type=MESH)
        return pltpu.make_async_remote_copy(
            src_ref=xsend.at[0], dst_ref=xrecv.at[kind, slot], send_sem=xs_sem.at[kind, 0],
            recv_sem=xr_sem.at[kind, slot], device_id={"x": dx}, device_id_type=MESH)

    def when(cond, act):
        if cond is True:
            act()
        else:
            pl.when(cond)(act)

    def both(one, two):
        return two if one is True else (one if two is True else one & two)

    def next_turn(turn_now):
        return jnp.where(turn_now == NB - 1, 0, turn_now + 1)

    senders = (has_right, has_left, True)
    delays = (trip_right, trip_left, T_Y)

    def block(n, turn_now):
        here = n & (NSEND - 1)
        slot = n & (RING - 1)
        now, last, before = n & 3, (n + 3) & 3, (n + 2) & 3

        outs = [xbuf[pl.ds(72 * q + 8, 8, stride=9), :] for q in range(6)]
        packs = [pack[before, 2], pack[before, 3], pack[last, 0], pack[last, 1]]
        for kind in THREE:
            when(both(senders[kind], n > delays[kind]), lambda kind=kind: arrival(kind, n).wait_recv())

        edges = []
        for q in range(6):
            rows = tile(q)
            from_left = jnp.where(mirror_x, pltpu.roll(outs[q], 64, 1), xrecv[1, slot, rows, :])
            edges.append(jnp.where(low_half, xrecv[0, slot, rows, :], from_left))
        got = [yrecv[slot, r] for r in range(2)]
        incoming = [jnp.where(even_mask, got[0], refl[0]), jnp.where(odd_mask, pltpu.roll(got[0], 64, 1), refl[1]),
                    jnp.where(even_mask, got[1], refl[2]), inodd[...]]
        inodd[...] = jnp.where(odd_mask, pltpu.roll(got[1], 64, 1), refl[3])
        for k in range(4):
            refl[k] = jnp.where(mirror_y, pltpu.roll(packs[k], 96 if k % 2 else 32, 1), 0.0)

        mains, mixes = {}, {}

        def serve(s, faces):
            group = s // 4
            for i in THREE:
                f = 3 * (s % 4) + i
                spot = SPOTS[f]
                mains[f] = pltpu.roll(faces[i], 1, 1)
                mixed = jnp.where(last_y, faces[i], incoming[group])
                mixes[PARTNER[f]] = pltpu.roll(mixed, (1 + spot + (16 if group % 2 else 112)) % 128, 1)
                pltpu.store(pack.at[last if group == 3 else now, group], mixes[PARTNER[f]], mask=patch_y == spot)
            for f in [f for f in mains if f in mixes]:
                ybuf[(12 * group + f + 24) % 48] = jnp.where(first_y, mixes.pop(f), mains.pop(f))

        for s in range(12, 16):
            serve(s, [yraw[3 * (s - 12) + i] for i in THREE])

        turns = [turn_now, next_turn(turn_now)]
        z_face = [zbuf[c] for c in CELLS]
        coef = [cbuf[pos] for pos in range(5)]
        for s in range(16):
            if s % 4 == 0:
                fresh = hbuf[...] == 2 * turns[s // 8] + (s // 4) % 2
                row = pl.ds(2 * n + s // 8, 1)
                coef = [jnp.where(fresh, ntab[pos, row, :], coef[pos]) for pos in range(5)]
                asum, ax, ay, az, wt = coef
                z_face = [jnp.where(fresh, 0.0, z_face[c]) for c in CELLS]
            if s == 4:
                for q in range(6):
                    xbuf[pl.ds(72 * q, 8, stride=9), :] = edges[q]
            rows = pl.ds(turns[s // 8] * PITCH + (FRONT + LEVEL * (s % 8)), 8)
            x_face = [xbuf[pl.ds(9 * (3 * s + j), 8), :] for j in THREE]
            y_out = []
            for i in THREE:
                y_face = ybuf[3 * s + i]
                for j in THREE:
                    c = 3 * i + j
                    total = ((tab[0, c, rows, :] + z_face[c]) + x_face[j]) + y_face
                    psi = total * (1.0 / (tab[1, c, rows, :] + asum))
                    x_face[j] = ax * psi - x_face[j]
                    y_face = ay * psi - y_face
                    z_face[c] = az * psi - z_face[c]
                    flux[c, rows, :] = flux[c, rows, :] + wt * psi
                y_out.append(y_face)
            if s < 12:
                serve(s, y_out)
            else:
                for i in THREE:
                    yraw[3 * (s - 12) + i] = y_out[i]
            for j in THREE:
                xbuf[pl.ds(9 * ((3 * s + j + 12) % 48) + 1, 8), :] = x_face[j]
        for c in CELLS:
            zbuf[c] = z_face[c]
        for pos in range(5):
            cbuf[pos] = coef[pos]
        for q in range(6):
            xsend[here, tile(q), :] = xbuf[pl.ds(72 * q + 8, 8, stride=9), :]
        for r in range(2):
            pair = (last, now)[r]
            ysend[here, r] = jnp.where(keep_send, pack[pair, 2 - 2 * r], pack[pair, 3 - 2 * r])
        for kind in (2, 0, 1):
            when(has[kind], lambda kind=kind: copy(kind, n).start())
        return next_turn(turns[1])

    def batch(first, turn_now):
        for kind in THREE:
            when(both(has[kind], first >= 2), lambda kind=kind: copy(kind, 8 * (first - 2), 8).wait_send())
        return lax.fori_loop(8 * first, jnp.minimum(8 * first + 8, BLOCKS), block, turn_now)

    lax.fori_loop(0, (BLOCKS + 7) // 8, batch, jnp.int32(0))

    @pl.loop(0, 9)
    def _(cell):
        for k in range(4):
            flux[cell, pl.ds(FRONT + NB * PITCH + LEVEL * k, 8), :] = flux[cell, pl.ds(FRONT + LEVEL * k, 8), :]

    @pl.loop(0, 12)
    def _(trip):
        i, half = trip // 4, trip & 3
        for odd in range(2):
            for j in THREE:
                cell = 3 * i + j
                blocks = turn_blocks([flux[cell, block_rows(v, half, odd), :] for v in range(NB)], -1)
                lo = jnp.concatenate(blocks[:16], axis=0).T
                hi = jnp.concatenate(blocks[16:] + [zero] * 7, axis=0).T
                for octant, side, x_abs, y_abs, rev in row_groups(2 * half + odd, i, j):
                    for zh in range(2):
                        val = (lo, hi)[zh][16 * octant + 8 * side:16 * octant + 8 * side + 8]
                        if rev:
                            val = jnp.take_along_axis(val, flip_rows, axis=0)
                        acc[octant, zh, x_abs, pl.ds(y_abs, 8, stride=3), :] = val

    @pl.loop(0, NX, step=4)
    def _(first):
        for x, yt in [(first + k, yt) for k in range(4) for yt in range(NY // 8)]:
            rows = tile(yt)
            (dn_a, up_a), (dn_b, up_b) = [
                [sum(acc[octant, zh, x, rows, :] for octant in range(bz + 2, 8, 2)) + acc[bz, zh, x, rows, :]
                 for bz in range(2)] for zh in range(2)]
            dn_a = jnp.take_along_axis(dn_a, mirror, axis=1)
            dn_b = jnp.take_along_axis(dn_b, mirror, axis=1)
            out_ref[x, rows, pl.ds(0, 128)] = up_a + jnp.where(tail, dn_b, dn_a)
            out_ref[x, rows, pl.ds(128, 72)] = (up_b + dn_a)[:, :72]

    for kind in THREE:
        for first in range(max(0, 8 * ((BLOCKS + 7) // 8 - 2)), BLOCKS, 8):
            when(has[kind], lambda kind=kind, first=first:
                 copy(kind, jnp.int32(first), min(8, BLOCKS - first)).wait_send())
        for late in range(1 + (max(T_NEAR, T_FAR) if kind < 2 else T_Y)):
            when(both(senders[kind], late <= delays[kind]), lambda kind=kind, late=late:
                 arrival(kind, jnp.int32(BLOCKS + late)).wait_recv())


def solution(mesh):
    grid_spec = P(("g", "x"), "y", None)

    def column_sweep(source, sigma_t, cos_x, cos_y, cos_z, weights):
        smem = pl.BlockSpec(memory_space=pltpu.SMEM)
        vmem = pl.BlockSpec(memory_space=pltpu.VMEM)
        return pl.pallas_call(
            kernel,
            out_shape=pltpu.VMEM((NX, NY, NZ), F32),
            in_specs=[smem] * 4 + [pl.BlockSpec(memory_space=pl.ANY)] * 2,
            out_specs=vmem,
            scratch_shapes=[
                pltpu.VMEM((2, NX, NY, NZ), F32),
                pltpu.VMEM((2, 4, NX, NY, 128), F32),
                pltpu.VMEM((2, 9, ROWS, 128), F32),
                pltpu.VMEM((9, ROWS, 128), F32),
                pltpu.VMEM((8, 2, NX, NY, 128), F32),
                pltpu.VMEM((8, 128), jnp.int32),
                pltpu.VMEM((5, 8, 128), F32),
                pltpu.VMEM((5, 64 * pl.cdiv(2 * BLOCKS, 64), 128), F32),
                pltpu.VMEM((5, 8, 128), F32),
                pltpu.VMEM((440, 128), F32),
                pltpu.VMEM((48, 8, 128), F32),
                pltpu.VMEM((12, 8, 128), F32),
                pltpu.VMEM((9, 8, 128), F32),
                pltpu.VMEM((8, 128), F32),
                pltpu.VMEM((4, 8, 128), F32),
                pltpu.VMEM((NSEND, 48, 128), F32),
                pltpu.VMEM((2, RING, 48, 128), F32),
                pltpu.VMEM((NSEND, 2, 8, 128), F32),
                pltpu.VMEM((RING, 2, 8, 128), F32),
                pltpu.VMEM((4, 4, 8, 128), F32),
                pltpu.SemaphoreType.DMA((2, PARTS)),
                pltpu.SemaphoreType.DMA((2, 2)),
                pltpu.SemaphoreType.DMA((2, RING)),
                pltpu.SemaphoreType.DMA((2,)),
                pltpu.SemaphoreType.DMA((RING,)),
            ],
            compiler_params=pltpu.CompilerParams(
                collective_id=0, has_side_effects=True, vmem_limit_bytes=60 * 1024 * 1024),
        )(cos_x, cos_y, cos_z, weights, source, sigma_t)

    return jax.shard_map(column_sweep, mesh=mesh, in_specs=(grid_spec, grid_spec, P(), P(), P(), P()),
                         out_specs=grid_spec, check_vma=False)
```

```python
import functools

import jax
import jax.numpy as jnp
from jax import lax
from jax.experimental import pallas as pl
from jax.experimental.pallas import tpu as pltpu
from jax.sharding import PartitionSpec as P

F32 = jnp.float32
MESH = pl.DeviceIdType.MESH
NX, NY, NZ = 24, 48, 200
ND = 10
NB = NZ // 8
LEVEL = 12
FRONT = 4 * LEVEL
PITCH = 8 * LEVEL
ROWS = NB * PITCH + 112
U = 2
SLOTS = 8 * U
FACES = 3 * SLOTS
T_NEAR = 3
T_FAR = 8
T_Y = 8
D_XR = U
D_YR = U + 1
RING = 32
NSEND = 16
HOIST = 44
THREE, CELLS = range(3), range(9)
PARTS = 2
SPOTS = [2, 13, 3, 4, 11, 12, 5, 10, 6, 7, 8, 9]
PARTNER = [SPOTS.index(15 - spot) for spot in SPOTS]


def x_lags():
    near, far = U * (T_NEAR + 1), U * (T_FAR + 1)
    hops = [near, far, near, D_XR, near, far, near]
    lags = [0]
    for hop in hops:
        lags.append(lags[-1] + 4 + hop)
    return lags


def y_lags():
    lags = [0]
    for hop in [U * (T_Y + 1) + 1, D_YR, U * (T_Y + 1) + 1]:
        lags.append(lags[-1] + 16 + hop)
    return lags


LAG_X, LAG_Y = x_lags(), y_lags()
STEPS = ND * NB + LAG_X[-1] + LAG_Y[-1] + 4 + 15
BLOCKS = (STEPS + U - 1) // U


def tile(k):
    return pl.ds(8 * k, 8)


def pick(values, idx):
    out = jnp.int32(values[0])
    for pos in range(1, len(values)):
        out = jnp.where(idx == pos, jnp.int32(values[pos]), out)
    return out


def kernel(cx_hbm, cy_hbm, cz_hbm, wt_hbm, src_hbm, sig_hbm, out_ref,
           cx_ref, cy_ref, cz_ref, wt_ref, inbuf, nat, tab, flux, acc, hbuf, ctab, ntab, cbuf, xbuf, ybuf, yraw, zbuf, inodd, refl,
           xsend, xrecv, ysend, yrecv, pack,
           c_sem, in_sem, xs_sem, xr_sem, ys_sem, yr_sem):
    def load(arr, part):
        planes = pl.ds(part * (NX // PARTS), NX // PARTS)
        return pltpu.make_async_copy((src_hbm, sig_hbm)[arr].at[planes], inbuf.at[arr, planes], in_sem.at[arr, part])

    coefs = [pltpu.make_async_copy(far, near, c_sem.at[k]) for k, (far, near) in enumerate(
        zip((cx_hbm, cy_hbm, cz_hbm, wt_hbm), (cx_ref, cy_ref, cz_ref, wt_ref)))]
    for one in coefs:
        one.start()
    for part in range(PARTS):
        for arr in range(2):
            load(arr, part).start()

    dx = lax.axis_index("x")
    dy = lax.axis_index("y")
    has_left, has_right = dx > 0, dx < 3
    odd_x = (dx & 1) == 1
    trip_left = jnp.where(odd_x, T_NEAR, T_FAR)
    trip_right = jnp.where(odd_x, T_FAR, T_NEAR)
    lane = lax.broadcasted_iota(jnp.int32, (8, 128), 1)
    subl = lax.broadcasted_iota(jnp.int32, (8, 128), 0)
    oct_id = lane // 16
    oct_y = (oct_id // 2) % 2
    patch_y = lane - 16 * oct_id
    zero = jnp.zeros((8, 128), F32)
    low_half = lane < 64
    first_y, last_y = patch_y == 0, patch_y == 15

    lag_xm, lag_xp = pick(LAG_X[:4][::-1], dx), pick(LAG_X[4:], dx)
    lag_ym, lag_yp = pick(LAG_Y[:2][::-1], dy), pick(LAG_Y[2:], dy)
    lag_oct = jnp.where(lane >= 64, lag_xp, lag_xm) + jnp.where(oct_y == 1, lag_yp, lag_ym)
    lag_lane = patch_y + lag_oct
    hbuf[...] = lax.rem(2 * lag_lane + subl, 2 * NB)
    turn = lax.rem(lag_lane, NB)
    turn_bits = [(turn >> bit) & 1 == 1 for bit in range(5)]

    for k in range(9 * FACES // 8 + 1):
        xbuf[tile(k), :] = zero
    for k in range(FACES):
        ybuf[k] = zero
    for k in range(12):
        yraw[k] = zero
    for k in CELLS:
        zbuf[k] = zero
    inodd[...] = zero
    refl[...] = zero
    for k in range(4):
        for j in range(2 * U):
            pack[k, j] = zero

    @pl.loop(0, RING)
    def _(k):
        for side in range(2):
            for q in range(SLOTS * 3 // 8):
                xrecv[side, k, tile(q), :] = zero
            for r in range(U):
                yrecv[k, r] = zero

    barrier = pltpu.get_barrier_semaphore()

    @pl.when(has_left)
    def _():
        pl.semaphore_signal(barrier, inc=1, device_id={"x": dx - 1}, device_id_type=MESH)

    @pl.when(has_right)
    def _():
        pl.semaphore_signal(barrier, inc=1, device_id={"x": dx + 1}, device_id_type=MESH)

    pl.semaphore_signal(barrier, inc=1, device_id={"y": 1 - dy}, device_id_type=MESH)

    for one in coefs:
        one.wait()
    for pos in range(5):
        col = jnp.ones((8, 128), F32) if pos == 0 else zero
        for m in range(ND):
            two_x, two_y, two_z = 2.0 * cx_ref[m], 2.0 * cy_ref[m], 2.0 * cz_ref[m]
            val = (two_x + two_y + two_z, 2.0 * two_x, 2.0 * two_y, 2.0 * two_z, wt_ref[m])[pos]
            col = jnp.where(lane == m + 1, val, col)
        ctab[pos] = col
        cbuf[pos] = jnp.ones((8, 128), F32) if pos == 0 else zero

    cols = [ctab[pos] for pos in range(5)]

    @pl.loop(0, ntab.shape[1] // 256)
    def _(k):
        for part in range(32):
            first = 256 * k + 8 * part
            c_idx = jnp.clip((((first + subl - lag_oct) * 1311) >> 15) + 1, 0, ND + 1)
            for pos in range(5):
                ntab[pos, pl.ds(first, 8), :] = jnp.take_along_axis(cols[pos], c_idx, axis=1)

    mirror = (71 - lane) & 127
    tail = lane < 72

    for part in range(PARTS):
        for arr in range(2):
            load(arr, part).wait()

        @pl.loop(part * (NX // PARTS), (part + 1) * (NX // PARTS), step=4)
        def _(first):
            for x in (first + k for k in range(4)):
                for arr in range(2):
                    for yt in range(NY // 8):
                        rows = tile(yt)
                        half_a = inbuf[arr, x, rows, pl.ds(0, 128)]
                        nat[arr, 0, x, rows, :] = half_a
                        nat[arr, 1, x, rows, pl.ds(0, 72)] = inbuf[arr, x, rows, pl.ds(128, 72)]
                        half_b = nat[arr, 1, x, rows, :]
                        flip_a = jnp.take_along_axis(half_a, mirror, axis=1)
                        flip_b = jnp.take_along_axis(half_b, mirror, axis=1)
                        nat[arr, 2, x, rows, :] = jnp.where(tail, flip_b, flip_a)
                        nat[arr, 3, x, rows, :] = flip_a

    flip_rows = 7 - subl

    def row_groups(x_patch, i, j):
        for octant in range(8):
            bx, by = octant // 4, (octant // 2) % 2
            x_rel = 3 * x_patch + i
            x_abs = x_rel if bx else NX - 1 - x_rel
            for half in range(2):
                y_abs = (24 * half + j) if by else (26 - 24 * half - j)
                yield octant, half, x_abs, y_abs, by == 0

    def turn_blocks(blocks, step):
        for bit in range(5):
            shift = step * (1 << bit)
            blocks = [jnp.where(turn_bits[bit], blocks[(v - shift) % NB], blocks[v]) for v in range(NB)]
        return blocks

    odd_patch = (subl & 1) == 1

    def block_rows(v, half, odd):
        return pl.ds(FRONT + lax.rem(v + half, NB) * PITCH + (2 * half + odd) + 4 * LEVEL * odd, 8, stride=LEVEL)

    @pl.loop(0, 12)
    def _(trip):
        i, half = trip // 4, trip & 3
        for odd in range(2):
            for j in THREE:
                cell = 3 * i + j
                for arr in range(2):
                    pieces = [[], []]
                    for octant, part, x_abs, y_abs, rev in row_groups(2 * half + odd, i, j):
                        for zh in range(2):
                            kind = zh + (0 if octant % 2 else 2)
                            val = nat[arr, kind, x_abs, pl.ds(y_abs, 8, stride=3), :]
                            if rev:
                                val = jnp.take_along_axis(val, flip_rows, axis=0)
                            pieces[zh].append(val)
                    lo = jnp.concatenate(pieces[0], axis=0).T
                    hi = jnp.concatenate(pieces[1], axis=0).T
                    blocks = [lo[8 * v:8 * v + 8] for v in range(16)] + [hi[8 * v:8 * v + 8] for v in CELLS]
                    blocks = turn_blocks(blocks, 1)
                    for v in range(NB):
                        tab[arr, cell, block_rows(v, half, odd), :] = blocks[v]
                        if arr == 0:
                            flux[cell, block_rows(v, half, odd), :] = zero

    @pl.loop(0, 9)
    def _(cell):
        for arr in range(2):
            for k in range(4):
                first, wrapped = pl.ds(FRONT + LEVEL * k, 8), pl.ds(FRONT + NB * PITCH + LEVEL * k, 8)
                tab[arr, cell, first, :] = jnp.where(odd_patch, tab[arr, cell, wrapped, :], tab[arr, cell, first, :])
        for k in range(4):
            flux[cell, pl.ds(FRONT + LEVEL * k, 8), :] = zero

    pl.semaphore_wait(barrier, has_left.astype(jnp.int32) + has_right.astype(jnp.int32) + 1)

    keep_send = oct_y == 1 - dy
    even_mask, odd_mask = oct_y == dy, oct_y == 1 - dy
    mirror_x, mirror_y = dx == 0, dy == 0
    has = (has_left, has_right, True)
    trips = (trip_left, trip_right, T_Y)

    def copy(kind, n, count=1):
        slot, here, batch = (n + 1 + trips[kind]) & (RING - 1), n & (NSEND - 1), (n >> 3) & 1
        if count > 1:
            here, slot = pl.ds(8 * batch, count), pl.ds(0, count)
        if kind == 2:
            return pltpu.make_async_remote_copy(
                src_ref=ysend.at[here], dst_ref=yrecv.at[slot], send_sem=ys_sem.at[batch],
                recv_sem=yr_sem.at[0 if count > 1 else slot], device_id={"y": 1 - dy}, device_id_type=MESH)
        return pltpu.make_async_remote_copy(
            src_ref=xsend.at[here], dst_ref=xrecv.at[kind, slot], send_sem=xs_sem.at[kind, batch],
            recv_sem=xr_sem.at[kind, 0 if count > 1 else slot],
            device_id={"x": dx - 1 if kind == 0 else dx + 1}, device_id_type=MESH)

    def arrival(kind, n):
        slot = n & (RING - 1)
        if kind == 2:
            return pltpu.make_async_remote_copy(
                src_ref=ysend.at[0], dst_ref=yrecv.at[slot], send_sem=ys_sem.at[0], recv_sem=yr_sem.at[slot],
                device_id={"y": dy}, device_id_type=MESH)
        return pltpu.make_async_remote_copy(
            src_ref=xsend.at[0], dst_ref=xrecv.at[kind, slot], send_sem=xs_sem.at[kind, 0],
            recv_sem=xr_sem.at[kind, slot], device_id={"x": dx}, device_id_type=MESH)

    def when(cond, act):
        if cond is True:
            act()
        else:
            pl.when(cond)(act)

    def both(one, two):
        return two if one is True else (one if two is True else one & two)

    def next_turn(turn_now):
        return jnp.where(turn_now == NB - 1, 0, turn_now + 1)

    senders = (has_right, has_left, True)
    delays = (trip_right, trip_left, T_Y)

    def block(n, turn_now):
        here = n & (NSEND - 1)
        slot = n & (RING - 1)
        now, last, before = n & 3, (n + 3) & 3, (n + 2) & 3

        outs = [xbuf[pl.ds(72 * q + 8, 8, stride=9), :] for q in range(3 * U)]
        for kind in THREE:
            when(both(senders[kind], n > delays[kind]), lambda kind=kind: arrival(kind, n).wait_recv())

        edges = []
        for q in range(3 * U):
            rows = tile(q)
            from_left = jnp.where(mirror_x, pltpu.roll(outs[q], 64, 1), xrecv[1, slot, rows, :])
            edges.append(jnp.where(low_half, xrecv[0, slot, rows, :], from_left))
        def mirrored(val, shift):
            return jnp.where(mirror_y, pltpu.roll(val, shift, 1), 0.0)

        def incoming(r, odd):
            old = pack[last, 2 * r - 2 + odd] if r else pack[before, 2 * U - 1]
            got = yrecv[slot, r]
            if odd:
                return jnp.where(odd_mask, pltpu.roll(got, 64, 1), mirrored(old, 96))
            return jnp.where(even_mask, got, mirrored(old, 32) if r else refl[...])

        delayed = inodd[...]
        arriving = {0: incoming(0, 0), 1: incoming(0, 1)}
        refl[...] = mirrored(pack[last, 2 * U - 2], 32)

        mains, mixes = {}, {}

        def serve(s, faces):
            group = s // 4
            for i in THREE:
                f = 3 * (s % 4) + i
                spot = SPOTS[f]
                mains[f] = pltpu.roll(faces[i], 1, 1)
                mixed = jnp.where(last_y, faces[i], delayed if group == 2 * U - 1 else arriving[group])
                mixes[PARTNER[f]] = pltpu.roll(mixed, (1 + spot + (16 if group % 2 else 112)) % 128, 1)
                pltpu.store(pack.at[last if group == 2 * U - 1 else now, group], mixes[PARTNER[f]], mask=patch_y == spot)
            for f in [f for f in mains if f in mixes]:
                ybuf[(12 * group + f + 24) % FACES] = jnp.where(first_y, mixes.pop(f), mains.pop(f))

        for s in range(SLOTS - 4, SLOTS):
            serve(s, [yraw[3 * (s + 4 - SLOTS) + i] for i in THREE])

        turns = [turn_now]
        for _ in range(U):
            turns.append(next_turn(turns[-1]))
        z_face = [zbuf[c] for c in CELLS]
        coef = [cbuf[pos] for pos in range(5)]
        for s in range(SLOTS):
            if s % 4 == 0:
                fresh = hbuf[...] == 2 * turns[s // 8] + (s // 4) % 2
                row = pl.ds(U * n + s // 8, 1)
                coef = [jnp.where(fresh, ntab[pos, row, :], coef[pos]) for pos in range(5)]
                asum, ax, ay, az, wt = coef
                z_face = [jnp.where(fresh, 0.0, z_face[c]) for c in CELLS]
            if s == 4:
                for q in range(3 * U):
                    xbuf[pl.ds(72 * q, 8, stride=9), :] = edges[q]
            rows = pl.ds(turns[s // 8] * PITCH + (FRONT + LEVEL * (s % 8)), 8)
            x_face = [xbuf[pl.ds(9 * (3 * s + j), 8), :] for j in THREE]
            y_out = []
            for i in THREE:
                y_face = ybuf[3 * s + i]
                for j in THREE:
                    c = 3 * i + j
                    total = ((tab[0, c, rows, :] + z_face[c]) + x_face[j]) + y_face
                    psi = total * (1.0 / (tab[1, c, rows, :] + asum))
                    x_face[j] = ax * psi - x_face[j]
                    y_face = ay * psi - y_face
                    z_face[c] = az * psi - z_face[c]
                    flux[c, rows, :] = flux[c, rows, :] + wt * psi
                y_out.append(y_face)
            if s % 4 == 0 and s < SLOTS - 8:
                arriving[s // 4 + 2] = incoming(s // 8 + 1, s // 4 % 2)
            if s < SLOTS - 4:
                serve(s, y_out)
            else:
                for i in THREE:
                    yraw[3 * (s + 4 - SLOTS) + i] = y_out[i]
            for j in THREE:
                xbuf[pl.ds(9 * ((3 * s + j + 12) % FACES) + 1, 8), :] = x_face[j]
        for c in CELLS:
            zbuf[c] = z_face[c]
        for pos in range(5):
            cbuf[pos] = coef[pos]
        inodd[...] = arriving[2 * U - 1]
        for q in range(3 * U):
            xsend[here, tile(q), :] = xbuf[pl.ds(72 * q + 8, 8, stride=9), :]
        for r in range(U):
            pair, first = (now, 2 * r - 2) if r else (last, 2 * U - 2)
            ysend[here, r] = jnp.where(keep_send, pack[pair, first], pack[pair, first + 1])
        for kind in (2, 0, 1):
            when(has[kind], lambda kind=kind: copy(kind, n).start())
        return turns[U]

    def batch(first, turn_now):
        for kind in THREE:
            when(both(has[kind], first >= 2), lambda kind=kind: copy(kind, 8 * (first - 2), 8).wait_send())
        return lax.fori_loop(8 * first, jnp.minimum(8 * first + 8, BLOCKS), block, turn_now)

    lax.fori_loop(0, (BLOCKS + 7) // 8, batch, jnp.int32(0))

    @pl.loop(0, 9)
    def _(cell):
        for k in range(4):
            flux[cell, pl.ds(FRONT + NB * PITCH + LEVEL * k, 8), :] = flux[cell, pl.ds(FRONT + LEVEL * k, 8), :]

    @pl.loop(0, 12)
    def _(trip):
        i, half = trip // 4, trip & 3
        for odd in range(2):
            for j in THREE:
                cell = 3 * i + j
                blocks = turn_blocks([flux[cell, block_rows(v, half, odd), :] for v in range(NB)], -1)
                lo = jnp.concatenate(blocks[:16], axis=0).T
                hi = jnp.concatenate(blocks[16:] + [zero] * 7, axis=0).T
                for octant, side, x_abs, y_abs, rev in row_groups(2 * half + odd, i, j):
                    for zh in range(2):
                        val = (lo, hi)[zh][16 * octant + 8 * side:16 * octant + 8 * side + 8]
                        if rev:
                            val = jnp.take_along_axis(val, flip_rows, axis=0)
                        acc[octant, zh, x_abs, pl.ds(y_abs, 8, stride=3), :] = val

    @pl.loop(0, NX, step=4)
    def _(first):
        for x, yt in [(first + k, yt) for k in range(4) for yt in range(NY // 8)]:
            rows = tile(yt)
            (dn_a, up_a), (dn_b, up_b) = [
                [sum(acc[octant, zh, x, rows, :] for octant in range(bz + 2, 8, 2)) + acc[bz, zh, x, rows, :]
                 for bz in range(2)] for zh in range(2)]
            dn_a = jnp.take_along_axis(dn_a, mirror, axis=1)
            dn_b = jnp.take_along_axis(dn_b, mirror, axis=1)
            out_ref[x, rows, pl.ds(0, 128)] = up_a + jnp.where(tail, dn_b, dn_a)
            out_ref[x, rows, pl.ds(128, 72)] = (up_b + dn_a)[:, :72]

    for kind in THREE:
        for first in range(max(0, 8 * ((BLOCKS + 7) // 8 - 2)), BLOCKS, 8):
            when(has[kind], lambda kind=kind, first=first:
                 copy(kind, jnp.int32(first), min(8, BLOCKS - first)).wait_send())
        for late in range(1 + (max(T_NEAR, T_FAR) if kind < 2 else T_Y)):
            when(both(senders[kind], late <= delays[kind]), lambda kind=kind, late=late:
                 arrival(kind, jnp.int32(BLOCKS + late)).wait_recv())


def solution(mesh):
    grid_spec = P(("g", "x"), "y", None)

    def column_sweep(source, sigma_t, cos_x, cos_y, cos_z, weights):
        vmem = pl.BlockSpec(memory_space=pltpu.VMEM)
        return pl.pallas_call(
            kernel,
            out_shape=pltpu.VMEM((NX, NY, NZ), F32),
            in_specs=[pl.BlockSpec(memory_space=pl.ANY)] * 6,
            out_specs=vmem,
            scratch_shapes=[pltpu.SMEM((ND,), F32)] * 4 + [
                pltpu.VMEM((2, NX, NY, NZ), F32),
                pltpu.VMEM((2, 4, NX, NY, 128), F32),
                pltpu.VMEM((2, 9, ROWS, 128), F32),
                pltpu.VMEM((9, ROWS, 128), F32),
                pltpu.VMEM((8, 2, NX, NY, 128), F32),
                pltpu.VMEM((8, 128), jnp.int32),
                pltpu.VMEM((5, 8, 128), F32),
                pltpu.VMEM((5, 256 * pl.cdiv(U * BLOCKS, 256), 128), F32),
                pltpu.VMEM((5, 8, 128), F32),
                pltpu.VMEM((9 * FACES + 8, 128), F32),
                pltpu.VMEM((FACES, 8, 128), F32),
                pltpu.VMEM((12, 8, 128), F32),
                pltpu.VMEM((9, 8, 128), F32),
                pltpu.VMEM((8, 128), F32),
                pltpu.VMEM((8, 128), F32),
                pltpu.VMEM((NSEND, FACES, 128), F32),
                pltpu.VMEM((2, RING, FACES, 128), F32),
                pltpu.VMEM((NSEND, U, 8, 128), F32),
                pltpu.VMEM((RING, U, 8, 128), F32),
                pltpu.VMEM((4, 2 * U, 8, 128), F32),
                pltpu.SemaphoreType.DMA((4,)),
                pltpu.SemaphoreType.DMA((2, PARTS)),
                pltpu.SemaphoreType.DMA((2, 2)),
                pltpu.SemaphoreType.DMA((2, RING)),
                pltpu.SemaphoreType.DMA((2,)),
                pltpu.SemaphoreType.DMA((RING,)),
            ],
            compiler_params=pltpu.CompilerParams(
                collective_id=0, has_side_effects=True, vmem_limit_bytes=60 * 1024 * 1024),
        )(cos_x, cos_y, cos_z, weights, source, sigma_t)

    return jax.shard_map(column_sweep, mesh=mesh, in_specs=(grid_spec, grid_spec, P(), P(), P(), P()),
                         out_specs=grid_spec, check_vma=False)
```

```python
import functools

import jax
import jax.numpy as jnp
from jax import lax
from jax.experimental import pallas as pl
from jax.experimental.pallas import tpu as pltpu
from jax.sharding import PartitionSpec as P

F32 = jnp.float32
MESH = pl.DeviceIdType.MESH
NX, NY, NZ = 24, 48, 200
ND = 10
NB = NZ // 8
VREG = (8, 128)
LEVEL = 12
FRONT = 4 * LEVEL
PITCH = 8 * LEVEL
ROWS = NB * PITCH + 112
U = 2
SLOTS = 8 * U
FACES = 3 * SLOTS
T_NEAR = 3
T_FAR = 8
T_Y = 8
D_XR = U
D_YR = U + 1
RING = 32
NSEND = 16
HOIST = 44
THREE, CELLS = range(3), range(9)
PARTS = 2
SPOTS = [2, 13, 3, 4, 11, 12, 5, 10, 6, 7, 8, 9]
PARTNER = [SPOTS.index(15 - spot) for spot in SPOTS]


def x_lags():
    near, far = U * (T_NEAR + 1), U * (T_FAR + 1)
    hops = [near, far, near, D_XR, near, far, near]
    lags = [0]
    for hop in hops:
        lags.append(lags[-1] + 4 + hop)
    return lags


def y_lags():
    lags = [0]
    for hop in [U * (T_Y + 1) + 1, D_YR, U * (T_Y + 1) + 1]:
        lags.append(lags[-1] + 16 + hop)
    return lags


LAG_X, LAG_Y = x_lags(), y_lags()
STEPS = ND * NB + LAG_X[-1] + LAG_Y[-1] + 4 + 15
BLOCKS = (STEPS + U - 1) // U


def gather(val, spots, axis):
    dims = lax.GatherDimensionNumbers(
        offset_dims=(), collapsed_slice_dims=(axis,), start_index_map=(axis,),
        operand_batching_dims=(1 - axis,), start_indices_batching_dims=(1 - axis,))
    return lax.gather(val, spots, dims, slice_sizes=(1, 1), mode=lax.GatherScatterMode.PROMISE_IN_BOUNDS)


def tile(k):
    return pl.ds(8 * k, 8)


def pick(values, idx):
    out = jnp.int32(values[0])
    for pos in range(1, len(values)):
        out = jnp.where(idx == pos, jnp.int32(values[pos]), out)
    return out


def kernel(cx_hbm, cy_hbm, cz_hbm, wt_hbm, src_hbm, sig_hbm, out_ref,
           cx_ref, cy_ref, cz_ref, wt_ref, inbuf, nat, tab, flux, acc, hbuf, ctab, ntab, cbuf, xbuf, ybuf, yraw, zbuf, inodd, refl,
           xsend, xrecv, ysend, yrecv, pack,
           c_sem, in_sem, xs_sem, xr_sem, ys_sem, yr_sem):
    def load(arr, part):
        planes = pl.ds(part * (NX // PARTS), NX // PARTS)
        return pltpu.make_async_copy((src_hbm, sig_hbm)[arr].at[planes], inbuf.at[arr, planes], in_sem.at[arr, part])

    coefs = [pltpu.make_async_copy(far, near, c_sem.at[k]) for k, (far, near) in enumerate(
        zip((cx_hbm, cy_hbm, cz_hbm, wt_hbm), (cx_ref, cy_ref, cz_ref, wt_ref)))]
    for one in coefs:
        one.start()
    for part in range(PARTS):
        for arr in range(2):
            load(arr, part).start()

    dx = lax.axis_index("x")
    dy = lax.axis_index("y")
    has_left, has_right = dx > 0, dx < 3
    odd_x = (dx & 1) == 1
    trip_left = jnp.where(odd_x, T_NEAR, T_FAR)
    trip_right = jnp.where(odd_x, T_FAR, T_NEAR)
    lane = lax.broadcasted_iota(jnp.int32, VREG, 1)
    subl = lax.broadcasted_iota(jnp.int32, VREG, 0)
    oct_id = lane // 16
    oct_y = (oct_id // 2) % 2
    patch_y = lane - 16 * oct_id
    zero = jnp.zeros(VREG, F32)
    low_half = lane < 64
    first_y, last_y = patch_y == 0, patch_y == 15

    lag_xm, lag_xp = pick(LAG_X[:4][::-1], dx), pick(LAG_X[4:], dx)
    lag_ym, lag_yp = pick(LAG_Y[:2][::-1], dy), pick(LAG_Y[2:], dy)
    lag_oct = jnp.where(lane >= 64, lag_xp, lag_xm) + jnp.where(oct_y == 1, lag_yp, lag_ym)
    lag_lane = patch_y + lag_oct
    hbuf[...] = lax.rem(2 * lag_lane + subl, 2 * NB)
    turn = lax.rem(lag_lane, NB)
    turn_bits = [(turn >> bit) & 1 == 1 for bit in range(5)]

    for k in range(9 * FACES // 8 + 1):
        xbuf[tile(k), :] = zero
    for k in range(FACES):
        ybuf[k] = zero
    for k in range(12):
        yraw[k] = zero
    for k in CELLS:
        zbuf[k] = zero
    inodd[...] = zero
    refl[...] = zero
    for k in range(4):
        for j in range(2 * U):
            pack[k, j] = zero

    @pl.loop(0, RING)
    def _(k):
        for side in range(2):
            for q in range(SLOTS * 3 // 8):
                xrecv[side, k, tile(q), :] = zero
            for r in range(U):
                yrecv[k, r] = zero

    barrier = pltpu.get_barrier_semaphore()

    @pl.when(has_left)
    def _():
        pl.semaphore_signal(barrier, inc=1, device_id={"x": dx - 1}, device_id_type=MESH)

    @pl.when(has_right)
    def _():
        pl.semaphore_signal(barrier, inc=1, device_id={"x": dx + 1}, device_id_type=MESH)

    pl.semaphore_signal(barrier, inc=1, device_id={"y": 1 - dy}, device_id_type=MESH)

    for one in coefs:
        one.wait()
    for pos in range(5):
        col = jnp.ones(VREG, F32) if pos == 0 else zero
        for m in range(ND):
            two_x, two_y, two_z = 2.0 * cx_ref[m], 2.0 * cy_ref[m], 2.0 * cz_ref[m]
            val = (two_x + two_y + two_z, 2.0 * two_x, 2.0 * two_y, 2.0 * two_z, wt_ref[m])[pos]
            col = jnp.where(lane == m + 1, val, col)
        ctab[pos] = col
        cbuf[pos] = jnp.ones(VREG, F32) if pos == 0 else zero

    cols = [ctab[pos] for pos in range(5)]

    @pl.loop(0, ntab.shape[1] // 256)
    def _(k):
        for part in range(32):
            first = 256 * k + 8 * part
            c_idx = jnp.clip((((first + subl - lag_oct) * 1311) >> 15) + 1, 0, ND + 1)[..., None]
            for pos in range(5):
                ntab[pos, pl.ds(first, 8), :] = gather(cols[pos], c_idx, 1)

    mirror = ((71 - lane) & 127)[..., None]
    tail = lane < 72

    for part in range(PARTS):
        for arr in range(2):
            load(arr, part).wait()

        @pl.loop(part * (NX // PARTS), (part + 1) * (NX // PARTS), step=4)
        def _(first):
            for x in (first + k for k in range(4)):
                for arr in range(2):
                    for yt in range(NY // 8):
                        rows = tile(yt)
                        half_a = inbuf[arr, x, rows, pl.ds(0, 128)]
                        nat[arr, 0, x, rows, :] = half_a
                        nat[arr, 1, x, rows, pl.ds(0, 72)] = inbuf[arr, x, rows, pl.ds(128, 72)]
                        half_b = nat[arr, 1, x, rows, :]
                        flip_a = gather(half_a, mirror, 1)
                        flip_b = gather(half_b, mirror, 1)
                        nat[arr, 2, x, rows, :] = jnp.where(tail, flip_b, flip_a)
                        nat[arr, 3, x, rows, :] = flip_a

    flip_rows = (7 - subl)[..., None]

    def row_groups(x_patch, i, j):
        x_up = 3 * x_patch + i
        x_both = (NX - 1 - x_up, x_up)
        for octant in range(8):
            by, x_abs = (octant // 2) % 2, x_both[octant // 4]
            for half in range(2):
                y_abs = (24 * half + j) if by else (26 - 24 * half - j)
                yield octant, half, x_abs, y_abs, by == 0

    def turn_blocks(blocks, step):
        for bit in range(5):
            cut = (-step * (1 << bit)) % NB
            shifted = jnp.concatenate([blocks[cut:], blocks[:cut]], axis=0)
            blocks = jnp.where(jnp.broadcast_to(turn_bits[bit][None], blocks.shape), shifted, blocks)
        return blocks

    odd_patch = (subl & 1) == 1

    def block_rows(half, odd):
        first = (FRONT + half * PITCH) + (2 * half + odd + 4 * LEVEL * odd)
        starts = [first + PITCH * v for v in range(NB)]
        for v in range(NB - 3, NB):
            over = half >= NB - v
            back = NB * PITCH * over if isinstance(half, int) else jnp.where(over, NB * PITCH, 0)
            starts[v] = starts[v] - back
        return [pl.ds(at, 8, stride=LEVEL) for at in starts]

    @pl.loop(0, 6)
    def _(trip):
        i = trip // 2
        for half, odd in [(2 * (trip & 1) + k // 2, k & 1) for k in range(4)]:
            places = block_rows(half, odd)
            for j in THREE:
                cell = 3 * i + j
                for arr in range(2):
                    pieces = [[], []]
                    for octant, part, x_abs, y_abs, rev in row_groups(2 * half + odd, i, j):
                        for zh in range(2):
                            kind = zh + (0 if octant % 2 else 2)
                            val = nat[arr, kind, x_abs, pl.ds(y_abs, 8, stride=3), :]
                            if rev:
                                val = gather(val, flip_rows, 0)
                            pieces[zh].append(val)
                    lo = jnp.concatenate(pieces[0], axis=0).T
                    hi = jnp.concatenate(pieces[1], axis=0).T
                    blocks = jnp.concatenate([lo, hi], axis=0)[:NZ].reshape(NB, 8, 128)
                    blocks = turn_blocks(blocks, 1)
                    for v in range(NB):
                        tab[arr, cell, places[v], :] = blocks[v]
                        if arr == 0:
                            flux[cell, places[v], :] = zero

    @pl.loop(0, 9)
    def _(cell):
        for arr in range(2):
            for k in range(4):
                first, wrapped = pl.ds(FRONT + LEVEL * k, 8), pl.ds(FRONT + NB * PITCH + LEVEL * k, 8)
                tab[arr, cell, first, :] = jnp.where(odd_patch, tab[arr, cell, wrapped, :], tab[arr, cell, first, :])
        for k in range(4):
            flux[cell, pl.ds(FRONT + LEVEL * k, 8), :] = zero

    pl.semaphore_wait(barrier, has_left.astype(jnp.int32) + has_right.astype(jnp.int32) + 1)

    keep_send = oct_y == 1 - dy
    even_mask, odd_mask = oct_y == dy, oct_y == 1 - dy
    mirror_x, mirror_y = dx == 0, dy == 0
    has = (has_left, has_right, True)
    trips = (trip_left, trip_right, T_Y)

    def copy(kind, n, count=1):
        slot, here, batch = (n + 1 + trips[kind]) & (RING - 1), n & (NSEND - 1), (n >> 3) & 1
        if count > 1:
            here, slot = pl.ds(8 * batch, count), pl.ds(0, count)
        if kind == 2:
            return pltpu.make_async_remote_copy(
                src_ref=ysend.at[here], dst_ref=yrecv.at[slot], send_sem=ys_sem.at[batch],
                recv_sem=yr_sem.at[0 if count > 1 else slot], device_id={"y": 1 - dy}, device_id_type=MESH)
        return pltpu.make_async_remote_copy(
            src_ref=xsend.at[here], dst_ref=xrecv.at[kind, slot], send_sem=xs_sem.at[kind, batch],
            recv_sem=xr_sem.at[kind, 0 if count > 1 else slot],
            device_id={"x": dx - 1 if kind == 0 else dx + 1}, device_id_type=MESH)

    def arrival(kind, n):
        slot = n & (RING - 1)
        if kind == 2:
            return pltpu.make_async_remote_copy(
                src_ref=ysend.at[0], dst_ref=yrecv.at[slot], send_sem=ys_sem.at[0], recv_sem=yr_sem.at[slot],
                device_id={"y": dy}, device_id_type=MESH)
        return pltpu.make_async_remote_copy(
            src_ref=xsend.at[0], dst_ref=xrecv.at[kind, slot], send_sem=xs_sem.at[kind, 0],
            recv_sem=xr_sem.at[kind, slot], device_id={"x": dx}, device_id_type=MESH)

    def when(cond, act):
        if cond is True:
            act()
        else:
            pl.when(cond)(act)

    def both(one, two):
        return two if one is True else (one if two is True else one & two)

    def next_turn(turn_now):
        return jnp.where(turn_now == NB - 1, 0, turn_now + 1)

    senders = (has_right, has_left, True)
    delays = (trip_right, trip_left, T_Y)

    def block(n, turn_now):
        here = n & (NSEND - 1)
        slot = n & (RING - 1)
        now, last, before = n & 3, (n + 3) & 3, (n + 2) & 3

        outs = [xbuf[pl.ds(72 * q + 8, 8, stride=9), :] for q in range(3 * U)]
        for kind in THREE:
            when(both(senders[kind], n > delays[kind]), lambda kind=kind: arrival(kind, n).wait_recv())

        edges = []
        for q in range(3 * U):
            rows = tile(q)
            from_left = jnp.where(mirror_x, pltpu.roll(outs[q], 64, 1), xrecv[1, slot, rows, :])
            edges.append(jnp.where(low_half, xrecv[0, slot, rows, :], from_left))
        def mirrored(val, shift):
            return jnp.where(mirror_y, pltpu.roll(val, shift, 1), 0.0)

        def incoming(r, odd):
            old = pack[last, 2 * r - 2 + odd] if r else pack[before, 2 * U - 1]
            got = yrecv[slot, r]
            if odd:
                return jnp.where(odd_mask, pltpu.roll(got, 64, 1), mirrored(old, 96))
            return jnp.where(even_mask, got, mirrored(old, 32) if r else refl[...])

        delayed = inodd[...]
        arriving = {0: incoming(0, 0), 1: incoming(0, 1)}
        refl[...] = mirrored(pack[last, 2 * U - 2], 32)

        mains, mixes = {}, {}

        def serve(s, faces):
            group = s // 4
            for i in THREE:
                f = 3 * (s % 4) + i
                spot = SPOTS[f]
                mains[f] = pltpu.roll(faces[i], 1, 1)
                mixed = jnp.where(last_y, faces[i], delayed if group == 2 * U - 1 else arriving[group])
                mixes[PARTNER[f]] = pltpu.roll(mixed, (1 + spot + (16 if group % 2 else 112)) % 128, 1)
                pltpu.store(pack.at[last if group == 2 * U - 1 else now, group], mixes[PARTNER[f]], mask=patch_y == spot)
            for f in [f for f in mains if f in mixes]:
                ybuf[(12 * group + f + 24) % FACES] = jnp.where(first_y, mixes.pop(f), mains.pop(f))

        for s in range(SLOTS - 4, SLOTS):
            serve(s, [yraw[3 * (s + 4 - SLOTS) + i] for i in THREE])

        turns = [turn_now]
        for _ in range(U):
            turns.append(next_turn(turns[-1]))
        z_face = [zbuf[c] for c in CELLS]
        coef = [cbuf[pos] for pos in range(5)]
        for s in range(SLOTS):
            if s % 4 == 0:
                fresh = hbuf[...] == 2 * turns[s // 8] + (s // 4) % 2
                row = pl.ds(U * n + s // 8, 1)
                coef = [jnp.where(fresh, ntab[pos, row, :], coef[pos]) for pos in range(5)]
                asum, ax, ay, az, wt = coef
                z_face = [jnp.where(fresh, 0.0, z_face[c]) for c in CELLS]
            if s == 4:
                for q in range(3 * U):
                    xbuf[pl.ds(72 * q, 8, stride=9), :] = edges[q]
            rows = pl.ds(turns[s // 8] * PITCH + (FRONT + LEVEL * (s % 8)), 8)
            x_face = [xbuf[pl.ds(9 * (3 * s + j), 8), :] for j in THREE]
            y_out = []
            for i in THREE:
                y_face = ybuf[3 * s + i]
                for j in THREE:
                    c = 3 * i + j
                    total = ((tab[0, c, rows, :] + z_face[c]) + x_face[j]) + y_face
                    psi = total * (1.0 / (tab[1, c, rows, :] + asum))
                    x_face[j] = ax * psi - x_face[j]
                    y_face = ay * psi - y_face
                    z_face[c] = az * psi - z_face[c]
                    flux[c, rows, :] = flux[c, rows, :] + wt * psi
                y_out.append(y_face)
            if s % 4 == 0 and s < SLOTS - 8:
                arriving[s // 4 + 2] = incoming(s // 8 + 1, s // 4 % 2)
            if s < SLOTS - 4:
                serve(s, y_out)
            else:
                for i in THREE:
                    yraw[3 * (s + 4 - SLOTS) + i] = y_out[i]
            for j in THREE:
                xbuf[pl.ds(9 * ((3 * s + j + 12) % FACES) + 1, 8), :] = x_face[j]
        for c in CELLS:
            zbuf[c] = z_face[c]
        for pos in range(5):
            cbuf[pos] = coef[pos]
        inodd[...] = arriving[2 * U - 1]
        for q in range(3 * U):
            xsend[here, tile(q), :] = xbuf[pl.ds(72 * q + 8, 8, stride=9), :]
        for r in range(U):
            pair, first = (now, 2 * r - 2) if r else (last, 2 * U - 2)
            ysend[here, r] = jnp.where(keep_send, pack[pair, first], pack[pair, first + 1])
        for kind in (2, 0, 1):
            when(has[kind], lambda kind=kind: copy(kind, n).start())
        return turns[U]

    def batch(first, turn_now):
        for kind in THREE:
            when(both(has[kind], first >= 2), lambda kind=kind: copy(kind, 8 * (first - 2), 8).wait_send())
        return lax.fori_loop(8 * first, jnp.minimum(8 * first + 8, BLOCKS), block, turn_now)

    lax.fori_loop(0, (BLOCKS + 7) // 8, batch, jnp.int32(0))

    @pl.loop(0, 9)
    def _(cell):
        for k in range(4):
            flux[cell, pl.ds(FRONT + NB * PITCH + LEVEL * k, 8), :] = flux[cell, pl.ds(FRONT + LEVEL * k, 8), :]

    @pl.loop(0, 3)
    def _(i):
        for half, odd in [(k // 2, k & 1) for k in range(8)]:
            for j in THREE:
                cell = 3 * i + j
                blocks = jnp.stack([flux[cell, place, :] for place in block_rows(half, odd)])
                blocks = turn_blocks(blocks, -1).reshape(NZ, 128)
                lo = blocks[:128].T
                hi = jnp.concatenate([blocks[128:], jnp.zeros((56, 128), F32)], axis=0).T
                for octant, side, x_abs, y_abs, rev in row_groups(2 * half + odd, i, j):
                    for zh in range(2):
                        val = (lo, hi)[zh][16 * octant + 8 * side:16 * octant + 8 * side + 8]
                        if rev:
                            val = gather(val, flip_rows, 0)
                        acc[octant, zh, x_abs, pl.ds(y_abs, 8, stride=3), :] = val

    @pl.loop(0, NX, step=4)
    def _(first):
        for x, yt in [(first + k, yt) for k in range(4) for yt in range(NY // 8)]:
            rows = tile(yt)
            (dn_a, up_a), (dn_b, up_b) = [
                [sum(acc[octant, zh, x, rows, :] for octant in range(bz + 2, 8, 2)) + acc[bz, zh, x, rows, :]
                 for bz in range(2)] for zh in range(2)]
            dn_a = gather(dn_a, mirror, 1)
            dn_b = gather(dn_b, mirror, 1)
            out_ref[x, rows, pl.ds(0, 128)] = up_a + jnp.where(tail, dn_b, dn_a)
            out_ref[x, rows, pl.ds(128, 72)] = (up_b + dn_a)[:, :72]

    for kind in THREE:
        for first in range(max(0, 8 * ((BLOCKS + 7) // 8 - 2)), BLOCKS, 8):
            when(has[kind], lambda kind=kind, first=first:
                 copy(kind, jnp.int32(first), min(8, BLOCKS - first)).wait_send())
        for late in range(1 + (max(T_NEAR, T_FAR) if kind < 2 else T_Y)):
            when(both(senders[kind], late <= delays[kind]), lambda kind=kind, late=late:
                 arrival(kind, jnp.int32(BLOCKS + late)).wait_recv())


def solution(mesh):
    grid_spec = P(("g", "x"), "y", None)

    def column_sweep(source, sigma_t, cos_x, cos_y, cos_z, weights):
        vmem = pl.BlockSpec(memory_space=pltpu.VMEM)
        return pl.pallas_call(
            kernel,
            out_shape=pltpu.VMEM((NX, NY, NZ), F32),
            in_specs=[pl.BlockSpec(memory_space=pl.ANY)] * 6,
            out_specs=vmem,
            scratch_shapes=[pltpu.SMEM((ND,), F32)] * 4 + [
                pltpu.VMEM((2, NX, NY, NZ), F32),
                pltpu.VMEM((2, 4, NX, NY, 128), F32),
                pltpu.VMEM((2, 9, ROWS, 128), F32),
                pltpu.VMEM((9, ROWS, 128), F32),
                pltpu.VMEM((8, 2, NX, NY, 128), F32),
                pltpu.VMEM((8, 128), jnp.int32),
                pltpu.VMEM((5, 8, 128), F32),
                pltpu.VMEM((5, 256 * pl.cdiv(U * BLOCKS, 256), 128), F32),
                pltpu.VMEM((5, 8, 128), F32),
                pltpu.VMEM((9 * FACES + 8, 128), F32),
                pltpu.VMEM((FACES, 8, 128), F32),
                pltpu.VMEM((12, 8, 128), F32),
                pltpu.VMEM((9, 8, 128), F32),
                pltpu.VMEM(VREG, F32),
                pltpu.VMEM(VREG, F32),
                pltpu.VMEM((NSEND, FACES, 128), F32),
                pltpu.VMEM((2, RING, FACES, 128), F32),
                pltpu.VMEM((NSEND, U, 8, 128), F32),
                pltpu.VMEM((RING, U, 8, 128), F32),
                pltpu.VMEM((4, 2 * U, 8, 128), F32),
                pltpu.SemaphoreType.DMA((4,)),
                pltpu.SemaphoreType.DMA((2, PARTS)),
                pltpu.SemaphoreType.DMA((2, 2)),
                pltpu.SemaphoreType.DMA((2, RING)),
                pltpu.SemaphoreType.DMA((2,)),
                pltpu.SemaphoreType.DMA((RING,)),
            ],
            compiler_params=pltpu.CompilerParams(
                collective_id=0, has_side_effects=True, vmem_limit_bytes=60 * 1024 * 1024),
        )(cos_x, cos_y, cos_z, weights, source, sigma_t)

    return jax.shard_map(column_sweep, mesh=mesh, in_specs=(grid_spec, grid_spec, P(), P(), P(), P()),
                         out_specs=grid_spec, check_vma=False)
```

```python
import functools

import jax
import jax.numpy as jnp
from jax import lax
from jax.experimental import pallas as pl
from jax.experimental.pallas import tpu as pltpu
from jax.sharding import PartitionSpec as P

F32 = jnp.float32
MESH = pl.DeviceIdType.MESH
NX, NY, NZ = 24, 48, 200
ND = 10
NB = NZ // 8
VREG = (8, 128)
LEVEL = 12
FRONT = 4 * LEVEL
PITCH = 8 * LEVEL
ROWS = NB * PITCH + 112
U = 2
SLOTS = 8 * U
FACES = 3 * SLOTS
T_NEAR = 3
T_FAR = 8
T_Y = 8
D_XR = U
D_YR = U + 1
RING = 32
NSEND = 16
HOIST = 44
THREE, CELLS = range(3), range(9)
PARTS = 2
SPOTS = [2, 13, 3, 4, 11, 12, 5, 10, 6, 7, 8, 9]
PARTNER = [SPOTS.index(15 - spot) for spot in SPOTS]


def x_lags():
    near, far = U * (T_NEAR + 1), U * (T_FAR + 1)
    hops = [near, far, near, D_XR, near, far, near]
    lags = [0]
    for hop in hops:
        lags.append(lags[-1] + 4 + hop)
    return lags


def y_lags():
    lags = [0]
    for hop in [U * (T_Y + 1) + 1, D_YR, U * (T_Y + 1) + 1]:
        lags.append(lags[-1] + 16 + hop)
    return lags


LAG_X, LAG_Y = x_lags(), y_lags()
STEPS = ND * NB + LAG_X[-1] + LAG_Y[-1] + 4 + 15
BLOCKS = (STEPS + U - 1) // U


def gather(val, spots, axis):
    dims = lax.GatherDimensionNumbers(
        offset_dims=(), collapsed_slice_dims=(axis,), start_index_map=(axis,),
        operand_batching_dims=(1 - axis,), start_indices_batching_dims=(1 - axis,))
    return lax.gather(val, spots, dims, slice_sizes=(1, 1), mode=lax.GatherScatterMode.PROMISE_IN_BOUNDS)


def tile(k):
    return pl.ds(8 * k, 8)


def pick(values, idx):
    out = jnp.int32(values[0])
    for pos in range(1, len(values)):
        out = jnp.where(idx == pos, jnp.int32(values[pos]), out)
    return out


def kernel(cx_hbm, cy_hbm, cz_hbm, wt_hbm, src_hbm, sig_hbm, out_ref,
           cx_ref, cy_ref, cz_ref, wt_ref, inbuf, nat, tab, flux, acc, hbuf, ctab, ntab, cbuf, xbuf, ybuf, yraw, zbuf, inodd, refl,
           xsend, xrecv, ysend, yrecv, pack,
           c_sem, in_sem, xs_sem, xr_sem, ys_sem, yr_sem):
    def load(arr, part):
        planes = pl.ds(part * (NX // PARTS), NX // PARTS)
        return pltpu.make_async_copy((src_hbm, sig_hbm)[arr].at[planes], inbuf.at[arr, planes], in_sem.at[arr, part])

    coefs = [pltpu.make_async_copy(far, near, c_sem.at[k]) for k, (far, near) in enumerate(
        zip((cx_hbm, cy_hbm, cz_hbm, wt_hbm), (cx_ref, cy_ref, cz_ref, wt_ref)))]
    for one in coefs:
        one.start()
    for part in range(PARTS):
        for arr in range(2):
            load(arr, part).start()

    dx = lax.axis_index("x")
    dy = lax.axis_index("y")
    has_left, has_right = dx > 0, dx < 3
    odd_x = (dx & 1) == 1
    trip_left = jnp.where(odd_x, T_NEAR, T_FAR)
    trip_right = jnp.where(odd_x, T_FAR, T_NEAR)
    lane = lax.broadcasted_iota(jnp.int32, VREG, 1)
    subl = lax.broadcasted_iota(jnp.int32, VREG, 0)
    oct_id = lane // 16
    oct_y = (oct_id // 2) % 2
    patch_y = lane - 16 * oct_id
    zero = jnp.zeros(VREG, F32)
    low_half = lane < 64
    first_y, last_y = patch_y == 0, patch_y == 15

    lag_xm, lag_xp = pick(LAG_X[:4][::-1], dx), pick(LAG_X[4:], dx)
    lag_ym, lag_yp = pick(LAG_Y[:2][::-1], dy), pick(LAG_Y[2:], dy)
    lag_oct = jnp.where(lane >= 64, lag_xp, lag_xm) + jnp.where(oct_y == 1, lag_yp, lag_ym)
    lag_lane = patch_y + lag_oct
    hbuf[...] = lax.rem(2 * lag_lane + subl, 2 * NB)
    turn = lax.rem(lag_lane, NB)
    turn_bits = [(turn >> bit) & 1 == 1 for bit in range(5)]

    for k in range(9 * FACES // 8 + 1):
        xbuf[tile(k), :] = zero
    for k in range(FACES):
        ybuf[k] = zero
    for k in range(12):
        yraw[k] = zero
    for k in CELLS:
        zbuf[k] = zero
    inodd[...] = zero
    refl[...] = zero
    for k in range(4):
        for j in range(2 * U):
            pack[k, j] = zero

    @pl.loop(0, RING)
    def _(k):
        for side in range(2):
            for q in range(SLOTS * 3 // 8):
                xrecv[side, k, tile(q), :] = zero
            for r in range(U):
                yrecv[k, r] = zero

    barrier = pltpu.get_barrier_semaphore()

    @pl.when(has_left)
    def _():
        pl.semaphore_signal(barrier, inc=1, device_id={"x": dx - 1}, device_id_type=MESH)

    @pl.when(has_right)
    def _():
        pl.semaphore_signal(barrier, inc=1, device_id={"x": dx + 1}, device_id_type=MESH)

    pl.semaphore_signal(barrier, inc=1, device_id={"y": 1 - dy}, device_id_type=MESH)

    for one in coefs:
        one.wait()
    for pos in range(5):
        col = jnp.ones(VREG, F32) if pos == 0 else zero
        for m in range(ND):
            two_x, two_y, two_z = 2.0 * cx_ref[m], 2.0 * cy_ref[m], 2.0 * cz_ref[m]
            val = (two_x + two_y + two_z, 2.0 * two_x, 2.0 * two_y, 2.0 * two_z, wt_ref[m])[pos]
            col = jnp.where(lane == m + 1, val, col)
        ctab[pos] = col
        cbuf[pos] = jnp.ones(VREG, F32) if pos == 0 else zero

    cols = [ctab[pos] for pos in range(5)]

    @pl.loop(0, ntab.shape[1] // 256)
    def _(k):
        for part in range(32):
            first = 256 * k + 8 * part
            c_idx = jnp.clip((((first + subl - lag_oct) * 1311) >> 15) + 1, 0, ND + 1)[..., None]
            for pos in range(5):
                ntab[pos, pl.ds(first, 8), :] = gather(cols[pos], c_idx, 1)

    mirror = ((71 - lane) & 127)[..., None]
    tail = lane < 72

    for part in range(PARTS):
        for arr in range(2):
            load(arr, part).wait()

        @pl.loop(part * (NX // PARTS), (part + 1) * (NX // PARTS), step=4)
        def _(first):
            for x in (first + k for k in range(4)):
                for arr in range(2):
                    for yt in range(NY // 8):
                        rows = tile(yt)
                        half_a = inbuf[arr, x, rows, pl.ds(0, 128)]
                        nat[arr, 0, x, rows, :] = half_a
                        nat[arr, 1, x, rows, pl.ds(0, 72)] = inbuf[arr, x, rows, pl.ds(128, 72)]
                        half_b = nat[arr, 1, x, rows, :]
                        flip_a = gather(half_a, mirror, 1)
                        flip_b = gather(half_b, mirror, 1)
                        nat[arr, 2, x, rows, :] = jnp.where(tail, flip_b, flip_a)
                        nat[arr, 3, x, rows, :] = flip_a

    flip_rows = (7 - subl)[..., None]

    def row_groups(x_patch, i, j):
        x_up = 3 * x_patch + i
        x_both = (NX - 1 - x_up, x_up)
        for octant in range(8):
            by, x_abs = (octant // 2) % 2, x_both[octant // 4]
            for half in range(2):
                y_abs = (24 * half + j) if by else (26 - 24 * half - j)
                yield octant, half, x_abs, y_abs, by == 0

    def turn_blocks(blocks, step):
        for bit in range(5):
            cut = (-step * (1 << bit)) % NB
            shifted = jnp.concatenate([blocks[cut:], blocks[:cut]], axis=0)
            blocks = jnp.where(jnp.broadcast_to(turn_bits[bit][None], blocks.shape), shifted, blocks)
        return blocks

    odd_patch = (subl & 1) == 1

    def block_rows(half, odd):
        blocks = [(v + half) % NB if isinstance(half, int) else lax.rem(v + half, NB) for v in range(NB)]
        return [pl.ds(block * PITCH + (FRONT + 2 * half + odd + 4 * LEVEL * odd), 8, stride=LEVEL) for block in blocks]

    @pl.loop(0, 6)
    def _(trip):
        i = trip // 2
        for half, odd in [(2 * (trip & 1) + k // 2, k & 1) for k in range(4)]:
            places = block_rows(half, odd)
            for j in THREE:
                cell = 3 * i + j
                for arr in range(2):
                    pieces = [[], []]
                    for octant, part, x_abs, y_abs, rev in row_groups(2 * half + odd, i, j):
                        for zh in range(2):
                            kind = zh + (0 if octant % 2 else 2)
                            val = nat[arr, kind, x_abs, pl.ds(y_abs, 8, stride=3), :]
                            if rev:
                                val = gather(val, flip_rows, 0)
                            pieces[zh].append(val)
                    lo = jnp.concatenate(pieces[0], axis=0).T
                    hi = jnp.concatenate(pieces[1], axis=0).T
                    blocks = jnp.concatenate([lo, hi], axis=0)[:NZ].reshape(NB, 8, 128)
                    blocks = turn_blocks(blocks, 1)
                    for v in range(NB):
                        tab[arr, cell, places[v], :] = blocks[v]
                        if arr == 0:
                            flux[cell, places[v], :] = zero

    @pl.loop(0, 9)
    def _(cell):
        for arr in range(2):
            for k in range(4):
                first, wrapped = pl.ds(FRONT + LEVEL * k, 8), pl.ds(FRONT + NB * PITCH + LEVEL * k, 8)
                tab[arr, cell, first, :] = jnp.where(odd_patch, tab[arr, cell, wrapped, :], tab[arr, cell, first, :])
        for k in range(4):
            flux[cell, pl.ds(FRONT + LEVEL * k, 8), :] = zero

    pl.semaphore_wait(barrier, has_left.astype(jnp.int32) + has_right.astype(jnp.int32) + 1)

    keep_send = oct_y == 1 - dy
    even_mask, odd_mask = oct_y == dy, oct_y == 1 - dy
    mirror_x, mirror_y = dx == 0, dy == 0
    has = (has_left, has_right, True)
    trips = (trip_left, trip_right, T_Y)

    def copy(kind, n, count=1):
        slot, here, batch = (n + 1 + trips[kind]) & (RING - 1), n & (NSEND - 1), (n >> 3) & 1
        if count > 1:
            here, slot = pl.ds(8 * batch, count), pl.ds(0, count)
        if kind == 2:
            return pltpu.make_async_remote_copy(
                src_ref=ysend.at[here], dst_ref=yrecv.at[slot], send_sem=ys_sem.at[batch],
                recv_sem=yr_sem.at[0 if count > 1 else slot], device_id={"y": 1 - dy}, device_id_type=MESH)
        return pltpu.make_async_remote_copy(
            src_ref=xsend.at[here], dst_ref=xrecv.at[kind, slot], send_sem=xs_sem.at[kind, batch],
            recv_sem=xr_sem.at[kind, 0 if count > 1 else slot],
            device_id={"x": dx - 1 if kind == 0 else dx + 1}, device_id_type=MESH)

    def arrival(kind, n):
        slot = n & (RING - 1)
        if kind == 2:
            return pltpu.make_async_remote_copy(
                src_ref=ysend.at[0], dst_ref=yrecv.at[slot], send_sem=ys_sem.at[0], recv_sem=yr_sem.at[slot],
                device_id={"y": dy}, device_id_type=MESH)
        return pltpu.make_async_remote_copy(
            src_ref=xsend.at[0], dst_ref=xrecv.at[kind, slot], send_sem=xs_sem.at[kind, 0],
            recv_sem=xr_sem.at[kind, slot], device_id={"x": dx}, device_id_type=MESH)

    def when(cond, act):
        if cond is True:
            act()
        else:
            pl.when(cond)(act)

    def both(one, two):
        return two if one is True else (one if two is True else one & two)

    def next_turn(turn_now):
        return jnp.where(turn_now == NB - 1, 0, turn_now + 1)

    senders = (has_right, has_left, True)
    delays = (trip_right, trip_left, T_Y)

    def block(n, turn_now):
        here = n & (NSEND - 1)
        slot = n & (RING - 1)
        now, last, before = n & 3, (n + 3) & 3, (n + 2) & 3

        outs = [xbuf[pl.ds(72 * q + 8, 8, stride=9), :] for q in range(3 * U)]
        for kind in THREE:
            when(both(senders[kind], n > delays[kind]), lambda kind=kind: arrival(kind, n).wait_recv())

        edges = []
        for q in range(3 * U):
            rows = tile(q)
            from_left = jnp.where(mirror_x, pltpu.roll(outs[q], 64, 1), xrecv[1, slot, rows, :])
            edges.append(jnp.where(low_half, xrecv[0, slot, rows, :], from_left))
        def mirrored(val, shift):
            return jnp.where(mirror_y, pltpu.roll(val, shift, 1), 0.0)

        def incoming(r, odd):
            old = pack[last, 2 * r - 2 + odd] if r else pack[before, 2 * U - 1]
            got = yrecv[slot, r]
            if odd:
                return jnp.where(odd_mask, pltpu.roll(got, 64, 1), mirrored(old, 96))
            return jnp.where(even_mask, got, mirrored(old, 32) if r else refl[...])

        delayed = inodd[...]
        arriving = {0: incoming(0, 0), 1: incoming(0, 1)}
        refl[...] = mirrored(pack[last, 2 * U - 2], 32)

        mains, mixes = {}, {}

        def serve(s, faces):
            group = s // 4
            for i in THREE:
                f = 3 * (s % 4) + i
                spot = SPOTS[f]
                mains[f] = pltpu.roll(faces[i], 1, 1)
                mixed = jnp.where(last_y, faces[i], delayed if group == 2 * U - 1 else arriving[group])
                mixes[PARTNER[f]] = pltpu.roll(mixed, (1 + spot + (16 if group % 2 else 112)) % 128, 1)
                pltpu.store(pack.at[last if group == 2 * U - 1 else now, group], mixes[PARTNER[f]], mask=patch_y == spot)
            for f in [f for f in mains if f in mixes]:
                ybuf[(12 * group + f + 24) % FACES] = jnp.where(first_y, mixes.pop(f), mains.pop(f))

        for s in range(SLOTS - 4, SLOTS):
            serve(s, [yraw[3 * (s + 4 - SLOTS) + i] for i in THREE])

        turns = [turn_now]
        for _ in range(U):
            turns.append(next_turn(turns[-1]))
        z_face = [zbuf[c] for c in CELLS]
        coef = [cbuf[pos] for pos in range(5)]
        for s in range(SLOTS):
            if s % 4 == 0:
                fresh = hbuf[...] == 2 * turns[s // 8] + (s // 4) % 2
                row = pl.ds(U * n + s // 8, 1)
                coef = [jnp.where(fresh, ntab[pos, row, :], coef[pos]) for pos in range(5)]
                asum, ax, ay, az, wt = coef
                z_face = [jnp.where(fresh, 0.0, z_face[c]) for c in CELLS]
            if s == 4:
                for q in range(3 * U):
                    xbuf[pl.ds(72 * q, 8, stride=9), :] = edges[q]
            rows = pl.ds(turns[s // 8] * PITCH + (FRONT + LEVEL * (s % 8)), 8)
            x_face = [xbuf[pl.ds(9 * (3 * s + j), 8), :] for j in THREE]
            y_out = []
            for i in THREE:
                y_face = ybuf[3 * s + i]
                for j in THREE:
                    c = 3 * i + j
                    total = ((tab[0, c, rows, :] + z_face[c]) + x_face[j]) + y_face
                    psi = total * (1.0 / (tab[1, c, rows, :] + asum))
                    x_face[j] = ax * psi - x_face[j]
                    y_face = ay * psi - y_face
                    z_face[c] = az * psi - z_face[c]
                    flux[c, rows, :] = flux[c, rows, :] + wt * psi
                y_out.append(y_face)
            if s % 4 == 0 and s < SLOTS - 8:
                arriving[s // 4 + 2] = incoming(s // 8 + 1, s // 4 % 2)
            if s < SLOTS - 4:
                serve(s, y_out)
            else:
                for i in THREE:
                    yraw[3 * (s + 4 - SLOTS) + i] = y_out[i]
            for j in THREE:
                xbuf[pl.ds(9 * ((3 * s + j + 12) % FACES) + 1, 8), :] = x_face[j]
        for c in CELLS:
            zbuf[c] = z_face[c]
        for pos in range(5):
            cbuf[pos] = coef[pos]
        inodd[...] = arriving[2 * U - 1]
        for q in range(3 * U):
            xsend[here, tile(q), :] = xbuf[pl.ds(72 * q + 8, 8, stride=9), :]
        for r in range(U):
            pair, first = (now, 2 * r - 2) if r else (last, 2 * U - 2)
            ysend[here, r] = jnp.where(keep_send, pack[pair, first], pack[pair, first + 1])
        for kind in (2, 0, 1):
            when(has[kind], lambda kind=kind: copy(kind, n).start())
        return turns[U]

    def batch(first, turn_now):
        for kind in THREE:
            when(both(has[kind], first >= 2), lambda kind=kind: copy(kind, 8 * (first - 2), 8).wait_send())
        return lax.fori_loop(8 * first, jnp.minimum(8 * first + 8, BLOCKS), block, turn_now)

    lax.fori_loop(0, (BLOCKS + 7) // 8, batch, jnp.int32(0))

    @pl.loop(0, 9)
    def _(cell):
        for k in range(4):
            flux[cell, pl.ds(FRONT + NB * PITCH + LEVEL * k, 8), :] = flux[cell, pl.ds(FRONT + LEVEL * k, 8), :]

    @pl.loop(0, 3)
    def _(i):
        for half, odd in [(k // 2, k & 1) for k in range(8)]:
            for j in THREE:
                cell = 3 * i + j
                blocks = jnp.stack([flux[cell, place, :] for place in block_rows(half, odd)])
                blocks = turn_blocks(blocks, -1).reshape(NZ, 128)
                lo = blocks[:128].T
                hi = jnp.concatenate([blocks[128:], jnp.zeros((56, 128), F32)], axis=0).T
                for octant, side, x_abs, y_abs, rev in row_groups(2 * half + odd, i, j):
                    for zh in range(2):
                        val = (lo, hi)[zh][16 * octant + 8 * side:16 * octant + 8 * side + 8]
                        if rev:
                            val = gather(val, flip_rows, 0)
                        acc[octant, zh, x_abs, pl.ds(y_abs, 8, stride=3), :] = val

    @pl.loop(0, NX, step=4)
    def _(first):
        for x, yt in [(first + k, yt) for k in range(4) for yt in range(NY // 8)]:
            rows = tile(yt)
            (dn_a, up_a), (dn_b, up_b) = [
                [sum(acc[octant, zh, x, rows, :] for octant in range(bz + 2, 8, 2)) + acc[bz, zh, x, rows, :]
                 for bz in range(2)] for zh in range(2)]
            dn_a = gather(dn_a, mirror, 1)
            dn_b = gather(dn_b, mirror, 1)
            out_ref[x, rows, pl.ds(0, 128)] = up_a + jnp.where(tail, dn_b, dn_a)
            out_ref[x, rows, pl.ds(128, 72)] = (up_b + dn_a)[:, :72]

    for kind in THREE:
        for first in range(max(0, 8 * ((BLOCKS + 7) // 8 - 2)), BLOCKS, 8):
            when(has[kind], lambda kind=kind, first=first:
                 copy(kind, jnp.int32(first), min(8, BLOCKS - first)).wait_send())
        for late in range(1 + (max(T_NEAR, T_FAR) if kind < 2 else T_Y)):
            when(both(senders[kind], late <= delays[kind]), lambda kind=kind, late=late:
                 arrival(kind, jnp.int32(BLOCKS + late)).wait_recv())


def solution(mesh):
    grid_spec = P(("g", "x"), "y", None)

    def column_sweep(source, sigma_t, cos_x, cos_y, cos_z, weights):
        vmem = pl.BlockSpec(memory_space=pltpu.VMEM)
        return pl.pallas_call(
            kernel,
            out_shape=pltpu.VMEM((NX, NY, NZ), F32),
            in_specs=[pl.BlockSpec(memory_space=pl.ANY)] * 6,
            out_specs=vmem,
            scratch_shapes=[pltpu.SMEM((ND,), F32)] * 4 + [
                pltpu.VMEM((2, NX, NY, NZ), F32),
                pltpu.VMEM((2, 4, NX, NY, 128), F32),
                pltpu.VMEM((2, 9, ROWS, 128), F32),
                pltpu.VMEM((9, ROWS, 128), F32),
                pltpu.VMEM((8, 2, NX, NY, 128), F32),
                pltpu.VMEM((8, 128), jnp.int32),
                pltpu.VMEM((5, 8, 128), F32),
                pltpu.VMEM((5, 256 * pl.cdiv(U * BLOCKS, 256), 128), F32),
                pltpu.VMEM((5, 8, 128), F32),
                pltpu.VMEM((9 * FACES + 8, 128), F32),
                pltpu.VMEM((FACES, 8, 128), F32),
                pltpu.VMEM((12, 8, 128), F32),
                pltpu.VMEM((9, 8, 128), F32),
                pltpu.VMEM(VREG, F32),
                pltpu.VMEM(VREG, F32),
                pltpu.VMEM((NSEND, FACES, 128), F32),
                pltpu.VMEM((2, RING, FACES, 128), F32),
                pltpu.VMEM((NSEND, U, 8, 128), F32),
                pltpu.VMEM((RING, U, 8, 128), F32),
                pltpu.VMEM((4, 2 * U, 8, 128), F32),
                pltpu.SemaphoreType.DMA((4,)),
                pltpu.SemaphoreType.DMA((2, PARTS)),
                pltpu.SemaphoreType.DMA((2, 2)),
                pltpu.SemaphoreType.DMA((2, RING)),
                pltpu.SemaphoreType.DMA((2,)),
                pltpu.SemaphoreType.DMA((RING,)),
            ],
            compiler_params=pltpu.CompilerParams(
                collective_id=0, has_side_effects=True, vmem_limit_bytes=60 * 1024 * 1024),
        )(cos_x, cos_y, cos_z, weights, source, sigma_t)

    return jax.shard_map(column_sweep, mesh=mesh, in_specs=(grid_spec, grid_spec, P(), P(), P(), P()),
                         out_specs=grid_spec, check_vma=False)
```

```python
import functools

import jax
import jax.numpy as jnp
from jax import lax
from jax.experimental import pallas as pl
from jax.experimental.pallas import tpu as pltpu
from jax.sharding import PartitionSpec as P

F32 = jnp.float32
MESH = pl.DeviceIdType.MESH
NX, NY, NZ = 24, 48, 200
ND = 10
NB = NZ // 8
VREG = (8, 128)
LEVEL = 12
FRONT = 4 * LEVEL
PITCH = 8 * LEVEL
ROWS = NB * PITCH + 112
U = 2
SLOTS = 8 * U
FACES = 3 * SLOTS
T_NEAR = 3
T_FAR = 8
T_Y = 8
D_XR = U
D_YR = U + 1
RING = 32
NSEND = 16
HOIST = 44
THREE, CELLS = range(3), range(9)
PARTS = 2
SPOTS = [2, 13, 3, 4, 11, 12, 5, 10, 6, 7, 8, 9]
PARTNER = [SPOTS.index(15 - spot) for spot in SPOTS]


def x_lags():
    near, far = U * (T_NEAR + 1), U * (T_FAR + 1)
    hops = [near, far, near, D_XR, near, far, near]
    lags = [0]
    for hop in hops:
        lags.append(lags[-1] + 4 + hop)
    return lags


def y_lags():
    lags = [0]
    for hop in [U * (T_Y + 1) + 1, D_YR, U * (T_Y + 1) + 1]:
        lags.append(lags[-1] + 16 + hop)
    return lags


LAG_X, LAG_Y = x_lags(), y_lags()
STEPS = ND * NB + LAG_X[-1] + LAG_Y[-1] + 4 + 15
BLOCKS = (STEPS + U - 1) // U


def gather(val, spots, axis):
    dims = lax.GatherDimensionNumbers(
        offset_dims=(), collapsed_slice_dims=(axis,), start_index_map=(axis,),
        operand_batching_dims=(1 - axis,), start_indices_batching_dims=(1 - axis,))
    return lax.gather(val, spots, dims, slice_sizes=(1, 1), mode=lax.GatherScatterMode.PROMISE_IN_BOUNDS)


def tile(k):
    return pl.ds(8 * k, 8)


def pick(values, idx):
    out = jnp.int32(values[0])
    for pos in range(1, len(values)):
        out = jnp.where(idx == pos, jnp.int32(values[pos]), out)
    return out


def kernel(cx_hbm, cy_hbm, cz_hbm, wt_hbm, src_hbm, sig_hbm, out_ref,
           cx_ref, cy_ref, cz_ref, wt_ref, inbuf, nat, tab, flux, acc, hbuf, ctab, ntab, cbuf, xbuf, ybuf, yraw, zbuf, inodd, refl,
           xsend, xrecv, ysend, yrecv, pack,
           c_sem, in_sem, xs_sem, xr_sem, ys_sem, yr_sem):
    def load(arr, part):
        planes = pl.ds(part * (NX // PARTS), NX // PARTS)
        return pltpu.make_async_copy((src_hbm, sig_hbm)[arr].at[planes], inbuf.at[arr, planes], in_sem.at[arr, part])

    coefs = [pltpu.make_async_copy(far, near, c_sem.at[k]) for k, (far, near) in enumerate(
        zip((cx_hbm, cy_hbm, cz_hbm, wt_hbm), (cx_ref, cy_ref, cz_ref, wt_ref)))]
    for one in coefs:
        one.start()
    for part in range(PARTS):
        for arr in range(2):
            load(arr, part).start()

    dx = lax.axis_index("x")
    dy = lax.axis_index("y")
    has_left, has_right = dx > 0, dx < 3
    odd_x = (dx & 1) == 1
    trip_left = jnp.where(odd_x, T_NEAR, T_FAR)
    trip_right = jnp.where(odd_x, T_FAR, T_NEAR)
    lane = lax.broadcasted_iota(jnp.int32, VREG, 1)
    subl = lax.broadcasted_iota(jnp.int32, VREG, 0)
    oct_id = lane // 16
    oct_y = (oct_id // 2) % 2
    patch_y = lane - 16 * oct_id
    zero = jnp.zeros(VREG, F32)
    low_half = lane < 64
    first_y, last_y = patch_y == 0, patch_y == 15

    lag_xm, lag_xp = pick(LAG_X[:4][::-1], dx), pick(LAG_X[4:], dx)
    lag_ym, lag_yp = pick(LAG_Y[:2][::-1], dy), pick(LAG_Y[2:], dy)
    lag_oct = jnp.where(lane >= 64, lag_xp, lag_xm) + jnp.where(oct_y == 1, lag_yp, lag_ym)
    lag_lane = patch_y + lag_oct
    hbuf[...] = lax.rem(2 * lag_lane + subl, 2 * NB)
    turn = lax.rem(lag_lane, NB)
    turn_bits = [(turn >> bit) & 1 == 1 for bit in range(5)]

    for k in range(9 * FACES // 8 + 1):
        xbuf[tile(k), :] = zero
    for k in range(FACES):
        ybuf[k] = zero
    for k in range(12):
        yraw[k] = zero
    for k in CELLS:
        zbuf[k] = zero
    inodd[...] = zero
    refl[...] = zero
    for k in range(4):
        for j in range(2 * U):
            pack[k, j] = zero

    @pl.loop(0, RING)
    def _(k):
        for side in range(2):
            for q in range(SLOTS * 3 // 8):
                xrecv[side, k, tile(q), :] = zero
            for r in range(U):
                yrecv[k, r] = zero

    barrier = pltpu.get_barrier_semaphore()

    @pl.when(has_left)
    def _():
        pl.semaphore_signal(barrier, inc=1, device_id={"x": dx - 1}, device_id_type=MESH)

    @pl.when(has_right)
    def _():
        pl.semaphore_signal(barrier, inc=1, device_id={"x": dx + 1}, device_id_type=MESH)

    pl.semaphore_signal(barrier, inc=1, device_id={"y": 1 - dy}, device_id_type=MESH)

    for one in coefs:
        one.wait()
    for pos in range(5):
        col = jnp.ones(VREG, F32) if pos == 0 else zero
        for m in range(ND):
            two_x, two_y, two_z = 2.0 * cx_ref[m], 2.0 * cy_ref[m], 2.0 * cz_ref[m]
            val = (two_x + two_y + two_z, 2.0 * two_x, 2.0 * two_y, 2.0 * two_z, wt_ref[m])[pos]
            col = jnp.where(lane == m + 1, val, col)
        ctab[pos] = col
        cbuf[pos] = jnp.ones(VREG, F32) if pos == 0 else zero

    cols = [ctab[pos] for pos in range(5)]

    @pl.loop(0, ntab.shape[1] // 256)
    def _(k):
        for part in range(32):
            first = 256 * k + 8 * part
            c_idx = jnp.clip((((first + subl - lag_oct) * 1311) >> 15) + 1, 0, ND + 1)[..., None]
            for pos in range(5):
                ntab[pos, pl.ds(first, 8), :] = gather(cols[pos], c_idx, 1)

    mirror = ((71 - lane) & 127)[..., None]
    tail = lax.broadcasted_iota(jnp.int32, (NY, 128), 1) < 72

    def mirror_plane(val):
        return jnp.concatenate([gather(val[8 * k:8 * k + 8], mirror, 1) for k in range(NY // 8)], axis=0)

    for part in range(PARTS):
        for arr in range(2):
            load(arr, part).wait()

        @pl.loop(part * (NX // PARTS), (part + 1) * (NX // PARTS), step=12)
        def _(first):
            for x in (first + k for k in range(12)):
                for arr in range(2):
                    half_a = inbuf[arr, x, :, pl.ds(0, 128)]
                    nat[arr, 0, x] = half_a
                    nat[arr, 1, x, :, pl.ds(0, 72)] = inbuf[arr, x, :, pl.ds(128, 72)]
                    flip_a, flip_b = mirror_plane(half_a), mirror_plane(nat[arr, 1, x])
                    nat[arr, 2, x] = jnp.where(tail, flip_b, flip_a)
                    nat[arr, 3, x] = flip_a

    flip_rows = (7 - subl)[..., None]

    def row_groups(x_patch, i, j):
        x_up = 3 * x_patch + i
        x_both = (NX - 1 - x_up, x_up)
        for octant in range(8):
            by, x_abs = (octant // 2) % 2, x_both[octant // 4]
            for half in range(2):
                y_abs = (24 * half + j) if by else (26 - 24 * half - j)
                yield octant, half, x_abs, y_abs, by == 0

    def turn_blocks(blocks, step):
        for bit in range(5):
            cut = (-step * (1 << bit)) % NB
            shifted = jnp.concatenate([blocks[cut:], blocks[:cut]], axis=0)
            blocks = jnp.where(jnp.broadcast_to(turn_bits[bit][None], blocks.shape), shifted, blocks)
        return blocks

    odd_patch = (subl & 1) == 1

    def block_rows(half, odd):
        blocks = [(v + half) % NB if isinstance(half, int) else lax.rem(v + half, NB) for v in range(NB)]
        return [pl.ds(block * PITCH + (FRONT + 2 * half + odd + 4 * LEVEL * odd), 8, stride=LEVEL) for block in blocks]

    @pl.loop(0, 6)
    def _(trip):
        i = trip // 2
        for half, odd in [(2 * (trip & 1) + k // 2, k & 1) for k in range(4)]:
            places = block_rows(half, odd)
            for j in THREE:
                cell = 3 * i + j
                for arr in range(2):
                    pieces = [[], []]
                    for octant, part, x_abs, y_abs, rev in row_groups(2 * half + odd, i, j):
                        for zh in range(2):
                            kind = zh + (0 if octant % 2 else 2)
                            val = nat[arr, kind, x_abs, pl.ds(y_abs, 8, stride=3), :]
                            if rev:
                                val = gather(val, flip_rows, 0)
                            pieces[zh].append(val)
                    lo = jnp.concatenate(pieces[0], axis=0).T
                    hi = jnp.concatenate(pieces[1], axis=0).T
                    blocks = jnp.concatenate([lo, hi], axis=0)[:NZ].reshape(NB, 8, 128)
                    blocks = turn_blocks(blocks, 1)
                    for v in range(NB):
                        tab[arr, cell, places[v], :] = blocks[v]
                        if arr == 0:
                            flux[cell, places[v], :] = zero

    @pl.loop(0, 9)
    def _(cell):
        for arr in range(2):
            for k in range(4):
                first, wrapped = pl.ds(FRONT + LEVEL * k, 8), pl.ds(FRONT + NB * PITCH + LEVEL * k, 8)
                tab[arr, cell, first, :] = jnp.where(odd_patch, tab[arr, cell, wrapped, :], tab[arr, cell, first, :])
        for k in range(4):
            flux[cell, pl.ds(FRONT + LEVEL * k, 8), :] = zero

    pl.semaphore_wait(barrier, has_left.astype(jnp.int32) + has_right.astype(jnp.int32) + 1)

    keep_send = oct_y == 1 - dy
    even_mask, odd_mask = oct_y == dy, oct_y == 1 - dy
    mirror_x, mirror_y = dx == 0, dy == 0
    has = (has_left, has_right, True)
    trips = (trip_left, trip_right, T_Y)

    def copy(kind, n, count=1):
        slot, here, batch = (n + 1 + trips[kind]) & (RING - 1), n & (NSEND - 1), (n >> 3) & 1
        if count > 1:
            here, slot = pl.ds(8 * batch, count), pl.ds(0, count)
        if kind == 2:
            return pltpu.make_async_remote_copy(
                src_ref=ysend.at[here], dst_ref=yrecv.at[slot], send_sem=ys_sem.at[batch],
                recv_sem=yr_sem.at[0 if count > 1 else slot], device_id={"y": 1 - dy}, device_id_type=MESH)
        return pltpu.make_async_remote_copy(
            src_ref=xsend.at[here], dst_ref=xrecv.at[kind, slot], send_sem=xs_sem.at[kind, batch],
            recv_sem=xr_sem.at[kind, 0 if count > 1 else slot],
            device_id={"x": dx - 1 if kind == 0 else dx + 1}, device_id_type=MESH)

    def arrival(kind, n):
        slot = n & (RING - 1)
        if kind == 2:
            return pltpu.make_async_remote_copy(
                src_ref=ysend.at[0], dst_ref=yrecv.at[slot], send_sem=ys_sem.at[0], recv_sem=yr_sem.at[slot],
                device_id={"y": dy}, device_id_type=MESH)
        return pltpu.make_async_remote_copy(
            src_ref=xsend.at[0], dst_ref=xrecv.at[kind, slot], send_sem=xs_sem.at[kind, 0],
            recv_sem=xr_sem.at[kind, slot], device_id={"x": dx}, device_id_type=MESH)

    def when(cond, act):
        if cond is True:
            act()
        else:
            pl.when(cond)(act)

    def both(one, two):
        return two if one is True else (one if two is True else one & two)

    def next_turn(turn_now):
        return jnp.where(turn_now == NB - 1, 0, turn_now + 1)

    senders = (has_right, has_left, True)
    delays = (trip_right, trip_left, T_Y)

    def block(n, turn_now):
        here = n & (NSEND - 1)
        slot = n & (RING - 1)
        now, last, before = n & 3, (n + 3) & 3, (n + 2) & 3

        outs = [xbuf[pl.ds(72 * q + 8, 8, stride=9), :] for q in range(3 * U)]
        for kind in THREE:
            when(both(senders[kind], n > delays[kind]), lambda kind=kind: arrival(kind, n).wait_recv())

        edges = []
        for q in range(3 * U):
            rows = tile(q)
            from_left = jnp.where(mirror_x, pltpu.roll(outs[q], 64, 1), xrecv[1, slot, rows, :])
            edges.append(jnp.where(low_half, xrecv[0, slot, rows, :], from_left))
        def mirrored(val, shift):
            return jnp.where(mirror_y, pltpu.roll(val, shift, 1), 0.0)

        def incoming(r, odd):
            old = pack[last, 2 * r - 2 + odd] if r else pack[before, 2 * U - 1]
            got = yrecv[slot, r]
            if odd:
                return jnp.where(odd_mask, pltpu.roll(got, 64, 1), mirrored(old, 96))
            return jnp.where(even_mask, got, mirrored(old, 32) if r else refl[...])

        delayed = inodd[...]
        arriving = {0: incoming(0, 0), 1: incoming(0, 1)}
        refl[...] = mirrored(pack[last, 2 * U - 2], 32)

        mains, mixes = {}, {}

        def serve(s, faces):
            group = s // 4
            for i in THREE:
                f = 3 * (s % 4) + i
                spot = SPOTS[f]
                mains[f] = pltpu.roll(faces[i], 1, 1)
                mixed = jnp.where(last_y, faces[i], delayed if group == 2 * U - 1 else arriving[group])
                mixes[PARTNER[f]] = pltpu.roll(mixed, (1 + spot + (16 if group % 2 else 112)) % 128, 1)
                pltpu.store(pack.at[last if group == 2 * U - 1 else now, group], mixes[PARTNER[f]], mask=patch_y == spot)
            for f in [f for f in mains if f in mixes]:
                ybuf[(12 * group + f + 24) % FACES] = jnp.where(first_y, mixes.pop(f), mains.pop(f))

        for s in range(SLOTS - 4, SLOTS):
            serve(s, [yraw[3 * (s + 4 - SLOTS) + i] for i in THREE])

        turns = [turn_now]
        for _ in range(U):
            turns.append(next_turn(turns[-1]))
        z_face = [zbuf[c] for c in CELLS]
        coef = [cbuf[pos] for pos in range(5)]
        for s in range(SLOTS):
            if s % 4 == 0:
                fresh = hbuf[...] == 2 * turns[s // 8] + (s // 4) % 2
                row = pl.ds(U * n + s // 8, 1)
                coef = [jnp.where(fresh, ntab[pos, row, :], coef[pos]) for pos in range(5)]
                asum, ax, ay, az, wt = coef
                z_face = [jnp.where(fresh, 0.0, z_face[c]) for c in CELLS]
            if s == 4:
                for q in range(3 * U):
                    xbuf[pl.ds(72 * q, 8, stride=9), :] = edges[q]
            rows = pl.ds(turns[s // 8] * PITCH + (FRONT + LEVEL * (s % 8)), 8)
            x_face = [xbuf[pl.ds(9 * (3 * s + j), 8), :] for j in THREE]
            y_out = []
            for i in THREE:
                y_face = ybuf[3 * s + i]
                for j in THREE:
                    c = 3 * i + j
                    total = ((tab[0, c, rows, :] + z_face[c]) + x_face[j]) + y_face
                    psi = total * (1.0 / (tab[1, c, rows, :] + asum))
                    x_face[j] = ax * psi - x_face[j]
                    y_face = ay * psi - y_face
                    z_face[c] = az * psi - z_face[c]
                    flux[c, rows, :] = flux[c, rows, :] + wt * psi
                y_out.append(y_face)
            if s % 4 == 0 and s < SLOTS - 8:
                arriving[s // 4 + 2] = incoming(s // 8 + 1, s // 4 % 2)
            if s < SLOTS - 4:
                serve(s, y_out)
            else:
                for i in THREE:
                    yraw[3 * (s + 4 - SLOTS) + i] = y_out[i]
            for j in THREE:
                xbuf[pl.ds(9 * ((3 * s + j + 12) % FACES) + 1, 8), :] = x_face[j]
        for c in CELLS:
            zbuf[c] = z_face[c]
        for pos in range(5):
            cbuf[pos] = coef[pos]
        inodd[...] = arriving[2 * U - 1]
        for q in range(3 * U):
            xsend[here, tile(q), :] = xbuf[pl.ds(72 * q + 8, 8, stride=9), :]
        for r in range(U):
            pair, first = (now, 2 * r - 2) if r else (last, 2 * U - 2)
            ysend[here, r] = jnp.where(keep_send, pack[pair, first], pack[pair, first + 1])
        for kind in (2, 0, 1):
            when(has[kind], lambda kind=kind: copy(kind, n).start())
        return turns[U]

    def batch(first, turn_now):
        for kind in THREE:
            when(both(has[kind], first >= 2), lambda kind=kind: copy(kind, 8 * (first - 2), 8).wait_send())
        return lax.fori_loop(8 * first, jnp.minimum(8 * first + 8, BLOCKS), block, turn_now)

    lax.fori_loop(0, (BLOCKS + 7) // 8, batch, jnp.int32(0))

    @pl.loop(0, 9)
    def _(cell):
        for k in range(4):
            flux[cell, pl.ds(FRONT + NB * PITCH + LEVEL * k, 8), :] = flux[cell, pl.ds(FRONT + LEVEL * k, 8), :]

    @pl.loop(0, 3)
    def _(i):
        for half, odd in [(k // 2, k & 1) for k in range(8)]:
            for j in THREE:
                cell = 3 * i + j
                blocks = jnp.stack([flux[cell, place, :] for place in block_rows(half, odd)])
                blocks = turn_blocks(blocks, -1).reshape(NZ, 128)
                lo = blocks[:128].T
                hi = jnp.concatenate([blocks[128:], jnp.zeros((56, 128), F32)], axis=0).T
                for octant, side, x_abs, y_abs, rev in row_groups(2 * half + odd, i, j):
                    for zh in range(2):
                        val = (lo, hi)[zh][16 * octant + 8 * side:16 * octant + 8 * side + 8]
                        if rev:
                            val = gather(val, flip_rows, 0)
                        acc[octant, zh, x_abs, pl.ds(y_abs, 8, stride=3), :] = val

    @pl.loop(0, NX, step=8)
    def _(first):
        for x in (first + k for k in range(8)):
            (dn_a, up_a), (dn_b, up_b) = [
                [sum(acc[octant, zh, x] for octant in range(bz + 2, 8, 2)) + acc[bz, zh, x]
                 for bz in range(2)] for zh in range(2)]
            dn_a, dn_b = mirror_plane(dn_a), mirror_plane(dn_b)
            out_ref[x, :, pl.ds(0, 128)] = up_a + jnp.where(tail, dn_b, dn_a)
            out_ref[x, :, pl.ds(128, 72)] = (up_b + dn_a)[:, :72]

    for kind in THREE:
        for first in range(max(0, 8 * ((BLOCKS + 7) // 8 - 2)), BLOCKS, 8):
            when(has[kind], lambda kind=kind, first=first:
                 copy(kind, jnp.int32(first), min(8, BLOCKS - first)).wait_send())
        for late in range(1 + (max(T_NEAR, T_FAR) if kind < 2 else T_Y)):
            when(both(senders[kind], late <= delays[kind]), lambda kind=kind, late=late:
                 arrival(kind, jnp.int32(BLOCKS + late)).wait_recv())


def solution(mesh):
    grid_spec = P(("g", "x"), "y", None)

    def column_sweep(source, sigma_t, cos_x, cos_y, cos_z, weights):
        vmem = pl.BlockSpec(memory_space=pltpu.VMEM)
        return pl.pallas_call(
            kernel,
            out_shape=pltpu.VMEM((NX, NY, NZ), F32),
            in_specs=[pl.BlockSpec(memory_space=pl.ANY)] * 6,
            out_specs=vmem,
            scratch_shapes=[pltpu.SMEM((ND,), F32)] * 4 + [
                pltpu.VMEM((2, NX, NY, NZ), F32),
                pltpu.VMEM((2, 4, NX, NY, 128), F32),
                pltpu.VMEM((2, 9, ROWS, 128), F32),
                pltpu.VMEM((9, ROWS, 128), F32),
                pltpu.VMEM((8, 2, NX, NY, 128), F32),
                pltpu.VMEM((8, 128), jnp.int32),
                pltpu.VMEM((5, 8, 128), F32),
                pltpu.VMEM((5, 256 * pl.cdiv(U * BLOCKS, 256), 128), F32),
                pltpu.VMEM((5, 8, 128), F32),
                pltpu.VMEM((9 * FACES + 8, 128), F32),
                pltpu.VMEM((FACES, 8, 128), F32),
                pltpu.VMEM((12, 8, 128), F32),
                pltpu.VMEM((9, 8, 128), F32),
                pltpu.VMEM(VREG, F32),
                pltpu.VMEM(VREG, F32),
                pltpu.VMEM((NSEND, FACES, 128), F32),
                pltpu.VMEM((2, RING, FACES, 128), F32),
                pltpu.VMEM((NSEND, U, 8, 128), F32),
                pltpu.VMEM((RING, U, 8, 128), F32),
                pltpu.VMEM((4, 2 * U, 8, 128), F32),
                pltpu.SemaphoreType.DMA((4,)),
                pltpu.SemaphoreType.DMA((2, PARTS)),
                pltpu.SemaphoreType.DMA((2, 2)),
                pltpu.SemaphoreType.DMA((2, RING)),
                pltpu.SemaphoreType.DMA((2,)),
                pltpu.SemaphoreType.DMA((RING,)),
            ],
            compiler_params=pltpu.CompilerParams(
                collective_id=0, has_side_effects=True, vmem_limit_bytes=60 * 1024 * 1024),
        )(cos_x, cos_y, cos_z, weights, source, sigma_t)

    return jax.shard_map(column_sweep, mesh=mesh, in_specs=(grid_spec, grid_spec, P(), P(), P(), P()),
                         out_specs=grid_spec, check_vma=False)
```

```python
import functools

import jax
import jax.numpy as jnp
from jax import lax
from jax.experimental import pallas as pl
from jax.experimental.pallas import tpu as pltpu
from jax.sharding import PartitionSpec as P

F32 = jnp.float32
MESH = pl.DeviceIdType.MESH
NX, NY, NZ = 24, 48, 200
ND = 10
NB = NZ // 8
VREG = (8, 128)
LEVEL = 12
FRONT = 4 * LEVEL
PITCH = 8 * LEVEL
ROWS = NB * PITCH + 112
U = 2
SLOTS = 8 * U
FACES = 3 * SLOTS
T_NEAR = 3
T_FAR = 8
T_Y = 8
D_XR = U
D_YR = U + 1
RING = 32
NSEND = 16
HOIST = 44
THREE, CELLS = range(3), range(9)
PARTS = 2
SPOTS = [2, 13, 3, 4, 11, 12, 5, 10, 6, 7, 8, 9]
PARTNER = [SPOTS.index(15 - spot) for spot in SPOTS]


def x_lags():
    near, far = U * (T_NEAR + 1), U * (T_FAR + 1)
    hops = [near, far, near, D_XR, near, far, near]
    lags = [0]
    for hop in hops:
        lags.append(lags[-1] + 4 + hop)
    return lags


def y_lags():
    lags = [0]
    for hop in [U * (T_Y + 1) + 1, D_YR, U * (T_Y + 1) + 1]:
        lags.append(lags[-1] + 16 + hop)
    return lags


LAG_X, LAG_Y = x_lags(), y_lags()
STEPS = ND * NB + LAG_X[-1] + LAG_Y[-1] + 4 + 15
BLOCKS = (STEPS + U - 1) // U


def gather(val, spots, axis):
    dims = lax.GatherDimensionNumbers(
        offset_dims=(), collapsed_slice_dims=(axis,), start_index_map=(axis,),
        operand_batching_dims=(1 - axis,), start_indices_batching_dims=(1 - axis,))
    return lax.gather(val, spots, dims, slice_sizes=(1, 1), mode=lax.GatherScatterMode.PROMISE_IN_BOUNDS)


def tile(k):
    return pl.ds(8 * k, 8)


def pick(values, idx):
    out = jnp.int32(values[0])
    for pos in range(1, len(values)):
        out = jnp.where(idx == pos, jnp.int32(values[pos]), out)
    return out


def kernel(cx_hbm, cy_hbm, cz_hbm, wt_hbm, src_hbm, sig_hbm, out_ref,
           cx_ref, cy_ref, cz_ref, wt_ref, inbuf, nat, tab, flux, acc, hbuf, ctab, ntab, cbuf, xbuf, ybuf, yraw, zbuf, inodd, refl,
           xsend, xrecv, ysend, yrecv, pack,
           c_sem, in_sem, xs_sem, xr_sem, ys_sem, yr_sem):
    def load(arr, part):
        planes = pl.ds(part * (NX // PARTS), NX // PARTS)
        return pltpu.make_async_copy((src_hbm, sig_hbm)[arr].at[planes], inbuf.at[arr, planes], in_sem.at[arr, part])

    coefs = [pltpu.make_async_copy(far, near, c_sem.at[k]) for k, (far, near) in enumerate(
        zip((cx_hbm, cy_hbm, cz_hbm, wt_hbm), (cx_ref, cy_ref, cz_ref, wt_ref)))]
    for one in coefs:
        one.start()
    for part in range(PARTS):
        for arr in range(2):
            load(arr, part).start()

    dx = lax.axis_index("x")
    dy = lax.axis_index("y")
    has_left, has_right = dx > 0, dx < 3
    odd_x = (dx & 1) == 1
    trip_left = jnp.where(odd_x, T_NEAR, T_FAR)
    trip_right = jnp.where(odd_x, T_FAR, T_NEAR)
    lane = lax.broadcasted_iota(jnp.int32, VREG, 1)
    subl = lax.broadcasted_iota(jnp.int32, VREG, 0)
    oct_id = lane // 16
    oct_y = (oct_id // 2) % 2
    patch_y = lane - 16 * oct_id
    zero = jnp.zeros(VREG, F32)
    low_half = lane < 64
    first_y, last_y = patch_y == 0, patch_y == 15

    lag_xm, lag_xp = pick(LAG_X[:4][::-1], dx), pick(LAG_X[4:], dx)
    lag_ym, lag_yp = pick(LAG_Y[:2][::-1], dy), pick(LAG_Y[2:], dy)
    lag_oct = jnp.where(lane >= 64, lag_xp, lag_xm) + jnp.where(oct_y == 1, lag_yp, lag_ym)
    lag_lane = patch_y + lag_oct
    hbuf[...] = lax.rem(2 * lag_lane + subl, 2 * NB)
    turn = lax.rem(lag_lane, NB)
    turn_bits = [(turn >> bit) & 1 == 1 for bit in range(5)]

    for k in range(9 * FACES // 8 + 1):
        xbuf[tile(k), :] = zero
    for k in range(FACES):
        ybuf[k] = zero
    for k in range(12):
        yraw[k] = zero
    for k in CELLS:
        zbuf[k] = zero
    inodd[...] = zero
    refl[...] = zero
    for k in range(4):
        for j in range(2 * U):
            pack[k, j] = zero

    @pl.loop(0, RING)
    def _(k):
        for side in range(2):
            for q in range(SLOTS * 3 // 8):
                xrecv[side, k, tile(q), :] = zero
            for r in range(U):
                yrecv[k, r] = zero

    barrier = pltpu.get_barrier_semaphore()

    @pl.when(has_left)
    def _():
        pl.semaphore_signal(barrier, inc=1, device_id={"x": dx - 1}, device_id_type=MESH)

    @pl.when(has_right)
    def _():
        pl.semaphore_signal(barrier, inc=1, device_id={"x": dx + 1}, device_id_type=MESH)

    pl.semaphore_signal(barrier, inc=1, device_id={"y": 1 - dy}, device_id_type=MESH)

    for one in coefs:
        one.wait()
    for pos in range(5):
        col = jnp.ones(VREG, F32) if pos == 0 else zero
        for m in range(ND):
            two_x, two_y, two_z = 2.0 * cx_ref[m], 2.0 * cy_ref[m], 2.0 * cz_ref[m]
            val = (two_x + two_y + two_z, 2.0 * two_x, 2.0 * two_y, 2.0 * two_z, wt_ref[m])[pos]
            col = jnp.where(lane == m + 1, val, col)
        ctab[pos] = col
        cbuf[pos] = jnp.ones(VREG, F32) if pos == 0 else zero

    cols = [ctab[pos] for pos in range(5)]

    @pl.loop(0, ntab.shape[1] // 256)
    def _(k):
        for part in range(32):
            first = 256 * k + 8 * part
            c_idx = jnp.clip((((first + subl - lag_oct) * 1311) >> 15) + 1, 0, ND + 1)[..., None]
            for pos in range(5):
                ntab[pos, pl.ds(first, 8), :] = gather(cols[pos], c_idx, 1)

    mirror = ((71 - lane) & 127)[..., None]
    tail = lax.broadcasted_iota(jnp.int32, (NY, 128), 1) < 72

    def mirror_plane(val):
        return jnp.concatenate([gather(val[8 * k:8 * k + 8], mirror, 1) for k in range(NY // 8)], axis=0)

    for part in range(PARTS):
        for arr in range(2):
            load(arr, part).wait()

        @pl.loop(part * (NX // PARTS), (part + 1) * (NX // PARTS), step=12)
        def _(first):
            for x in (first + k for k in range(12)):
                for arr in range(2):
                    half_a = inbuf[arr, x, :, pl.ds(0, 128)]
                    nat[arr, 0, x] = half_a
                    nat[arr, 1, x, :, pl.ds(0, 72)] = inbuf[arr, x, :, pl.ds(128, 72)]
                    flip_a, flip_b = mirror_plane(half_a), mirror_plane(nat[arr, 1, x])
                    nat[arr, 2, x] = jnp.where(tail, flip_b, flip_a)
                    nat[arr, 3, x] = flip_a

    flip_rows = (7 - subl)[..., None]

    def row_groups(x_patch, i, j):
        x_up = 3 * x_patch + i
        x_both = (NX - 1 - x_up, x_up)
        for octant in range(8):
            by, x_abs = (octant // 2) % 2, x_both[octant // 4]
            for half in range(2):
                y_abs = (24 * half + j) if by else (26 - 24 * half - j)
                yield octant, half, x_abs, y_abs, by == 0

    def turn_blocks(blocks, step):
        for bit in range(5):
            cut = (-step * (1 << bit)) % NB
            shifted = jnp.concatenate([blocks[cut:], blocks[:cut]], axis=0)
            blocks = jnp.where(jnp.broadcast_to(turn_bits[bit][None], blocks.shape), shifted, blocks)
        return blocks

    odd_patch = (subl & 1) == 1

    def block_rows(half, odd):
        blocks = [(v + half) % NB if isinstance(half, int) else lax.rem(v + half, NB) for v in range(NB)]
        return [pl.ds(block * PITCH + (FRONT + 2 * half + odd + 4 * LEVEL * odd), 8, stride=LEVEL) for block in blocks]

    @pl.loop(0, 6)
    def _(trip):
        i = trip // 2
        for half, odd in [(2 * (trip & 1) + k // 2, k & 1) for k in range(4)]:
            places = block_rows(half, odd)
            for j in THREE:
                cell = 3 * i + j
                for arr in range(2):
                    pieces = [[], []]
                    for octant, part, x_abs, y_abs, rev in row_groups(2 * half + odd, i, j):
                        for zh in range(2):
                            kind = zh + (0 if octant % 2 else 2)
                            val = nat[arr, kind, x_abs, pl.ds(y_abs, 8, stride=3), :]
                            if rev:
                                val = gather(val, flip_rows, 0)
                            pieces[zh].append(val)
                    lo = jnp.concatenate(pieces[0], axis=0).T
                    hi = jnp.concatenate(pieces[1], axis=0).T
                    blocks = jnp.concatenate([lo, hi], axis=0)[:NZ].reshape(NB, 8, 128)
                    blocks = turn_blocks(blocks, 1)
                    for v in range(NB):
                        tab[arr, cell, places[v], :] = blocks[v]
                        if arr == 0:
                            flux[cell, places[v], :] = zero

    @pl.loop(0, 9)
    def _(cell):
        for arr in range(2):
            for k in range(4):
                first, wrapped = pl.ds(FRONT + LEVEL * k, 8), pl.ds(FRONT + NB * PITCH + LEVEL * k, 8)
                tab[arr, cell, first, :] = jnp.where(odd_patch, tab[arr, cell, wrapped, :], tab[arr, cell, first, :])
        for k in range(4):
            flux[cell, pl.ds(FRONT + LEVEL * k, 8), :] = zero

    pl.semaphore_wait(barrier, has_left.astype(jnp.int32) + has_right.astype(jnp.int32) + 1)

    keep_send = oct_y == 1 - dy
    even_mask, odd_mask = oct_y == dy, oct_y == 1 - dy
    mirror_x, mirror_y = dx == 0, dy == 0
    has = (has_left, has_right, True)
    trips = (trip_left, trip_right, T_Y)

    def copy(kind, n, count=1):
        slot, here, batch = (n + 1 + trips[kind]) & (RING - 1), n & (NSEND - 1), (n >> 3) & 1
        if count > 1:
            here, slot = pl.ds(8 * batch, count), pl.ds(0, count)
        if kind == 2:
            return pltpu.make_async_remote_copy(
                src_ref=ysend.at[here], dst_ref=yrecv.at[slot], send_sem=ys_sem.at[batch],
                recv_sem=yr_sem.at[0 if count > 1 else slot], device_id={"y": 1 - dy}, device_id_type=MESH)
        return pltpu.make_async_remote_copy(
            src_ref=xsend.at[here], dst_ref=xrecv.at[kind, slot], send_sem=xs_sem.at[kind, batch],
            recv_sem=xr_sem.at[kind, 0 if count > 1 else slot],
            device_id={"x": dx - 1 if kind == 0 else dx + 1}, device_id_type=MESH)

    def arrival(kind, n):
        slot = n & (RING - 1)
        if kind == 2:
            return pltpu.make_async_remote_copy(
                src_ref=ysend.at[0], dst_ref=yrecv.at[slot], send_sem=ys_sem.at[0], recv_sem=yr_sem.at[slot],
                device_id={"y": dy}, device_id_type=MESH)
        return pltpu.make_async_remote_copy(
            src_ref=xsend.at[0], dst_ref=xrecv.at[kind, slot], send_sem=xs_sem.at[kind, 0],
            recv_sem=xr_sem.at[kind, slot], device_id={"x": dx}, device_id_type=MESH)

    def when(cond, act):
        if cond is True:
            act()
        else:
            pl.when(cond)(act)

    def both(one, two):
        return two if one is True else (one if two is True else one & two)

    def next_turn(turn_now):
        return jnp.where(turn_now == NB - 1, 0, turn_now + 1)

    senders = (has_right, has_left, True)
    delays = (trip_right, trip_left, T_Y)

    def block(n, turn_now):
        here = n & (NSEND - 1)
        slot = n & (RING - 1)
        now, last, before = n & 3, (n + 3) & 3, (n + 2) & 3

        outs = [xbuf[pl.ds(72 * q + 8, 8, stride=9), :] for q in range(3 * U)]
        for kind in THREE:
            when(both(senders[kind], n > delays[kind]), lambda kind=kind: arrival(kind, n).wait_recv())

        edges = []
        for q in range(3 * U):
            rows = tile(q)
            from_left = jnp.where(mirror_x, pltpu.roll(outs[q], 64, 1), xrecv[1, slot, rows, :])
            edges.append(jnp.where(low_half, xrecv[0, slot, rows, :], from_left))
        def mirrored(val, shift):
            return jnp.where(mirror_y, pltpu.roll(val, shift, 1), 0.0)

        def incoming(r, odd):
            old = pack[last, 2 * r - 2 + odd] if r else pack[before, 2 * U - 1]
            got = yrecv[slot, r]
            if odd:
                return jnp.where(odd_mask, pltpu.roll(got, 64, 1), mirrored(old, 96))
            return jnp.where(even_mask, got, mirrored(old, 32) if r else refl[...])

        delayed = inodd[...]
        arriving = {0: incoming(0, 0), 1: incoming(0, 1)}
        refl[...] = mirrored(pack[last, 2 * U - 2], 32)

        mains, mixes = {}, {}

        def serve(s, faces):
            group = s // 4
            for i in THREE:
                f = 3 * (s % 4) + i
                spot = SPOTS[f]
                mains[f] = pltpu.roll(faces[i], 1, 1)
                mixed = jnp.where(last_y, faces[i], delayed if group == 2 * U - 1 else arriving[group])
                mixes[PARTNER[f]] = pltpu.roll(mixed, (1 + spot + (16 if group % 2 else 112)) % 128, 1)
                pltpu.store(pack.at[last if group == 2 * U - 1 else now, group], mixes[PARTNER[f]], mask=patch_y == spot)
            for f in [f for f in mains if f in mixes]:
                ybuf[(12 * group + f + 24) % FACES] = jnp.where(first_y, mixes.pop(f), mains.pop(f))

        for s in range(SLOTS - 4, SLOTS):
            serve(s, [yraw[3 * (s + 4 - SLOTS) + i] for i in THREE])

        turns = [turn_now]
        for _ in range(U):
            turns.append(next_turn(turns[-1]))
        z_face = [zbuf[c] for c in CELLS]
        coef = [cbuf[pos] for pos in range(5)]
        for s in range(SLOTS):
            if s % 4 == 0:
                fresh = hbuf[...] == 2 * turns[s // 8] + (s // 4) % 2
                row = pl.ds(U * n + s // 8, 1)
                coef = [jnp.where(fresh, ntab[pos, row, :], coef[pos]) for pos in range(5)]
                asum, ax, ay, az, wt = coef
                z_face = [jnp.where(fresh, 0.0, z_face[c]) for c in CELLS]
            if s == 4:
                for q in range(3 * U):
                    xbuf[pl.ds(72 * q, 8, stride=9), :] = edges[q]
            rows = pl.ds(turns[s // 8] * PITCH + (FRONT + LEVEL * (s % 8)), 8)
            x_face = [xbuf[pl.ds(9 * (3 * s + j), 8), :] for j in THREE]
            y_out = []
            for i in THREE:
                y_face = ybuf[3 * s + i]
                for j in THREE:
                    c = 3 * i + j
                    total = ((tab[0, c, rows, :] + z_face[c]) + x_face[j]) + y_face
                    psi = total * (1.0 / (tab[1, c, rows, :] + asum))
                    x_face[j] = ax * psi - x_face[j]
                    y_face = ay * psi - y_face
                    z_face[c] = az * psi - z_face[c]
                    flux[c, rows, :] = flux[c, rows, :] + wt * psi
                y_out.append(y_face)
            if s % 4 == 0 and s < SLOTS - 8:
                arriving[s // 4 + 2] = incoming(s // 8 + 1, s // 4 % 2)
            if s < SLOTS - 4:
                serve(s, y_out)
            else:
                for i in THREE:
                    yraw[3 * (s + 4 - SLOTS) + i] = y_out[i]
            for j in THREE:
                xbuf[pl.ds(9 * ((3 * s + j + 12) % FACES) + 1, 8), :] = x_face[j]
        for c in CELLS:
            zbuf[c] = z_face[c]
        for pos in range(5):
            cbuf[pos] = coef[pos]
        inodd[...] = arriving[2 * U - 1]
        for q in range(3 * U):
            xsend[here, tile(q), :] = xbuf[pl.ds(72 * q + 8, 8, stride=9), :]
        for r in range(U):
            pair, first = (now, 2 * r - 2) if r else (last, 2 * U - 2)
            ysend[here, r] = jnp.where(keep_send, pack[pair, first], pack[pair, first + 1])
        for kind in (2, 0, 1):
            when(has[kind], lambda kind=kind: copy(kind, n).start())
        return turns[U]

    def batch(first, turn_now):
        for kind in THREE:
            when(both(has[kind], first >= 2), lambda kind=kind: copy(kind, 8 * (first - 2), 8).wait_send())
        return lax.fori_loop(8 * first, jnp.minimum(8 * first + 8, BLOCKS), block, turn_now)

    lax.fori_loop(0, (BLOCKS + 7) // 8, batch, jnp.int32(0))

    @pl.loop(0, 9)
    def _(cell):
        for k in range(4):
            flux[cell, pl.ds(FRONT + NB * PITCH + LEVEL * k, 8), :] = flux[cell, pl.ds(FRONT + LEVEL * k, 8), :]

    @pl.loop(0, 3)
    def _(i):
        for half, odd in [(k // 2, k & 1) for k in range(8)]:
            for j in THREE:
                cell = 3 * i + j
                blocks = jnp.stack([flux[cell, place, :] for place in block_rows(half, odd)])
                blocks = turn_blocks(blocks, -1).reshape(NZ, 128)
                lo = blocks[:128].T
                hi = jnp.concatenate([blocks[128:], jnp.zeros((56, 128), F32)], axis=0).T
                for octant, side, x_abs, y_abs, rev in row_groups(2 * half + odd, i, j):
                    for zh in range(2):
                        val = (lo, hi)[zh][16 * octant + 8 * side:16 * octant + 8 * side + 8]
                        if rev:
                            val = gather(val, flip_rows, 0)
                        acc[octant, zh, x_abs, pl.ds(y_abs, 8, stride=3), :] = val

    @pl.loop(0, NX, step=12)
    def _(first):
        for x in (first + k for k in range(12)):
            (dn_a, up_a), (dn_b, up_b) = [
                [sum(acc[octant, zh, x] for octant in range(bz + 2, 8, 2)) + acc[bz, zh, x]
                 for bz in range(2)] for zh in range(2)]
            dn_a, dn_b = mirror_plane(dn_a), mirror_plane(dn_b)
            out_ref[x, :, pl.ds(0, 128)] = up_a + jnp.where(tail, dn_b, dn_a)
            out_ref[x, :, pl.ds(128, 72)] = (up_b + dn_a)[:, :72]

    for kind in THREE:
        for first in range(max(0, 8 * ((BLOCKS + 7) // 8 - 2)), BLOCKS, 8):
            when(has[kind], lambda kind=kind, first=first:
                 copy(kind, jnp.int32(first), min(8, BLOCKS - first)).wait_send())
        for late in range(1 + (max(T_NEAR, T_FAR) if kind < 2 else T_Y)):
            when(both(senders[kind], late <= delays[kind]), lambda kind=kind, late=late:
                 arrival(kind, jnp.int32(BLOCKS + late)).wait_recv())


def solution(mesh):
    grid_spec = P(("g", "x"), "y", None)

    def column_sweep(source, sigma_t, cos_x, cos_y, cos_z, weights):
        vmem = pl.BlockSpec(memory_space=pltpu.VMEM)
        return pl.pallas_call(
            kernel,
            out_shape=pltpu.VMEM((NX, NY, NZ), F32),
            in_specs=[pl.BlockSpec(memory_space=pl.ANY)] * 6,
            out_specs=vmem,
            scratch_shapes=[pltpu.SMEM((ND,), F32)] * 4 + [
                pltpu.VMEM((2, NX, NY, NZ), F32),
                pltpu.VMEM((2, 4, NX, NY, 128), F32),
                pltpu.VMEM((2, 9, ROWS, 128), F32),
                pltpu.VMEM((9, ROWS, 128), F32),
                pltpu.VMEM((8, 2, NX, NY, 128), F32),
                pltpu.VMEM((8, 128), jnp.int32),
                pltpu.VMEM((5, 8, 128), F32),
                pltpu.VMEM((5, 256 * pl.cdiv(U * BLOCKS, 256), 128), F32),
                pltpu.VMEM((5, 8, 128), F32),
                pltpu.VMEM((9 * FACES + 8, 128), F32),
                pltpu.VMEM((FACES, 8, 128), F32),
                pltpu.VMEM((12, 8, 128), F32),
                pltpu.VMEM((9, 8, 128), F32),
                pltpu.VMEM(VREG, F32),
                pltpu.VMEM(VREG, F32),
                pltpu.VMEM((NSEND, FACES, 128), F32),
                pltpu.VMEM((2, RING, FACES, 128), F32),
                pltpu.VMEM((NSEND, U, 8, 128), F32),
                pltpu.VMEM((RING, U, 8, 128), F32),
                pltpu.VMEM((4, 2 * U, 8, 128), F32),
                pltpu.SemaphoreType.DMA((4,)),
                pltpu.SemaphoreType.DMA((2, PARTS)),
                pltpu.SemaphoreType.DMA((2, 2)),
                pltpu.SemaphoreType.DMA((2, RING)),
                pltpu.SemaphoreType.DMA((2,)),
                pltpu.SemaphoreType.DMA((RING,)),
            ],
            compiler_params=pltpu.CompilerParams(
                collective_id=0, has_side_effects=True, vmem_limit_bytes=60 * 1024 * 1024),
        )(cos_x, cos_y, cos_z, weights, source, sigma_t)

    return jax.shard_map(column_sweep, mesh=mesh, in_specs=(grid_spec, grid_spec, P(), P(), P(), P()),
                         out_specs=grid_spec, check_vma=False)
```
